32 devices in a mesh: gz: 8 (over y, x, core), gy: 4 (over z).
Axes of the slice: x: 2, y: 2, z: 4, core: 2. Of those that a mesh axis runs over, the one named last changes fastest.
Arguments:
- coarse_density: float32 [96, 96, 96], P(None, 'gy'), may hold values from -4 to 4
- density_in: float32 [192, 36864], P('gz', 'gy'), may hold values from -9 to 9
- history: float32 [8, 192, 36864], P(None, 'gz', 'gy'), may hold values from -12 to 12
- atom_cell: int32 [8, 4, 1], P('gz', 'gy'), may hold values from 0 to 221183
- atom_offset: float32 [3, 8, 4, 1], P(None, 'gz', 'gy'), may hold values from 0 to 1
- atom_charge: float32 [8, 4, 1], P('gz', 'gy'), may hold values from -16 to 16
- atom_width: float32 [8, 4, 1], P('gz', 'gy'), may hold values from 0.25 to 1
Outputs:
- residual: float32 [192, 36864], P('gz', 'gy')
- potential: float32 [192, 36864], P('gz', 'gy')
- intersections: float32 [9], replicated
The draws below stay inside these ranges and needn't reach their ends.
Inputs may be any that keep to these rules, and one draw needn't show every extreme that they name: `atom_cell`: the cell lies inside the block of 24 x 48 x 192 fine cells of the slot's first two indices.
All inputs are finite; a program needn't handle non-finite values.
Results may differ from the reference program's by a relative error of at most 0.0003.
Values sent between devices are 32-bit elements; how exact they have to be, the bound alone decides.
No kernel may reach another device: no remote copies, remote signals or barrier semaphores. Data moves between devices by JAX's collectives and lax.ppermute only.
A program may use at most 64 MiB of HBM per device.

```python
import math
import jax
import jax.numpy as jnp
from jax import lax

NC = 96
HIST = 8
ATOM_DEV = 1
RC = 4
NF = 192
FZ = 24
FY = 48
N_GZ = 8
N_GY = 4


def midpoint_drawn(extended, dimension, cells_in):

    def window(offset):
        return lax.slice_in_dim(extended, offset, offset + cells_in, axis=dimension)
    even_cells = window(2)
    odd_cells = (9.0 * (window(2) + window(3)) - window(1) - window(4)) / 16.0
    merged = jnp.stack([even_cells, odd_cells], dimension + 1)
    new_shape = list(even_cells.shape)
    new_shape[dimension] = 2 * cells_in
    return merged.reshape(new_shape)


def periodic_drawn(values, dimension):
    length = values.shape[dimension]
    leading = lax.slice_in_dim(values, length - 2, length, axis=dimension)
    trailing = lax.slice_in_dim(values, 0, 2, axis=dimension)
    return jnp.concatenate([leading, values, trailing], dimension)


def coarse_field(key):
    values = jax.random.truncated_normal(jax.random.fold_in(key, 31), -4.0, 4.0, (NC, NC, NC), jnp.float32)
    return values


def common_field(key):
    base = jax.random.truncated_normal(jax.random.fold_in(key, 11), -6.0, 6.0, (NF, NF, NF), jnp.float32)
    return base


def draw_coarse_density(key, part):
    return coarse_field(key)


def draw_density_in(key, part):
    smooth = coarse_field(key)
    for dimension in (2, 1, 0):
        smooth = midpoint_drawn(periodic_drawn(smooth, dimension), dimension, smooth.shape[dimension])
    return (smooth + 0.05 * common_field(key)).reshape(NF, NF * NF)


def draw_history(key, part):
    base = common_field(key)
    gains = jax.random.uniform(jax.random.fold_in(key, 12), (HIST, 1, 1, 1), jnp.float32, 0.3, 1.2)
    noise = jax.random.truncated_normal(jax.random.fold_in(key, 13), -6.0, 6.0, (HIST, NF, NF, NF), jnp.float32)
    return (gains * base[None] + 0.5 * noise).reshape(HIST, NF, NF * NF)


def place_ends(values, rng, least, high):
    longest = values.shape.index(max(values.shape))
    spots = []
    for shift in (0, 1):
        where = [jax.random.randint(jax.random.fold_in(rng, axis), (), 0, length) for axis, length in enumerate(values.shape)]
        where[longest] = (where[longest] + shift) % values.shape[longest]
        spots.append(tuple(where))
    return values.at[spots[0]].set(least).at[spots[1]].set(high)


def levels(key, extent, split, smallest, high):
    def one(dim, parts):
        heights = jax.random.uniform(jax.random.fold_in(jax.random.fold_in(key, 6), dim), (parts,), jnp.float32, smallest / len(split), high / len(split))
        return jnp.repeat(jnp.exp(heights), extent[dim] // parts).reshape((-1,) + (1,) * (len(extent) - dim - 1))

    factor_of = one(*split[0])
    for cut in split[1:]:
        factor_of = factor_of * one(*cut)
    return factor_of


def bell_draw(own_key, dims, deviation, most, shards=(), held_as=jnp.bfloat16):
    level = levels(own_key, dims, shards, -0.22, 0.18) if shards else 1.0
    entries = jax.random.normal(own_key, dims, jnp.float32) * deviation * level
    return jnp.minimum(jnp.maximum(entries, -most), most).astype(held_as)


def setup_inputs(seed: int = 0) -> dict:
    key_list = jax.random.split(jax.random.key(seed), 8)
    return {
        "coarse_density": draw_coarse_density(jax.random.fold_in(key_list[7], 71), 0),
        "density_in": draw_density_in(jax.random.fold_in(key_list[7], 71), 0),
        "history": draw_history(jax.random.fold_in(key_list[7], 71), 0),
        "atom_cell": place_ends(jax.random.randint(key_list[3], (N_GZ, N_GY, ATOM_DEV), 0, FZ * FY * NF), jax.random.fold_in(key_list[3], 1), 0, (FZ * FY * NF) - 1).astype(jnp.int32),
        "atom_offset": jnp.clip(1.0 * jax.random.uniform(key_list[4], (3, N_GZ, N_GY, ATOM_DEV), jnp.float32) ** levels(key_list[4], (3, N_GZ, N_GY, ATOM_DEV), ((1, 8), (2, 4)), -0.2, 0.2), 0.0, 1.0),
        "atom_charge": bell_draw(key_list[5], (N_GZ, N_GY, ATOM_DEV), 4.0, 16.0, ((0, 8), (1, 4)), jnp.float32),
        "atom_width": jnp.clip(jnp.exp(math.log(1.0) - 1.3862944 * jax.random.uniform(key_list[6], (N_GZ, N_GY, ATOM_DEV), jnp.float32) ** levels(key_list[6], (N_GZ, N_GY, ATOM_DEV), ((0, 8), (1, 4)), -0.2, 0.2)), 0.25, 1.0),
    }


def midpoint(extended, dimension, cells_in):
    def window(offset):
        return lax.slice_in_dim(extended, offset, offset + cells_in, axis=dimension)
    even_cells = window(2)
    odd_cells = (9.0 * (window(2) + window(3)) - window(1) - window(4)) / 16.0
    merged = jnp.stack([even_cells, odd_cells], dimension + 1)
    new_shape = list(even_cells.shape)
    new_shape[dimension] = 2 * cells_in
    return merged.reshape(new_shape)


def periodic(values, dimension):
    length = values.shape[dimension]
    leading = lax.slice_in_dim(values, length - 2, length, axis=dimension)
    trailing = lax.slice_in_dim(values, 0, 2, axis=dimension)
    return jnp.concatenate([leading, values, trailing], dimension)


def signed(counter, length):
    return jnp.where(counter < length // 2, counter, counter - length)


def shape_value(squared, charge, exponent):
    factor = charge * (exponent / jnp.pi) ** 1.5
    return factor * jnp.maximum(jnp.exp(-exponent * squared) - jnp.exp(-exponent * float(RC * RC)), 0.0)


def compensation(atom_cell, atom_offset, atom_charge, atom_width):
    plane_cells = FY * NF
    slab_z = jnp.arange(N_GZ, dtype=jnp.int32)[:, None, None] * FZ
    slab_y = jnp.arange(N_GY, dtype=jnp.int32)[None, :, None] * FY
    cell_z = (slab_z + atom_cell // plane_cells).reshape(-1)
    cell_y = (slab_y + (atom_cell // NF) % FY).reshape(-1)
    cell_x = (atom_cell % NF).reshape(-1)
    shifts = jnp.arange(-RC, RC + 2, dtype=jnp.int32)
    offsets = atom_offset.reshape(3, -1)
    charge = atom_charge.reshape(-1)[:, None, None, None]
    exponent = atom_width.reshape(-1)[:, None, None, None]
    index_z = (cell_z[:, None] + shifts[None, :]) % NF
    index_y = (cell_y[:, None] + shifts[None, :]) % NF
    index_x = (cell_x[:, None] + shifts[None, :]) % NF
    moved = shifts[None, :].astype(jnp.float32)
    dist_z = moved - offsets[0][:, None]
    dist_y = moved - offsets[1][:, None]
    dist_x = moved - offsets[2][:, None]
    squared = dist_z[:, :, None, None] ** 2 + dist_y[:, None, :, None] ** 2 + dist_x[:, None, None, :] ** 2
    values = shape_value(squared, charge, exponent)
    density = jnp.zeros((NF, NF, NF), jnp.float32)
    return density.at[index_z[:, :, None, None], index_y[:, None, :, None], index_x[:, None, None, :]].add(values)


def poisson_weight():
    wave = signed(jnp.arange(NF, dtype=jnp.int32), NF)
    squares = wave[:, None, None] * wave[:, None, None] + wave[None, :, None] * wave[None, :, None] + wave[None, None, :] * wave[None, None, :]
    scaled = (2.0 * jnp.pi / NF) ** 2 * jnp.maximum(squares, 1).astype(jnp.float32)
    return jnp.where(squares > 0, 4.0 * jnp.pi / scaled, 0.0).astype(jnp.float32)


def reference(coarse_density, density_in, history, atom_cell, atom_offset, atom_charge, atom_width):
    density_cube = density_in.reshape(NF, NF, NF)
    history_cube = history.reshape(HIST, NF, NF, NF)
    smooth = coarse_density
    for dimension in (2, 1, 0):
        smooth = midpoint(periodic(smooth, dimension), dimension, smooth.shape[dimension])
    residual = smooth + compensation(atom_cell, atom_offset, atom_charge, atom_width) - density_cube
    spectrum = jnp.fft.fftn(residual)
    potential = jnp.real(jnp.fft.ifftn(spectrum * poisson_weight())).astype(jnp.float32)
    cells_all = float(NF) ** 3
    intersections = jnp.concatenate([jnp.sum(history_cube * potential[None], axis=(1, 2, 3)), jnp.sum(residual * potential)[None]]) / cells_all
    return residual.reshape(NF, NF * NF), potential.reshape(NF, NF * NF), intersections
```

```python
import math

import jax
import jax.numpy as jnp
import numpy as np
from jax import lax
from jax.experimental import pallas as pl
from jax.experimental.pallas import tpu as pltpu
from jax.sharding import PartitionSpec as P

RC = 4
NF = 192


def with_halo(block, sides, width):
    for axis, dim in sides:
        count = lax.axis_size(axis)
        forward = [(i, i + 1) for i in range(count - 1)]
        forward.append((count - 1, 0))
        backward = [(target, source) for source, target in forward]
        low = lax.ppermute(
            lax.slice_in_dim(block, block.shape[dim] - width, None, axis=dim), axis, forward
        )
        high = lax.ppermute(lax.slice_in_dim(block, 0, width, axis=dim), axis, backward)
        block = jnp.concatenate([low, block, high], axis=dim)
    return block


def midpoint(extended, dimension, cells_in):

    def window(offset):
        return lax.slice_in_dim(extended, offset, offset + cells_in, axis=dimension)

    even_cells = window(2)
    odd_cells = (9.0 * (window(2) + window(3)) - window(1) - window(4)) / 16.0
    merged = jnp.stack([even_cells, odd_cells], dimension + 1)
    new_shape = list(even_cells.shape)
    new_shape[dimension] = 2 * cells_in
    return merged.reshape(new_shape)


def signed(counter, length):
    return jnp.where(counter < length // 2, counter, counter - length)


def shape_value(squared, charge, exponent):
    factor = charge * (exponent / jnp.pi) ** 1.5
    return factor * jnp.maximum(
        jnp.exp(-exponent * squared) - jnp.exp(-exponent * float(RC * RC)), 0.0
    )


def gaussians(dist_z, dist_y, dist_x, charge, exponent):
    squared = (
        dist_z[:, :, None, None] ** 2
        + dist_y[:, None, :, None] ** 2
        + dist_x[:, None, None, :] ** 2
    )
    return jnp.sum(
        shape_value(squared, charge[:, None, None, None], exponent[:, None, None, None]), 0
    )


def tables(length):
    counter = jnp.arange(length, dtype=jnp.int32)
    phase = counter[:, None] * counter[None, :] % length
    angle = 2.0 * jnp.pi / length * phase.astype(jnp.float32)
    return (jnp.cos(angle), jnp.sin(angle))


def contract(values, table, dimension):
    product = jnp.tensordot(values, table, axes=([dimension], [0]), precision=lax.Precision.HIGHEST)
    return jnp.moveaxis(product, -1, dimension)


def transform(spectra, dimension, direction):
    cosine, sine_table = tables(spectra.shape[dimension])
    inner_dim = dimension - 1
    real_part = spectra[:, 0]
    imag_part = spectra[:, 1]
    new_real = contract(real_part, cosine, inner_dim) - direction * contract(
        imag_part, sine_table, inner_dim
    )
    new_imag = contract(imag_part, cosine, inner_dim) + direction * contract(
        real_part, sine_table, inner_dim
    )
    result = jnp.stack([new_real, new_imag], 1)
    if direction > 0:
        result = result / spectra.shape[dimension]
    return result


def transform_y(pieces):
    return transform(pieces, 3, -1.0)


def transform_z(pieces):
    return transform(pieces, 2, -1.0)


def inverse_y(pieces):
    return transform(pieces, 3, 1.0)


def inverse_x_real(pieces):
    cosine, sine_table = tables(pieces.shape[4])
    real_part = contract(pieces[:, 0], cosine, 3) - contract(pieces[:, 1], sine_table, 3)
    return real_part / pieces.shape[4]


def forward(fields):
    cosine, sine_table = tables(fields.shape[3])
    spectra = jnp.stack([contract(fields, cosine, 3), -contract(fields, sine_table, 3)], 1)
    columns = transform_y(lax.all_to_all(spectra, "gy", split_axis=4, concat_axis=3, tiled=True))
    return transform_z(lax.all_to_all(columns, "gz", split_axis=3, concat_axis=2, tiled=True))


def inverse(spectra):
    local_z = transform(spectra, 2, 1.0)
    rows_back = inverse_y(lax.all_to_all(local_z, "gz", split_axis=2, concat_axis=3, tiled=True))
    return inverse_x_real(lax.all_to_all(rows_back, "gy", split_axis=3, concat_axis=4, tiled=True))


def poisson_weight(spectra):
    length = spectra.shape[2]
    y_block = spectra.shape[3]
    x_block = spectra.shape[4]
    wave_z = signed(jnp.arange(length, dtype=jnp.int32), length)
    wave_y = signed(lax.axis_index("gz") * y_block + jnp.arange(y_block, dtype=jnp.int32), length)
    wave_x = signed(lax.axis_index("gy") * x_block + jnp.arange(x_block, dtype=jnp.int32), length)
    squares = (
        wave_z[:, None, None] * wave_z[:, None, None]
        + wave_y[None, :, None] * wave_y[None, :, None]
        + wave_x[None, None, :] * wave_x[None, None, :]
    )
    scaled = (2.0 * jnp.pi / length) ** 2 * jnp.maximum(squares, 1).astype(jnp.float32)
    return jnp.where(squares > 0, 4.0 * jnp.pi / scaled, 0.0)


def total_intersections(own_terms):
    return lax.psum(own_terms, ("gz", "gy"))


def deposit_rims(atom_cell, atom_offset, atom_charge, atom_width, slab_z, slab_y, length):
    cell_ids = atom_cell.reshape(-1)
    local_z = cell_ids // (slab_y * length)
    local_y = cell_ids // length % slab_y
    local_x = cell_ids % length
    offsets = atom_offset.reshape(3, -1)
    dist_z = (jnp.arange(slab_z + 2 * RC, dtype=jnp.int32)[None, :] - RC - local_z[:, None]).astype(
        jnp.float32
    ) - offsets[0][:, None]
    dist_y = (jnp.arange(slab_y + 2 * RC, dtype=jnp.int32)[None, :] - RC - local_y[:, None]).astype(
        jnp.float32
    ) - offsets[1][:, None]
    dist_x = (
        signed(
            (jnp.arange(length, dtype=jnp.int32)[None, :] - local_x[:, None]) % length, length
        ).astype(jnp.float32)
        - offsets[2][:, None]
    )
    buffer_sum = gaussians(dist_z, dist_y, dist_x, atom_charge.reshape(-1), atom_width.reshape(-1))
    rims_z = jnp.concatenate([buffer_sum[:RC], buffer_sum[-RC:]], 0)
    near_z = with_halo(rims_z, (("gz", 0),), RC)
    middle = buffer_sum[RC : RC + slab_z]
    middle = middle.at[:RC].add(near_z[:RC]).at[slab_z - RC :].add(near_z[3 * RC :])
    rims_y = jnp.concatenate([middle[:, :RC], middle[:, -RC:]], 1)
    near_y = with_halo(rims_y, (("gy", 1),), RC)
    inside = middle[:, RC : RC + slab_y]
    return inside.at[:, :RC].add(near_y[:, :RC]).at[:, slab_y - RC :].add(near_y[:, 3 * RC :])


def local(coarse_density, density_in, history, atom_cell, atom_offset, atom_charge, atom_width):
    length = NF
    slab_z = density_in.shape[0]
    slab_y = density_in.shape[1] // length
    density_cube = density_in.reshape(slab_z, slab_y, length)
    history_cube = history.reshape(history.shape[0], slab_z, slab_y, length)
    extended = with_halo(coarse_density, (("gy", 1),), 2)
    coarse_rows = coarse_density.shape[0] // lax.axis_size("gz")
    beside_all = jnp.concatenate([extended[-2:], extended, extended[:2]], 0)
    start = lax.axis_index("gz") * coarse_rows
    own_planes = lax.dynamic_slice_in_dim(beside_all, start, coarse_rows + 4, 0)
    wrapped = jnp.concatenate([own_planes[:, :, -2:], own_planes, own_planes[:, :, :2]], 2)
    smooth = midpoint(wrapped, 2, coarse_density.shape[2])
    smooth = midpoint(smooth, 1, coarse_density.shape[1])
    smooth = midpoint(smooth, 0, coarse_rows)
    charge_field = deposit_rims(
        atom_cell, atom_offset, atom_charge, atom_width, slab_z, slab_y, length
    )
    residual = smooth + charge_field - density_cube
    cells_all = float(length) ** 3
    spectra = forward(residual[None])
    weight = poisson_weight(spectra)
    potential = inverse(weight * spectra)[0]
    own_terms = (
        jnp.concatenate(
            [
                jnp.sum(history_cube * potential[None], axis=(1, 2, 3)),
                jnp.sum(residual * potential)[None],
            ]
        )
        / cells_all
    )
    intersections = total_intersections(own_terms)
    return (
        residual.reshape(slab_z, slab_y * length),
        potential.reshape(slab_z, slab_y * length),
        intersections,
    )


GROUP = 16
LANES = 128
SUB = 8


def basis(length):
    half = length // 2
    wave = np.concatenate([np.arange(half + 1), np.arange(1, half)])
    angle = 2.0 * np.pi / length * (np.outer(wave, np.arange(length)) % length)
    rows = np.where(np.arange(length)[:, None] <= half, np.cos(angle), np.sin(angle))
    scale = np.where((wave == 0) | (wave == half), 1.0, np.sqrt(2.0)) / np.sqrt(length)
    return rows * scale[:, None], wave


def split_table(table):
    table = np.asarray(table, np.float32)
    high = table.astype(jnp.bfloat16)
    low = (table - high.astype(np.float32)).astype(jnp.bfloat16)
    return jnp.asarray(np.stack([high, low]))


def halves(values):
    high = values.astype(jnp.bfloat16)
    return high, (values - high.astype(jnp.float32)).astype(jnp.bfloat16)


def thirds(values):
    high = values.astype(jnp.bfloat16)
    rest = values - high.astype(jnp.float32)
    middle = rest.astype(jnp.bfloat16)
    return high, middle, (rest - middle.astype(jnp.float32)).astype(jnp.bfloat16)


NN = (((1,), (0,)), ((), ()))
NT = (((1,), (1,)), ((), ()))


def mm(left, right, dims):
    return lax.dot_general(left, right, dims, preferred_element_type=jnp.float32)


def mm3(left, right, dims=NN):
    return (
        mm(left[0], right[1], dims) + mm(left[1], right[0], dims) + mm(left[0], right[0], dims)
    )


def tile_masks():
    row = lax.broadcasted_iota(jnp.int32, (SUB, LANES), 0)
    group = lax.broadcasted_iota(jnp.int32, (SUB, LANES), 1) // SUB
    return row, group


def rotate_up(upper, lower, masks):
    row, group = masks
    bit = (group & 8) != 0
    upper, lower = jnp.where(bit, lower, upper), jnp.where(bit, upper, lower)
    for shift in (4, 2, 1):
        bit = (group & shift) != 0
        roll_u = pltpu.roll(upper, SUB - shift, 0)
        roll_l = pltpu.roll(lower, SUB - shift, 0)
        stay = row < SUB - shift
        new_u = jnp.where(stay, roll_u, roll_l)
        new_l = jnp.where(stay, roll_l, roll_u)
        upper, lower = jnp.where(bit, new_u, upper), jnp.where(bit, new_l, lower)
    return upper, lower


def skew(values, start):
    return pltpu.roll(values, start, 1, stride=SUB, stride_axis=0)


def block_turn(upper, lower, masks):
    upper, lower = rotate_up(skew(upper, 0), skew(lower, 64), masks)
    return skew(upper, 0), skew(lower, 64)


class Plan:
    def __init__(self, mesh_shape, length, coarse, fz, fy):
        self.nz, self.ny = mesh_shape
        self.count = self.nz * self.ny
        self.length, self.coarse, self.fz, self.fy = length, coarse, fz, fy
        self.j = length // self.count
        self.zo, self.yo = fz // SUB, fy // GROUP
        self.main = self.j * self.zo * self.yo
        self.tail = self.main + self.j
        self.rows_out = self.tail + 4
        self.rows_back = -(-self.main // SUB) * SUB
        self.ext = length + 24

    def ok(self):
        return (
            (self.nz, self.ny, self.zo, self.yo, self.j) == (8, 4, 3, 3, 6)
            and self.fz % SUB == 0
            and self.fy % GROUP == 0
            and self.length == self.coarse * 2
            and self.rows_out % SUB == 0
        )


def ext_slot(edge, zo):
    return ((15, 3, 1)[edge] + 5 * zo) % GROUP


def fast_tables(plan):
    length, nz = plan.length, plan.nz
    rows, wave = basis(length)
    fine_of = np.zeros((plan.coarse, length), np.float32)
    for i in range(plan.coarse):
        fine_of[i, 2 * i] += 1.0
        for step, value in ((0, 9), (1, 9), (-1, -1), (2, -1)):
            fine_of[(i + step) % plan.coarse, 2 * i + 1] += value / 16.0
    local_z = np.zeros((plan.fz, GROUP), np.float32)
    for i in range(plan.fz // 2):
        local_z[2 * i, i + 1] = 1.0
        for step, value in ((1, 9), (2, 9), (0, -1), (3, -1)):
            local_z[2 * i + 1, i + step] += value / 16.0

    def along_z(turn):
        half_of, owner = turn // SUB, turn % SUB
        lane = np.arange(SUB)
        z_main = (owner[:, None] * plan.fz + half_of[:, None] * SUB + lane[None]).reshape(-1)
        z_shared = (owner[:, None] * plan.fz + 2 * SUB + lane[None]).reshape(-1)
        odd = np.repeat(half_of, SUB)
        tables_z = []
        for parity in (0, 1):
            table = np.zeros((2 * LANES, length))
            table[:LANES] = rows[:, z_main].T
            table[LANES:] = np.where((odd == parity)[:, None], rows[:, z_shared].T, 0.0)
            tables_z.append(table)
        return tables_z, (z_main, z_shared, odd)

    z_tables, z_lanes = along_z(np.arange(GROUP))
    z_back = along_z((-np.arange(GROUP)) % GROUP)[0]
    y_of_row = (np.arange(plan.ext) - SUB) % length
    lanes = np.zeros((SUB, LANES), np.float32)
    lanes[0], lanes[1], lanes[2] = z_lanes
    squares = (wave.astype(np.float64) ** 2).astype(np.float32)
    x_window = np.zeros((plan.count, length + GROUP, SUB), np.float32)
    x_of_row = (np.arange(length + GROUP) - SUB) % length
    for d in range(plan.count):
        for j in range(plan.j):
            x_window[d, :, j] = rows[j * plan.count + d, x_of_row]
    return {
        "x": split_table(rows),
        "fine": jnp.asarray(fine_of, jnp.bfloat16),
        "kron": jnp.asarray(np.kron(np.eye(SUB), local_z), jnp.bfloat16),
        "z": split_table(np.stack(z_tables)),
        "zt": split_table(np.stack([t.T for t in z_back])),
        "y": split_table(rows[:, y_of_row]),
        "yt": split_table(rows.T),
        "lanes": jnp.asarray(lanes),
        "wave": jnp.asarray(np.stack([np.broadcast_to(squares, (SUB, length))])),
        "wave_c": jnp.asarray(np.broadcast_to(squares[:, None], (length, LANES))),
        "window": jnp.asarray(x_window.reshape(plan.count, -1)),
    }


def part_a(plan):
    length, fz, fy, count = plan.length, plan.fz, plan.fy, plan.count
    rows_c = fy // 2
    per = plan.rows_out

    def kernel(cell, offset, charge, width, coarse, density, fine, kron, xt, send, partial, planes, smooth, field):
        a = lax.axis_index("gz")
        b = lax.axis_index("gy")
        own = plan.coarse // plan.nz
        for t in range(GROUP):
            planes[pl.ds(t * rows_c, rows_c), :] = coarse[lax.rem(own * a + plan.coarse - 1 + t, plan.coarse)]
        for part in range(rows_c // SUB):
            block = jnp.concatenate(
                [planes[pl.ds(part * SUB + y, GROUP, stride=rows_c), :] for y in range(SUB)], 0
            )
            wide = sum(mm(piece, fine[...], NN) for piece in thirds(block)[::-1])
            tall = sum(mm(kron[...], piece, NN) for piece in thirds(wide)[::-1])
            for y in range(SUB):
                smooth[part * SUB + y] = tall[y * fz : (y + 1) * fz]

        def row(i):
            return smooth[i] if 0 <= i < rows_c else jnp.zeros((fz, length), jnp.float32)

        for i in range(rows_c):
            odd_row = (9.0 * (row(i) + row(i + 1)) - row(i - 1) - row(i + 2)) * (1.0 / 16.0)
            old = density[:, 2 * i * length : (2 * i + 2) * length]
            even_out = smooth[i] - old[:, :length]
            odd_out = odd_row - old[:, length:]
            field[2 * i] = even_out
            field[2 * i + 1] = odd_out
            partial[:, 2 * i * length : (2 * i + 2) * length] = jnp.concatenate([even_out, odd_out], 1)
        edges = (
            row(rows_c - 1) * (-1.0 / 16.0),
            row(0) * (-1.0 / 16.0),
            (9.0 * row(0) - row(1)) * (1.0 / 16.0),
        )
        table = (xt[0], xt[1])

        def emit(block, first_row):
            high, low = halves(block)
            out = mm3(table, (high, low), NT)
            for j in range(plan.j):
                for g in range(out.shape[1] // LANES):
                    send[pl.ds(first_row(g) + j, count, stride=per), :] = out[
                        j * count : (j + 1) * count, g * LANES : (g + 1) * LANES
                    ]

        for yo in range(plan.yo):
            block = jnp.concatenate(
                [
                    field[yo * GROUP + (-g) % GROUP, zo * SUB : (zo + 1) * SUB, :]
                    for zo in range(plan.zo)
                    for g in range(GROUP)
                ],
                0,
            )
            emit(block, lambda g, yo=yo: (yo * plan.zo + g) * plan.j)
        slots = [jnp.zeros((SUB, length), jnp.float32)] * GROUP
        for zo in range(plan.zo):
            for edge in range(3):
                slots[ext_slot(edge, zo)] = edges[edge][zo * SUB : (zo + 1) * SUB]
        emit(jnp.concatenate(slots, 0), lambda g: plan.main)
        number = cell[0, 0]
        plane = fy * length
        facts = (
            (a * fz + number // plane).astype(jnp.float32),
            (b * fy + lax.rem(number // length, fy)).astype(jnp.float32),
            lax.rem(number, length).astype(jnp.float32),
            offset[0, 0],
            offset[1, 0],
            offset[2, 0],
            charge[0, 0],
            width[0, 0],
        )
        lane = lax.broadcasted_iota(jnp.int32, (1, LANES), 1)
        atom = jnp.zeros((1, LANES), jnp.float32)
        for i, fact in enumerate(facts):
            atom = jnp.where(lane == i, fact, atom)
        send[pl.ds(plan.tail, count, stride=per), :] = jnp.broadcast_to(atom, (count, LANES))
        pad = jnp.zeros((1, LANES - plan.coarse), jnp.float32)
        ahead = lax.rem(b + 1, plan.ny)
        behind = lax.rem(b + plan.ny - 1, plan.ny)
        for dest in range(plan.nz):
            for zz in range(2):
                p = lax.rem(own * dest + plan.coarse - 1 + 2 * a + zz, plan.coarse)
                for edge, target, slot in ((rows_c - 1, ahead, 0), (0, behind, 0), (1, behind, 2)):
                    line = jnp.concatenate([pad, coarse[p, edge : edge + 1, :]], 1)
                    index = slot + zz
                    if index == 0:
                        line = jnp.where(lane < SUB, atom, line)
                    send[pl.ds((dest * plan.ny + target) * per + plan.tail + index, 1), :] = line

    smem = pl.BlockSpec(memory_space=pltpu.SMEM)
    vmem = pl.BlockSpec(memory_space=pltpu.VMEM)
    return pl.pallas_call(
        kernel,
        name="spread",
        in_specs=[smem] * 4 + [vmem] * 5,
        out_specs=[vmem, vmem],
        out_shape=[
            jax.ShapeDtypeStruct((count * per, LANES), jnp.float32),
            jax.ShapeDtypeStruct((fz, fy * length), jnp.float32),
        ],
        scratch_shapes=[
            pltpu.VMEM((GROUP * rows_c, plan.coarse), jnp.float32),
            pltpu.VMEM((rows_c, fz, length), jnp.float32),
            pltpu.VMEM((fy, fz, length), jnp.float32),
        ],
        cost_estimate=pl.CostEstimate(flops=500_000_000, bytes_accessed=4_000_000, transcendentals=0),
    )


def wrapped(distance, length):
    half = length // 2
    distance = jnp.where(distance >= half, distance - length, distance)
    return jnp.where(distance < -half, distance + length, distance)


def part_b(plan):
    length, count, ext = plan.length, plan.count, plan.ext
    per, per_back = plan.rows_out, plan.rows_back

    def kernel(window, recv, zt, zti, yt, yti, lanes, wave, wave_c, send, main, shared, atoms_v, atoms, sem):
        device = lax.axis_index("gz") * plan.ny + lax.axis_index("gy")
        atoms_v[...] = recv[pl.ds(plan.tail, count, stride=per), :]
        copy = pltpu.make_async_copy(atoms_v, atoms, sem)
        copy.start()
        masks = tile_masks()
        group = masks[1]
        for j in range(plan.j):
            main[j, :SUB, :] = jnp.zeros((SUB, LANES), jnp.float32)
            main[j, SUB + length :, :] = jnp.zeros((ext - SUB - length, LANES), jnp.float32)
        for jp in range(plan.j // 2):
            shared[jp, :SUB, :] = jnp.zeros((SUB, LANES), jnp.float32)
            shared[jp, SUB + length :, :] = jnp.zeros((ext - SUB - length, LANES), jnp.float32)
        stride = plan.ny * per

        def gather(step, carry):
            jp = step // plan.ny
            b = lax.rem(step, plan.ny)
            edge_ahead = lax.rem(b + 1, plan.ny) * per
            edge_behind = lax.rem(b + plan.ny - 1, plan.ny) * per
            edges = []
            for source in (edge_behind, edge_ahead):
                edges.append(
                    [recv[pl.ds(source + plan.main + 2 * jp + k, SUB, stride=stride), :] for k in (0, 1)]
                )
            for yo in range(plan.yo):
                tiles = []
                for k in (0, 1):
                    for zo in range(plan.zo):
                        start = b * per + (yo * plan.zo + zo) * plan.j + 2 * jp + k
                        tile = recv[pl.ds(start, SUB, stride=stride), :]
                        shift = (LANES - 5 * zo * SUB) % LANES
                        if yo == 0:
                            extra = pltpu.roll(edges[0][k], shift, 1) if shift else edges[0][k]
                            tile = jnp.where(group == 15, tile + extra, tile)
                        if yo == plan.yo - 1:
                            extra = pltpu.roll(edges[1][k], shift, 1) if shift else edges[1][k]
                            tile = jnp.where((group == 3) | (group == 1), tile + extra, tile)
                        tiles.append(tile)
                at = pl.multiple_of(SUB + b * plan.fy + yo * GROUP, SUB)
                for k in (0, 1):
                    upper, lower = block_turn(tiles[3 * k], tiles[3 * k + 1], masks)
                    main[2 * jp + k, pl.ds(at, SUB), :] = upper
                    main[2 * jp + k, pl.ds(at + SUB, SUB), :] = lower
                upper, lower = block_turn(tiles[2], tiles[5], masks)
                shared[jp, pl.ds(at, SUB), :] = upper
                shared[jp, pl.ds(at + SUB, SUB), :] = lower
            return carry

        lax.fori_loop(0, plan.ny * (plan.j // 2), gather, 0)
        copy.wait()
        z_main, z_shared = lanes[0:1, :], lanes[1:2, :]
        odd = lanes[2:3, :] > 0.5
        window_rows = lax.broadcasted_iota(jnp.int32, (GROUP, LANES), 0).astype(jnp.float32) - RC

        def deposit(i, carry):
            z0, y0, x0 = atoms[i, 0], atoms[i, 1], atoms[i, 2]
            off_z, off_y, off_x = atoms[i, 3], atoms[i, 4], atoms[i, 5]
            charge, width = atoms[i, 6], atoms[i, 7]
            ratio = jnp.full((SUB, LANES), width / jnp.pi, jnp.float32)
            factor = ratio * jnp.sqrt(ratio) * charge
            factor = factor[0:1]
            cut = jnp.exp(jnp.full((SUB, LANES), -width * float(RC * RC), jnp.float32))[0:1]
            profile_y = jnp.exp(-width * (window_rows - off_y) ** 2)
            profile_x = jnp.exp(-width * (window_rows - off_x) ** 2)
            planes = []
            for z in (z_main, z_shared):
                profile_z = jnp.exp(-width * (wrapped(z - z0, length) - off_z) ** 2)
                planes.append(profile_y * profile_z)
            base = (x0.astype(jnp.int32) - RC + SUB) * SUB
            zero = jnp.zeros((GROUP, LANES), jnp.float32)
            sums = [[zero, zero, zero] for _ in range(plan.j // 2)]
            for dx in range(2 * RC + 2):
                line = profile_x[dx : dx + 1]
                bell = [jnp.maximum(plane * line - cut, 0.0) for plane in planes]
                for jp in range(plan.j // 2):
                    even = window[0, base + dx * SUB + 2 * jp]
                    odd_value = window[0, base + dx * SUB + 2 * jp + 1]
                    sums[jp][0] += bell[0] * even
                    sums[jp][1] += bell[0] * odd_value
                    sums[jp][2] += bell[1] * jnp.where(odd, odd_value, even)
            at = y0.astype(jnp.int32) - RC + SUB
            for jp in range(plan.j // 2):
                for k in (0, 1):
                    main[2 * jp + k, pl.ds(at, GROUP), :] += sums[jp][k] * factor
                shared[jp, pl.ds(at, GROUP), :] += sums[jp][2] * factor
            return carry

        lax.fori_loop(0, count, deposit, 0)
        scale = float(length) ** 2 / math.pi
        wave_y = wave_c[...][:, 0:1]
        wave_z = wave[0, 0:1, :]
        for jp in range(plan.j // 2):
            shared_back = None
            for k in (0, 1):
                j = 2 * jp + k
                left = halves(jnp.concatenate([main[j], shared[jp]], 1))
                rows_z = halves(mm3(left, (zt[0, k], zt[1, k])))
                full = mm3((yt[0], yt[1]), rows_z)
                p = j * count + device
                wave_x = jnp.where(p <= length // 2, p, p - length // 2).astype(jnp.float32)
                squares = wave_y + (wave_z + wave_x * wave_x)
                weight = jnp.where(squares > 0.0, scale / jnp.maximum(squares, 1.0), 0.0)
                weighted = halves(full * weight)
                rows_y = halves(mm3((yti[0], yti[1]), weighted))
                back = mm3(rows_y, (zti[0, k], zti[1, k]))
                main[j, SUB : SUB + length, :] = back[:, :LANES]
                part = back[:, LANES:]
                shared_back = part if shared_back is None else shared_back + part
            shared[jp, SUB : SUB + length, :] = shared_back
        stride_back = plan.ny * per_back

        def scatter(step, carry):
            jp = step // plan.ny
            b = lax.rem(step, plan.ny)
            for yo in range(plan.yo):
                at = pl.multiple_of(SUB + b * plan.fy + yo * GROUP, SUB)
                tiles = []
                for k in (0, 1):
                    tiles.append(
                        block_turn(
                            main[2 * jp + k, pl.ds(at, SUB), :],
                            main[2 * jp + k, pl.ds(at + SUB, SUB), :],
                            masks,
                        )
                    )
                both = block_turn(
                    shared[jp, pl.ds(at, SUB), :], shared[jp, pl.ds(at + SUB, SUB), :], masks
                )
                for k in (0, 1):
                    for zo, tile in enumerate((tiles[k][0], tiles[k][1], both[k])):
                        start = b * per_back + (yo * plan.zo + zo) * plan.j + 2 * jp + k
                        send[pl.ds(start, SUB, stride=stride_back), :] = tile
            return carry

        lax.fori_loop(0, plan.ny * (plan.j // 2), scatter, 0)

    smem = pl.BlockSpec(memory_space=pltpu.SMEM)
    vmem = pl.BlockSpec(memory_space=pltpu.VMEM)
    return pl.pallas_call(
        kernel,
        name="solve",
        in_specs=[smem] + [vmem] * 8,
        out_specs=vmem,
        out_shape=jax.ShapeDtypeStruct((count * per_back, LANES), jnp.float32),
        scratch_shapes=[
            pltpu.VMEM((plan.j, ext, LANES), jnp.float32),
            pltpu.VMEM((plan.j // 2, ext, LANES), jnp.float32),
            pltpu.VMEM((count, LANES), jnp.float32),
            pltpu.SMEM((count, LANES), jnp.float32),
            pltpu.SemaphoreType.DMA,
        ],
        cost_estimate=pl.CostEstimate(flops=2_000_000_000, bytes_accessed=4_000_000, transcendentals=0),
    )


def part_r(plan):
    length, fz, fy, count = plan.length, plan.fz, plan.fy, plan.count
    per = plan.rows_out

    def kernel(recv, partial, fine, kron, out, field, lines, atoms_v, atoms, sem):
        a = lax.axis_index("gz")
        b = lax.axis_index("gy")
        atoms_v[...] = recv[pl.ds(plan.tail, count, stride=per), :]
        copy = pltpu.make_async_copy(atoms_v, atoms, sem)
        copy.start()
        ahead = lax.rem(b + 1, plan.ny)
        behind = lax.rem(b + plan.ny - 1, plan.ny)
        lines[...] = jnp.zeros_like(lines)
        for source in range(plan.nz):
            for zz in range(2):
                for slot, (origin, index) in enumerate(((behind, 0), (ahead, 0), (ahead, 2))):
                    at = (source * plan.ny + origin) * per + plan.tail + index + zz
                    lines[pl.ds(slot * GROUP + 2 * source + zz, 1), :] = recv[pl.ds(at, 1), :]
        block = lines[...][:, LANES - plan.coarse :]
        wide = sum(mm(piece, fine[...], NN) for piece in thirds(block)[::-1])
        tall = sum(mm(kron[...], piece, NN) for piece in thirds(wide)[::-1])
        below, above, above2 = (tall[i * fz : (i + 1) * fz] for i in range(3))
        field[...] = jnp.zeros_like(field)
        field[1] = below * (-1.0 / 16.0)
        field[fy - 3] = above * (-1.0 / 16.0)
        field[fy - 1] = (9.0 * above - above2) * (1.0 / 16.0)
        copy.wait()
        z_here = lax.broadcasted_iota(jnp.int32, (fz, length), 0).astype(jnp.float32)
        x_here = lax.broadcasted_iota(jnp.int32, (fz, length), 1).astype(jnp.float32)

        def deposit(i, carry):
            z0 = wrapped(atoms[i, 0] - (a * fz).astype(jnp.float32), length)
            y0 = wrapped(atoms[i, 1] - (b * fy).astype(jnp.float32), length).astype(jnp.int32)
            first = jnp.maximum(y0 - RC, 0)
            last = jnp.minimum(y0 + RC + 2, fy)
            near_z = (z0 > -RC - 2.0) & (z0 < fz + RC + 1.0)

            @pl.when(near_z & (first < last))
            def _():
                off_z, off_y, off_x = atoms[i, 3], atoms[i, 4], atoms[i, 5]
                charge, width = atoms[i, 6], atoms[i, 7]
                ratio = jnp.full((fz, length), width / jnp.pi, jnp.float32)
                factor = ratio * jnp.sqrt(ratio) * charge
                cut = jnp.exp(jnp.full((fz, length), -width * float(RC * RC), jnp.float32))
                dist_z = z_here - z0 - off_z
                dist_x = wrapped(x_here - atoms[i, 2], length) - off_x
                flat = dist_z * dist_z + dist_x * dist_x

                def row(y, inner):
                    dist_y = (y - y0).astype(jnp.float32) - off_y
                    bell = jnp.maximum(jnp.exp(-width * (flat + dist_y * dist_y)) - cut, 0.0)
                    field[y] += bell * factor
                    return inner

                lax.fori_loop(first, last, row, 0)

            return carry

        lax.fori_loop(0, count, deposit, 0)
        for i in range(fy // 2):
            span = slice(2 * i * length, (2 * i + 2) * length)
            out[:, span] = partial[:, span] + jnp.concatenate([field[2 * i], field[2 * i + 1]], 1)

    vmem = pl.BlockSpec(memory_space=pltpu.VMEM)
    return pl.pallas_call(
        kernel,
        name="finish",
        in_specs=[vmem] * 4,
        out_specs=vmem,
        out_shape=jax.ShapeDtypeStruct((fz, fy * length), jnp.float32),
        scratch_shapes=[
            pltpu.VMEM((fy, fz, length), jnp.float32),
            pltpu.VMEM((SUB * GROUP, LANES), jnp.float32),
            pltpu.VMEM((count, LANES), jnp.float32),
            pltpu.SMEM((count, LANES), jnp.float32),
            pltpu.SemaphoreType.DMA,
        ],
        cost_estimate=pl.CostEstimate(flops=3_000_000_000, bytes_accessed=4_000_000, transcendentals=0),
    )


def part_c(plan, terms):
    length, fz, fy, count = plan.length, plan.fz, plan.fy, plan.count
    per = plan.rows_back
    span = GROUP * length

    def kernel(recv, xt, history, residual, potential, sums, acc):
        step = pl.program_id(0)
        pieces = []
        for zo in range(plan.zo):
            spectrum = jnp.concatenate(
                [
                    recv[pl.ds((step * plan.zo + zo) * plan.j + j, count, stride=per), :]
                    for j in range(plan.j)
                ],
                0,
            )
            pieces.append(spectrum.T)
        values = mm3(halves(jnp.concatenate(pieces, 0)), (xt[0], xt[1]))
        for pair in range(GROUP // 2):
            for zo in range(plan.zo):
                at = zo * LANES + 2 * pair * SUB
                potential[zo * SUB : (zo + 1) * SUB, 2 * pair * length : (2 * pair + 2) * length] = (
                    jnp.concatenate([values[at : at + SUB], values[at + SUB : at + 2 * SUB]], 1)
                )

        @pl.when(step == 0)
        def _():
            acc[...] = jnp.zeros_like(acc)

        wide = 3 * LANES
        for i in range(terms + 1):
            total = jnp.zeros((fz, wide), jnp.float32)
            for c in range(span // wide):
                cut = slice(c * wide, (c + 1) * wide)
                other = history[i, :, cut] if i < terms else residual[:, cut]
                total += other * potential[:, cut]
            acc[i * SUB : (i + 1) * SUB, :] += sum(
                total[r * SUB : (r + 1) * SUB, q * LANES : (q + 1) * LANES]
                for r in range(plan.zo)
                for q in range(3)
            )

        @pl.when(step == pl.num_programs(0) - 1)
        def _():
            lane = lax.broadcasted_iota(jnp.int32, (1, LANES), 1)
            line = jnp.zeros((1, LANES), jnp.float32)
            for i in range(terms + 1):
                line = jnp.where(lane == i, jnp.sum(acc[i * SUB : (i + 1) * SUB, :]), line)
            sums[...] = jnp.broadcast_to(line * (1.0 / float(length) ** 3), (count, LANES))

    return pl.pallas_call(
        kernel,
        name="finish_potential",
        grid=(plan.yo,),
        in_specs=[
            pl.BlockSpec((count * per, LANES), lambda s: (0, 0)),
            pl.BlockSpec((2, length, length), lambda s: (0, 0, 0)),
            pl.BlockSpec((terms, fz, span), lambda s: (0, 0, s)),
            pl.BlockSpec((fz, span), lambda s: (0, s)),
        ],
        out_specs=[
            pl.BlockSpec((fz, span), lambda s: (0, s)),
            pl.BlockSpec((count, LANES), lambda s: (0, 0)),
        ],
        out_shape=[
            jax.ShapeDtypeStruct((fz, fy * length), jnp.float32),
            jax.ShapeDtypeStruct((count, LANES), jnp.float32),
        ],
        scratch_shapes=[pltpu.VMEM(((terms + 1) * SUB, LANES), jnp.float32)],
        compiler_params=pltpu.CompilerParams(dimension_semantics=("arbitrary",)),
        cost_estimate=pl.CostEstimate(flops=500_000_000, bytes_accessed=10_000_000, transcendentals=0),
    )


def exchange(sent, count, axes):
    blocks = sent.reshape(count, sent.shape[0] // count, LANES)
    return lax.all_to_all(blocks, axes, 0, 0, tiled=True).reshape(sent.shape)


def local_fast(plan, coarse_density, density_in, history, atom_cell, atom_offset, atom_charge, atom_width):
    axes = ("gz", "gy")
    count = plan.count
    tables_ = fast_tables(plan)
    sent, partial = part_a(plan)(
        atom_cell.reshape(1, 1),
        atom_offset.reshape(3, 1),
        atom_charge.reshape(1, 1),
        atom_width.reshape(1, 1),
        coarse_density,
        density_in,
        tables_["fine"],
        tables_["kron"],
        tables_["x"],
    )
    spectra = exchange(sent, count, axes)
    device = lax.axis_index("gz") * plan.ny + lax.axis_index("gy")
    window = lax.dynamic_slice_in_dim(tables_["window"], device, 1, 0)
    solved = part_b(plan)(
        window,
        spectra,
        tables_["z"],
        tables_["zt"],
        tables_["y"],
        tables_["yt"],
        tables_["lanes"],
        tables_["wave"],
        tables_["wave_c"],
    )
    back = exchange(solved, count, axes)
    residual = part_r(plan)(spectra, partial, tables_["fine"], tables_["kron"])
    potential, sums = part_c(plan, history.shape[0])(back, tables_["x"], history, residual)
    rows = lax.all_to_all(sums, axes, 0, 0, tiled=True)
    return residual, potential, jnp.sum(rows, 0)[: history.shape[0] + 1]


def solution(mesh):
    in_specs = (
        P(None, "gy", None),
        P("gz", "gy"),
        P(None, "gz", "gy"),
        P("gz", "gy", None),
        P(None, "gz", "gy", None),
        P("gz", "gy", None),
        P("gz", "gy", None),
    )
    out_specs = (P("gz", "gy"), P("gz", "gy"), P())

    def body(*arguments):
        coarse_density, density_in = arguments[:2]
        plan = Plan(
            (mesh.shape["gz"], mesh.shape["gy"]),
            2 * coarse_density.shape[0],
            coarse_density.shape[0],
            density_in.shape[0],
            2 * coarse_density.shape[1],
        )
        if plan.ok():
            return local_fast(plan, *arguments)
        return local(*arguments)

    return jax.shard_map(body, mesh=mesh, in_specs=in_specs, out_specs=out_specs, check_vma=False)
```

```python
import math

import jax
import jax.numpy as jnp
import numpy as np
from jax import lax
from jax.experimental import pallas as pl
from jax.experimental.pallas import tpu as pltpu
from jax.sharding import PartitionSpec as P

RC = 4
NF = 192


def with_halo(block, sides, width):
    for axis, dim in sides:
        count = lax.axis_size(axis)
        forward = [(i, i + 1) for i in range(count - 1)]
        forward.append((count - 1, 0))
        backward = [(target, source) for source, target in forward]
        low = lax.ppermute(
            lax.slice_in_dim(block, block.shape[dim] - width, None, axis=dim), axis, forward
        )
        high = lax.ppermute(lax.slice_in_dim(block, 0, width, axis=dim), axis, backward)
        block = jnp.concatenate([low, block, high], axis=dim)
    return block


def midpoint(extended, dimension, cells_in):

    def window(offset):
        return lax.slice_in_dim(extended, offset, offset + cells_in, axis=dimension)

    even_cells = window(2)
    odd_cells = (9.0 * (window(2) + window(3)) - window(1) - window(4)) / 16.0
    merged = jnp.stack([even_cells, odd_cells], dimension + 1)
    new_shape = list(even_cells.shape)
    new_shape[dimension] = 2 * cells_in
    return merged.reshape(new_shape)


def signed(counter, length):
    return jnp.where(counter < length // 2, counter, counter - length)


def shape_value(squared, charge, exponent):
    factor = charge * (exponent / jnp.pi) ** 1.5
    return factor * jnp.maximum(
        jnp.exp(-exponent * squared) - jnp.exp(-exponent * float(RC * RC)), 0.0
    )


def gaussians(dist_z, dist_y, dist_x, charge, exponent):
    squared = (
        dist_z[:, :, None, None] ** 2
        + dist_y[:, None, :, None] ** 2
        + dist_x[:, None, None, :] ** 2
    )
    return jnp.sum(
        shape_value(squared, charge[:, None, None, None], exponent[:, None, None, None]), 0
    )


def tables(length):
    counter = jnp.arange(length, dtype=jnp.int32)
    phase = counter[:, None] * counter[None, :] % length
    angle = 2.0 * jnp.pi / length * phase.astype(jnp.float32)
    return (jnp.cos(angle), jnp.sin(angle))


def contract(values, table, dimension):
    product = jnp.tensordot(values, table, axes=([dimension], [0]), precision=lax.Precision.HIGHEST)
    return jnp.moveaxis(product, -1, dimension)


def transform(spectra, dimension, direction):
    cosine, sine_table = tables(spectra.shape[dimension])
    inner_dim = dimension - 1
    real_part = spectra[:, 0]
    imag_part = spectra[:, 1]
    new_real = contract(real_part, cosine, inner_dim) - direction * contract(
        imag_part, sine_table, inner_dim
    )
    new_imag = contract(imag_part, cosine, inner_dim) + direction * contract(
        real_part, sine_table, inner_dim
    )
    result = jnp.stack([new_real, new_imag], 1)
    if direction > 0:
        result = result / spectra.shape[dimension]
    return result


def transform_y(pieces):
    return transform(pieces, 3, -1.0)


def transform_z(pieces):
    return transform(pieces, 2, -1.0)


def inverse_y(pieces):
    return transform(pieces, 3, 1.0)


def inverse_x_real(pieces):
    cosine, sine_table = tables(pieces.shape[4])
    real_part = contract(pieces[:, 0], cosine, 3) - contract(pieces[:, 1], sine_table, 3)
    return real_part / pieces.shape[4]


def forward(fields):
    cosine, sine_table = tables(fields.shape[3])
    spectra = jnp.stack([contract(fields, cosine, 3), -contract(fields, sine_table, 3)], 1)
    columns = transform_y(lax.all_to_all(spectra, "gy", split_axis=4, concat_axis=3, tiled=True))
    return transform_z(lax.all_to_all(columns, "gz", split_axis=3, concat_axis=2, tiled=True))


def inverse(spectra):
    local_z = transform(spectra, 2, 1.0)
    rows_back = inverse_y(lax.all_to_all(local_z, "gz", split_axis=2, concat_axis=3, tiled=True))
    return inverse_x_real(lax.all_to_all(rows_back, "gy", split_axis=3, concat_axis=4, tiled=True))


def poisson_weight(spectra):
    length = spectra.shape[2]
    y_block = spectra.shape[3]
    x_block = spectra.shape[4]
    wave_z = signed(jnp.arange(length, dtype=jnp.int32), length)
    wave_y = signed(lax.axis_index("gz") * y_block + jnp.arange(y_block, dtype=jnp.int32), length)
    wave_x = signed(lax.axis_index("gy") * x_block + jnp.arange(x_block, dtype=jnp.int32), length)
    squares = (
        wave_z[:, None, None] * wave_z[:, None, None]
        + wave_y[None, :, None] * wave_y[None, :, None]
        + wave_x[None, None, :] * wave_x[None, None, :]
    )
    scaled = (2.0 * jnp.pi / length) ** 2 * jnp.maximum(squares, 1).astype(jnp.float32)
    return jnp.where(squares > 0, 4.0 * jnp.pi / scaled, 0.0)


def total_intersections(own_terms):
    return lax.psum(own_terms, ("gz", "gy"))


def deposit_rims(atom_cell, atom_offset, atom_charge, atom_width, slab_z, slab_y, length):
    cell_ids = atom_cell.reshape(-1)
    local_z = cell_ids // (slab_y * length)
    local_y = cell_ids // length % slab_y
    local_x = cell_ids % length
    offsets = atom_offset.reshape(3, -1)
    dist_z = (jnp.arange(slab_z + 2 * RC, dtype=jnp.int32)[None, :] - RC - local_z[:, None]).astype(
        jnp.float32
    ) - offsets[0][:, None]
    dist_y = (jnp.arange(slab_y + 2 * RC, dtype=jnp.int32)[None, :] - RC - local_y[:, None]).astype(
        jnp.float32
    ) - offsets[1][:, None]
    dist_x = (
        signed(
            (jnp.arange(length, dtype=jnp.int32)[None, :] - local_x[:, None]) % length, length
        ).astype(jnp.float32)
        - offsets[2][:, None]
    )
    buffer_sum = gaussians(dist_z, dist_y, dist_x, atom_charge.reshape(-1), atom_width.reshape(-1))
    rims_z = jnp.concatenate([buffer_sum[:RC], buffer_sum[-RC:]], 0)
    near_z = with_halo(rims_z, (("gz", 0),), RC)
    middle = buffer_sum[RC : RC + slab_z]
    middle = middle.at[:RC].add(near_z[:RC]).at[slab_z - RC :].add(near_z[3 * RC :])
    rims_y = jnp.concatenate([middle[:, :RC], middle[:, -RC:]], 1)
    near_y = with_halo(rims_y, (("gy", 1),), RC)
    inside = middle[:, RC : RC + slab_y]
    return inside.at[:, :RC].add(near_y[:, :RC]).at[:, slab_y - RC :].add(near_y[:, 3 * RC :])


def local(coarse_density, density_in, history, atom_cell, atom_offset, atom_charge, atom_width):
    length = NF
    slab_z = density_in.shape[0]
    slab_y = density_in.shape[1] // length
    density_cube = density_in.reshape(slab_z, slab_y, length)
    history_cube = history.reshape(history.shape[0], slab_z, slab_y, length)
    extended = with_halo(coarse_density, (("gy", 1),), 2)
    coarse_rows = coarse_density.shape[0] // lax.axis_size("gz")
    beside_all = jnp.concatenate([extended[-2:], extended, extended[:2]], 0)
    start = lax.axis_index("gz") * coarse_rows
    own_planes = lax.dynamic_slice_in_dim(beside_all, start, coarse_rows + 4, 0)
    wrapped = jnp.concatenate([own_planes[:, :, -2:], own_planes, own_planes[:, :, :2]], 2)
    smooth = midpoint(wrapped, 2, coarse_density.shape[2])
    smooth = midpoint(smooth, 1, coarse_density.shape[1])
    smooth = midpoint(smooth, 0, coarse_rows)
    charge_field = deposit_rims(
        atom_cell, atom_offset, atom_charge, atom_width, slab_z, slab_y, length
    )
    residual = smooth + charge_field - density_cube
    cells_all = float(length) ** 3
    spectra = forward(residual[None])
    weight = poisson_weight(spectra)
    potential = inverse(weight * spectra)[0]
    own_terms = (
        jnp.concatenate(
            [
                jnp.sum(history_cube * potential[None], axis=(1, 2, 3)),
                jnp.sum(residual * potential)[None],
            ]
        )
        / cells_all
    )
    intersections = total_intersections(own_terms)
    return (
        residual.reshape(slab_z, slab_y * length),
        potential.reshape(slab_z, slab_y * length),
        intersections,
    )


GROUP = 16
LANES = 128
SUB = 8


def basis(length):
    half = length // 2
    wave = np.concatenate([np.arange(half + 1), np.arange(1, half)])
    angle = 2.0 * np.pi / length * (np.outer(wave, np.arange(length)) % length)
    rows = np.where(np.arange(length)[:, None] <= half, np.cos(angle), np.sin(angle))
    scale = np.where((wave == 0) | (wave == half), 1.0, np.sqrt(2.0)) / np.sqrt(length)
    return rows * scale[:, None], wave


def halves(values):
    high = values.astype(jnp.bfloat16)
    return high, (values - high.astype(jnp.float32)).astype(jnp.bfloat16)


def thirds(values):
    high = values.astype(jnp.bfloat16)
    rest = values - high.astype(jnp.float32)
    middle = rest.astype(jnp.bfloat16)
    return high, middle, (rest - middle.astype(jnp.float32)).astype(jnp.bfloat16)


NN = (((1,), (0,)), ((), ()))
NT = (((1,), (1,)), ((), ()))


def mm(left, right, dims):
    return lax.dot_general(left, right, dims, preferred_element_type=jnp.float32)


def mm3(left, right, dims=NN):
    rows = left[0].shape[0]
    both = mm(jnp.concatenate(left, 0), right[0], dims)
    return mm(left[0], right[1], dims) + both[rows:] + both[:rows]


def turn_tiles(tiles):
    row = lax.broadcasted_iota(jnp.int32, (SUB, LANES), 0)
    tiles = list(tiles)
    for step in (4, 2, 1):
        own = (row & step) == 0
        for i in range(SUB):
            if i & step == 0:
                first, second = tiles[i], tiles[i + step]
                tiles[i] = jnp.where(own, first, pltpu.roll(second, step, 0))
                tiles[i + step] = jnp.where(own, pltpu.roll(first, SUB - step, 0), second)
    return tiles


def slot(g, pair, k):
    if g < 7:
        return SUB * g + 2 * pair + k
    return SUB * (3 * (g - 7) + pair) + 6 + k


def fetch(pairs, sems, first=0):
    copies = [
        pltpu.make_async_copy(source, target, sems.at[first + i])
        for i, (source, target) in enumerate(pairs)
    ]
    for copy in copies:
        copy.start()
    return copies


def room(array):
    return pltpu.VMEM(array.shape, array.dtype)


TAIL = (54, 55, 62, 63)
EDGE = 56
VMEM_LIMIT = 60 * 1024 * 1024
LATE_LIMIT = 48 * 1024 * 1024


def tile_masks():
    row = lax.broadcasted_iota(jnp.int32, (SUB, LANES), 0)
    group = lax.broadcasted_iota(jnp.int32, (SUB, LANES), 1) // SUB
    return row, group


def rotate_up(upper, lower, masks):
    row, group = masks
    bit = (group & 8) != 0
    upper, lower = jnp.where(bit, lower, upper), jnp.where(bit, upper, lower)
    for shift in (4, 2, 1):
        bit = (group & shift) != 0
        roll_u = pltpu.roll(upper, SUB - shift, 0)
        roll_l = pltpu.roll(lower, SUB - shift, 0)
        stay = row < SUB - shift
        new_u = jnp.where(stay, roll_u, roll_l)
        new_l = jnp.where(stay, roll_l, roll_u)
        upper, lower = jnp.where(bit, new_u, upper), jnp.where(bit, new_l, lower)
    return upper, lower


def skew(values, start):
    return pltpu.roll(values, start, 1, stride=SUB, stride_axis=0)


def block_turn(upper, lower, masks):
    upper, lower = rotate_up(skew(upper, 0), skew(lower, 64), masks)
    return skew(upper, 0), skew(lower, 64)


class Plan:
    def __init__(self, mesh_shape, length, coarse, fz, fy):
        self.nz, self.ny = mesh_shape
        self.count = self.nz * self.ny
        self.length, self.coarse, self.fz, self.fy = length, coarse, fz, fy
        self.j = length // self.count
        self.zo, self.yo = fz // SUB, fy // GROUP
        self.rows_out = 64
        self.rows_back = 56
        self.ext = length + 32

    def ok(self):
        return (
            (self.nz, self.ny, self.zo, self.yo, self.j) == (8, 4, 3, 3, 6)
            and self.fz % SUB == 0
            and self.fy % GROUP == 0
            and self.length == self.coarse * 2
        )


def ext_slot(edge, zo):
    return ((15, 3, 1)[edge] + 5 * zo) % GROUP


def fast_tables(plan):
    length, nz = plan.length, plan.nz
    rows, wave = basis(length)
    fine_of = np.zeros((plan.coarse, length), np.float32)
    for i in range(plan.coarse):
        fine_of[i, 2 * i] += 1.0
        for step, value in ((0, 9), (1, 9), (-1, -1), (2, -1)):
            fine_of[(i + step) % plan.coarse, 2 * i + 1] += value / 16.0
    local_z = np.zeros((plan.fz, GROUP), np.float32)
    for i in range(plan.fz // 2):
        local_z[2 * i, i + 1] = 1.0
        for step, value in ((1, 9), (2, 9), (0, -1), (3, -1)):
            local_z[2 * i + 1, i + step] += value / 16.0

    def along_z(turn):
        half_of, owner = turn // SUB, turn % SUB
        lane = np.arange(SUB)
        z_main = (owner[:, None] * plan.fz + half_of[:, None] * SUB + lane[None]).reshape(-1)
        z_shared = (owner[:, None] * plan.fz + 2 * SUB + lane[None]).reshape(-1)
        odd = np.repeat(half_of, SUB)
        tables_z = []
        for parity in (0, 1):
            table = np.zeros((2 * LANES, length))
            table[:LANES] = rows[:, z_main].T
            table[LANES:] = np.where((odd == parity)[:, None], rows[:, z_shared].T, 0.0)
            tables_z.append(table)
        return tables_z

    z_tables = along_z(np.arange(GROUP))
    z_back = along_z((-np.arange(GROUP)) % GROUP)
    y_of_row = (np.arange(plan.ext) - SUB) % length
    count = plan.count
    x_window = np.zeros((count, length + GROUP, SUB), np.float32)
    x_of_row = (np.arange(length + GROUP) - SUB) % length
    padded = np.zeros((count, SUB, length))
    kept = np.zeros((count, SUB, length))
    donors = np.zeros((3, count, SUB, length))
    for d in range(count):
        for j in range(plan.j):
            mode = rows[j * count + d]
            x_window[d, :, j] = mode[x_of_row]
            padded[d, j] = kept[d, j] = mode
            donors[j // 2, d, 6 + j % 2] = mode
        padded[d, 6:] = padded[d, 4:6]
    flat = lambda table: table.reshape(count * SUB, length)
    def halves_of(table):
        table = np.asarray(table, np.float32)
        high = table.astype(jnp.bfloat16)
        return [high, (table - high.astype(np.float32)).astype(jnp.bfloat16)]

    def pack(tables_in):
        width = max(table.shape[-1] for table in tables_in)
        return jnp.asarray(
            np.concatenate(
                [
                    np.pad(table, ((0, 0), (0, width - table.shape[-1])))
                    for table in tables_in
                ],
                0,
            )
        )

    z_all = np.stack(z_tables).reshape(-1, length)
    zt_all = np.stack([t.T for t in z_back]).reshape(-1, 2 * LANES)
    near = [np.kron(np.eye(SUB), local_z), fine_of]
    return {
        "a": pack(halves_of(flat(padded)) + [table.astype(jnp.bfloat16) for table in near]),
        "b": pack(
            halves_of(z_all) + halves_of(zt_all) + halves_of(rows[:, y_of_row]) + halves_of(rows.T)
        ),
        "c": pack(halves_of(np.stack([flat(kept)] + [flat(donors[i]) for i in range(3)]).reshape(-1, length))),
        "window": jnp.asarray(x_window.reshape(count, 1, -1)),
    }


def near_tables(plan, near, first):
    kron_rows = SUB * plan.fz
    kron = near[first : first + kron_rows, :LANES]
    return kron, near[first + kron_rows : first + kron_rows + plan.coarse, :]


def part_a(plan, t):
    length, fz, fy, count = plan.length, plan.fz, plan.fy, plan.count
    rows_c = fy // 2
    per = plan.rows_out

    def kernel(
        cell_h, offset_h, charge_h, width_h, coarse_h, density_h, table_h, send_h, partial_h,
        cell, offset, charge, width, coarse, density, tables_v, send, partial, planes, smooth, field, donor, sems,
    ):
        first = fetch([(coarse_h, coarse), (table_h, tables_v)], sems)
        second = fetch([(density_h, density)], sems, 3)
        facts_in = fetch(
            [(cell_h, cell), (offset_h, offset), (charge_h, charge), (width_h, width)], sems, 4
        )
        for copy in first:
            copy.wait()
        kron, fine = near_tables(plan, tables_v, 2 * count * SUB)
        a = lax.axis_index("gz")
        b = lax.axis_index("gy")
        own = plan.coarse // plan.nz
        for t in range(GROUP):
            planes[pl.ds(t * rows_c, rows_c), :] = coarse[lax.rem(own * a + plan.coarse - 1 + t, plan.coarse)]
        for part in range(rows_c // SUB):
            block = jnp.concatenate(
                [planes[pl.ds(part * SUB + y, GROUP, stride=rows_c), :] for y in range(SUB)], 0
            )
            wide = sum(mm(piece, fine, NN) for piece in thirds(block)[::-1])
            tall = sum(mm(kron, piece, NN) for piece in thirds(wide)[::-1])
            for y in range(SUB):
                smooth[part * SUB + y] = tall[y * fz : (y + 1) * fz]

        def row(i):
            return smooth[i] if 0 <= i < rows_c else jnp.zeros((fz, length), jnp.float32)

        second[0].wait()
        for i in range(rows_c):
            odd_row = (9.0 * (row(i) + row(i + 1)) - row(i - 1) - row(i + 2)) * (1.0 / 16.0)
            old = density[:, 2 * i * length : (2 * i + 2) * length]
            even_out = smooth[i] - old[:, :length]
            odd_out = odd_row - old[:, length:]
            field[2 * i] = even_out
            field[2 * i + 1] = odd_out
            partial[:, 2 * i * length : (2 * i + 2) * length] = jnp.concatenate([even_out, odd_out], 1)
        edges = (
            row(rows_c - 1) * (-1.0 / 16.0),
            row(0) * (-1.0 / 16.0),
            (9.0 * row(0) - row(1)) * (1.0 / 16.0),
        )
        out_partial = fetch([(partial, partial_h)], sems, 9)
        table = (tables_v[: count * SUB, :], tables_v[count * SUB : 2 * count * SUB, :])
        sub_row = lax.broadcasted_iota(jnp.int32, (count, SUB, LANES), 1)

        def modes(block):
            out = mm3(table, halves(block), NT)
            return [
                out[:, g * LANES : (g + 1) * LANES].reshape(count, SUB, LANES)
                for g in range(out.shape[1] // LANES)
            ]

        for yo in (2, 0, 1):
            block = jnp.concatenate(
                [
                    field[yo * GROUP + (-g) % GROUP, zo * SUB : (zo + 1) * SUB, :]
                    for zo in range(plan.zo)
                    for g in range(GROUP)
                ],
                0,
            )
            found = modes(block)
            if yo == 2:
                send[:, 48:56, :] = found[0]
                donor[0] = found[1]
                donor[1] = found[2]
            else:
                for pair in range(3):
                    other = donor[yo]
                    if pair < 2:
                        other = pltpu.roll(other, 6 - 2 * pair, 1)
                    at = SUB * (3 * yo + pair)
                    send[:, at : at + SUB, :] = jnp.where(sub_row < 6, found[pair], other)
        slots = [jnp.zeros((SUB, length), jnp.float32)] * GROUP
        for zo in range(plan.zo):
            for edge in range(3):
                slots[ext_slot(edge, zo)] = edges[edge][zo * SUB : (zo + 1) * SUB]
        send[:, EDGE : EDGE + SUB, :] = modes(jnp.concatenate(slots, 0))[0]
        for copy in facts_in:
            copy.wait()
        number = cell[0]
        plane = fy * length
        facts = (
            (a * fz + number // plane).astype(jnp.float32),
            (b * fy + lax.rem(number // length, fy)).astype(jnp.float32),
            lax.rem(number, length).astype(jnp.float32),
            offset[0],
            offset[1],
            offset[2],
            charge[0],
            width[0],
        )
        lane = lax.broadcasted_iota(jnp.int32, (1, LANES), 1)
        atom = jnp.zeros((1, LANES), jnp.float32)
        for i, fact in enumerate(facts):
            atom = jnp.where(lane == i, fact, atom)
        send[:, TAIL[0] : TAIL[0] + 1, :] = jnp.broadcast_to(atom[None], (count, 1, LANES))
        pad = jnp.zeros((1, LANES - plan.coarse), jnp.float32)
        ahead = lax.rem(b + 1, plan.ny)
        behind = lax.rem(b + plan.ny - 1, plan.ny)
        for dest in range(plan.nz):
            for zz in range(2):
                p = lax.rem(own * dest + plan.coarse - 1 + 2 * a + zz, plan.coarse)
                for edge, target, slot in ((rows_c - 1, ahead, 0), (0, behind, 0), (1, behind, 2)):
                    line = jnp.concatenate([pad, coarse[p, edge : edge + 1, :]], 1)
                    index = slot + zz
                    if index == 0:
                        line = jnp.where(lane < SUB, atom, line)
                    send[dest * plan.ny + target, TAIL[index] : TAIL[index] + 1, :] = line
        out_send = fetch([(send, send_h)], sems, 10)
        for copy in out_partial + out_send:
            copy.wait()

    hbm = pl.BlockSpec(memory_space=pltpu.HBM)
    return pl.pallas_call(
        kernel,
        name="spread",
        in_specs=[hbm] * 7,
        out_specs=[hbm, hbm],
        out_shape=[
            jax.ShapeDtypeStruct((count, per, LANES), jnp.float32),
            jax.ShapeDtypeStruct((fz, fy * length), jnp.float32),
        ],
        compiler_params=pltpu.CompilerParams(vmem_limit_bytes=VMEM_LIMIT),
        scratch_shapes=[
            pltpu.SMEM((1,), jnp.int32),
            pltpu.SMEM((3,), jnp.float32),
            pltpu.SMEM((1,), jnp.float32),
            pltpu.SMEM((1,), jnp.float32),
            pltpu.VMEM((plan.coarse, rows_c, plan.coarse), jnp.float32),
            pltpu.VMEM((fz, fy * length), jnp.float32),
            room(t["a"]),
            pltpu.VMEM((count, per, LANES), jnp.float32),
            pltpu.VMEM((fz, fy * length), jnp.float32),
            pltpu.VMEM((GROUP * rows_c, plan.coarse), jnp.float32),
            pltpu.VMEM((rows_c, fz, length), jnp.float32),
            pltpu.VMEM((fy, fz, length), jnp.float32),
            pltpu.VMEM((2, count, SUB, LANES), jnp.float32),
            pltpu.SemaphoreType.DMA((11,)),
        ],
        cost_estimate=pl.CostEstimate(flops=500_000_000, bytes_accessed=4_000_000, transcendentals=0),
    )


def wrapped(distance, length):
    half = length // 2
    distance = jnp.where(distance >= half, distance - length, distance)
    return jnp.where(distance < -half, distance + length, distance)


def part_b(plan, t):
    length, count, ext = plan.length, plan.count, plan.ext
    per, per_back = plan.rows_out, plan.rows_back

    def kernel(
        window_h, recv_h, table_h, send_h,
        window, recv, tables_v, send, main, shared, turned, ready, atoms_v, atoms, sem, sems, sems_in, sems_out,
    ):
        device = lax.axis_index("gz") * plan.ny + lax.axis_index("gy")

        def incoming(b):
            return pltpu.make_async_copy(recv_h.at[:, b], recv.at[:, b], sems_in.at[b])

        def outgoing(b):
            return pltpu.make_async_copy(send.at[:, b], send_h.at[:, b], sems_out.at[b])

        for b in range(plan.ny):
            incoming(b).start()
        copies = fetch(
            [
                (window_h.at[device], window),
                (table_h, tables_v),
            ],
            sems,
        )
        def unpack(b, carry):
            incoming(b).wait()
            for t in range(per // SUB):
                tiles = turn_tiles(
                    [recv[a, b, t * SUB : (t + 1) * SUB, :] for a in range(plan.nz)]
                )
                for i, tile in enumerate(tiles):
                    turned[b, t * SUB + i] = tile
            atoms_v[pl.ds(pl.multiple_of(b * SUB, SUB), SUB), :] = turned[b, TAIL[0]]
            return carry

        lax.fori_loop(0, plan.ny, unpack, 0)
        copy = pltpu.make_async_copy(atoms_v, atoms, sem)
        copy.start()
        masks = tile_masks()
        group = masks[1]
        for j in range(plan.j):
            main[j, :SUB, :] = jnp.zeros((SUB, LANES), jnp.float32)
            main[j, SUB + length :, :] = jnp.zeros((ext - SUB - length, LANES), jnp.float32)
        for jp in range(plan.j // 2):
            shared[jp, :SUB, :] = jnp.zeros((SUB, LANES), jnp.float32)
            shared[jp, SUB + length :, :] = jnp.zeros((ext - SUB - length, LANES), jnp.float32)
        def gather(step, carry):
            jp = step // plan.ny
            b = lax.rem(step, plan.ny)
            edge_ahead = lax.rem(b + 1, plan.ny)
            edge_behind = lax.rem(b + plan.ny - 1, plan.ny)
            edges = []
            for source in (edge_behind, edge_ahead):
                edges.append([turned[source, EDGE + 2 * jp + k] for k in (0, 1)])
            for yo in range(plan.yo):
                tiles = []
                for k in (0, 1):
                    for zo in range(plan.zo):
                        tile = turned[b, slot(yo * plan.zo + zo, jp, k)]
                        shift = (LANES - 5 * zo * SUB) % LANES
                        if yo == 0:
                            extra = pltpu.roll(edges[0][k], shift, 1) if shift else edges[0][k]
                            tile = jnp.where(group == 15, tile + extra, tile)
                        if yo == plan.yo - 1:
                            extra = pltpu.roll(edges[1][k], shift, 1) if shift else edges[1][k]
                            tile = jnp.where((group == 3) | (group == 1), tile + extra, tile)
                        tiles.append(tile)
                at = pl.multiple_of(SUB + b * plan.fy + yo * GROUP, SUB)
                for k in (0, 1):
                    upper, lower = block_turn(tiles[3 * k], tiles[3 * k + 1], masks)
                    main[2 * jp + k, pl.ds(at, SUB), :] = upper
                    main[2 * jp + k, pl.ds(at + SUB, SUB), :] = lower
                upper, lower = block_turn(tiles[2], tiles[5], masks)
                shared[jp, pl.ds(at, SUB), :] = upper
                shared[jp, pl.ds(at + SUB, SUB), :] = lower
            return carry

        lax.fori_loop(0, plan.ny * (plan.j // 2), gather, 0)
        copy.wait()
        for item in copies:
            item.wait()
        lane = lax.broadcasted_iota(jnp.int32, (1, LANES), 1)
        block = lane // SUB
        odd = block >= SUB
        z_first = (block & (SUB - 1)) * plan.fz + (lane & (SUB - 1))
        z_main = (z_first + jnp.where(odd, SUB, 0)).astype(jnp.float32)
        z_shared = (z_first + 2 * SUB).astype(jnp.float32)
        window_rows = lax.broadcasted_iota(jnp.int32, (GROUP, LANES), 0).astype(jnp.float32) - RC

        def deposit(i, carry):
            z0, y0, x0 = atoms[i, 0], atoms[i, 1], atoms[i, 2]
            off_z, off_y, off_x = atoms[i, 3], atoms[i, 4], atoms[i, 5]
            charge, width = atoms[i, 6], atoms[i, 7]
            ratio = jnp.full((SUB, LANES), width / jnp.pi, jnp.float32)
            factor = ratio * jnp.sqrt(ratio) * charge
            factor = factor[0:1]
            cut = jnp.exp(jnp.full((SUB, LANES), -width * float(RC * RC), jnp.float32))[0:1]
            profile_y = jnp.exp(-width * (window_rows - off_y) ** 2)
            profile_x = jnp.exp(-width * (window_rows - off_x) ** 2)
            planes = []
            for z in (z_main, z_shared):
                profile_z = jnp.exp(-width * (wrapped(z - z0, length) - off_z) ** 2)
                planes.append(profile_y * profile_z)
            base = (x0.astype(jnp.int32) - RC + SUB) * SUB
            zero = jnp.zeros((GROUP, LANES), jnp.float32)
            sums = [[zero, zero, zero] for _ in range(plan.j // 2)]
            for dx in range(2 * RC + 2):
                line = profile_x[dx : dx + 1]
                bell = [jnp.maximum(plane * line - cut, 0.0) for plane in planes]
                for jp in range(plan.j // 2):
                    even = window[0, base + dx * SUB + 2 * jp]
                    odd_value = window[0, base + dx * SUB + 2 * jp + 1]
                    sums[jp][0] += bell[0] * even
                    sums[jp][1] += bell[0] * odd_value
                    sums[jp][2] += bell[1] * jnp.where(odd, odd_value, even)
            at = y0.astype(jnp.int32) - RC + SUB
            for jp in range(plan.j // 2):
                for k in (0, 1):
                    main[2 * jp + k, pl.ds(at, GROUP), :] += sums[jp][k] * factor
                shared[jp, pl.ds(at, GROUP), :] += sums[jp][2] * factor
            return carry

        lax.fori_loop(0, count, deposit, 0)
        scale = float(length) ** 2 / math.pi
        half = length // 2

        def square(mode):
            wave = jnp.where(mode <= half, mode, mode - half)
            return (wave * wave).astype(jnp.float32)

        plane = square(lax.broadcasted_iota(jnp.int32, (length, length), 0)) + square(
            lax.broadcasted_iota(jnp.int32, (length, length), 1)
        )
        zt, zti, yt, yti = [], [], [], []
        at = 0
        for into, size, width, parts in (
            (zt, 2 * LANES, length, 2),
            (zti, length, 2 * LANES, 2),
            (yt, length, ext, 1),
            (yti, length, length, 1),
        ):
            for half_index in range(2):
                into.append(
                    [tables_v[at + i * size : at + (i + 1) * size, :width] for i in range(parts)]
                )
                at += parts * size
        backs = []
        energy = jnp.zeros((SUB, length), jnp.float32)
        for k in (0, 1):
            left = jnp.concatenate(
                [
                    jnp.concatenate([main[2 * jp + k], shared[jp]], 1)
                    for jp in range(plan.j // 2)
                ],
                0,
            )
            rows_z = mm3(halves(left), (zt[0][k], zt[1][k]))
            rows_y = []
            for jp in range(plan.j // 2):
                full = mm3((yt[0][0], yt[1][0]), halves(rows_z[jp * ext : (jp + 1) * ext]))
                squares = plane + square((2 * jp + k) * count + device)
                weight = jnp.where(squares > 0.0, scale / jnp.maximum(squares, 1.0), 0.0)
                weighted = full * weight
                product = full * weighted
                for i in range(length // SUB):
                    energy += product[i * SUB : (i + 1) * SUB]
                rows_y.append(mm3((yti[0][0], yti[1][0]), halves(weighted)))
            backs.append(mm3(halves(jnp.concatenate(rows_y, 0)), (zti[0][k], zti[1][k])))
        for jp in range(plan.j // 2):
            here = slice(jp * length, (jp + 1) * length)
            for k in (0, 1):
                main[2 * jp + k, SUB : SUB + length, :] = backs[k][here, :LANES]
            shared[jp, SUB : SUB + length, :] = backs[0][here, LANES:] + backs[1][here, LANES:]

        def scatter(step, carry):
            jp = step // plan.ny
            b = lax.rem(step, plan.ny)
            for yo in range(plan.yo):
                at = pl.multiple_of(SUB + b * plan.fy + yo * GROUP, SUB)
                tiles = []
                for k in (0, 1):
                    tiles.append(
                        block_turn(
                            main[2 * jp + k, pl.ds(at, SUB), :],
                            main[2 * jp + k, pl.ds(at + SUB, SUB), :],
                            masks,
                        )
                    )
                both = block_turn(
                    shared[jp, pl.ds(at, SUB), :], shared[jp, pl.ds(at + SUB, SUB), :], masks
                )
                for k in (0, 1):
                    for zo, tile in enumerate((tiles[k][0], tiles[k][1], both[k])):
                        ready[b, slot(yo * plan.zo + zo, jp, k)] = tile
            return carry

        lax.fori_loop(0, plan.ny * (plan.j // 2), scatter, 0)

        share = jnp.sum(energy) * (1.0 / count)

        def pack(b, carry):
            for row in TAIL[:2]:
                ready[b, row] = jnp.full((SUB, LANES), share, jnp.float32)
            for t in range(per_back // SUB):
                tiles = turn_tiles([ready[b, t * SUB + i] for i in range(SUB)])
                for a, tile in enumerate(tiles):
                    send[a, b, t * SUB : (t + 1) * SUB, :] = tile
            outgoing(b).start()
            return carry

        lax.fori_loop(0, plan.ny, pack, 0)
        for b in range(plan.ny):
            outgoing(b).wait()

    hbm = pl.BlockSpec(memory_space=pltpu.HBM)
    vmem = pl.BlockSpec(memory_space=pltpu.VMEM)
    return pl.pallas_call(
        kernel,
        name="solve",
        in_specs=[hbm, hbm, hbm],
        out_specs=hbm,
        out_shape=jax.ShapeDtypeStruct((plan.nz, plan.ny, per_back, LANES), jnp.float32),
        compiler_params=pltpu.CompilerParams(vmem_limit_bytes=VMEM_LIMIT),
        scratch_shapes=[
            pltpu.SMEM(t["window"].shape[1:], jnp.float32),
            pltpu.VMEM((plan.nz, plan.ny, per, LANES), jnp.float32),
            room(t["b"]),
            pltpu.VMEM((plan.nz, plan.ny, per_back, LANES), jnp.float32),
            pltpu.VMEM((plan.j, ext, LANES), jnp.float32),
            pltpu.VMEM((plan.j // 2, ext, LANES), jnp.float32),
            pltpu.VMEM((plan.ny, per, SUB, LANES), jnp.float32),
            pltpu.VMEM((plan.ny, per_back, SUB, LANES), jnp.float32),
            pltpu.VMEM((count, LANES), jnp.float32),
            pltpu.SMEM((count, LANES), jnp.float32),
            pltpu.SemaphoreType.DMA,
            pltpu.SemaphoreType.DMA((2,)),
            pltpu.SemaphoreType.DMA((plan.ny,)),
            pltpu.SemaphoreType.DMA((plan.ny,)),
        ],
        cost_estimate=pl.CostEstimate(flops=2_000_000_000, bytes_accessed=4_000_000, transcendentals=0),
    )


def part_r(plan, t):
    length, fz, fy, count = plan.length, plan.fz, plan.fy, plan.count
    per = plan.rows_out

    def kernel(
        recv, partial_h, table_h, out_h,
        partial, tables_v, out, field, lines, atoms_v, atoms, sem, sems,
    ):
        copies = fetch([(partial_h, partial), (table_h, tables_v)], sems)
        a = lax.axis_index("gz")
        b = lax.axis_index("gy")
        for i in range(count):
            atoms_v[i : i + 1, :] = recv[i, TAIL[0] : TAIL[0] + 1, :]
        copy = pltpu.make_async_copy(atoms_v, atoms, sem)
        copy.start()
        ahead = lax.rem(b + 1, plan.ny)
        behind = lax.rem(b + plan.ny - 1, plan.ny)
        lines[...] = jnp.zeros_like(lines)
        for source in range(plan.nz):
            for zz in range(2):
                for number, (origin, index) in enumerate(((behind, 0), (ahead, 0), (ahead, 2))):
                    at = TAIL[index + zz]
                    into = number * GROUP + 2 * source + zz
                    lines[into : into + 1, :] = recv[source * plan.ny + origin, at : at + 1, :]
        block = lines[...][:, LANES - plan.coarse :]
        for item in copies:
            item.wait()
        kron, fine = near_tables(plan, tables_v, 2 * count * SUB)
        wide = sum(mm(piece, fine, NN) for piece in thirds(block)[::-1])
        tall = sum(mm(kron, piece, NN) for piece in thirds(wide)[::-1])
        below, above, above2 = (tall[i * fz : (i + 1) * fz] for i in range(3))
        field[...] = jnp.zeros_like(field)
        field[1] = below * (-1.0 / 16.0)
        field[fy - 3] = above * (-1.0 / 16.0)
        field[fy - 1] = (9.0 * above - above2) * (1.0 / 16.0)
        copy.wait()
        z_here = lax.broadcasted_iota(jnp.int32, (fz, length), 0).astype(jnp.float32)
        x_here = lax.broadcasted_iota(jnp.int32, (fz, length), 1).astype(jnp.float32)

        def deposit(i, carry):
            z0 = wrapped(atoms[i, 0] - (a * fz).astype(jnp.float32), length)
            y0 = wrapped(atoms[i, 1] - (b * fy).astype(jnp.float32), length).astype(jnp.int32)
            first = jnp.maximum(y0 - RC, 0)
            last = jnp.minimum(y0 + RC + 2, fy)
            near_z = (z0 > -RC - 2.0) & (z0 < fz + RC + 1.0)

            @pl.when(near_z & (first < last))
            def _():
                off_z, off_y, off_x = atoms[i, 3], atoms[i, 4], atoms[i, 5]
                charge, width = atoms[i, 6], atoms[i, 7]
                ratio = jnp.full((fz, length), width / jnp.pi, jnp.float32)
                factor = ratio * jnp.sqrt(ratio) * charge
                cut = jnp.exp(jnp.full((fz, length), -width * float(RC * RC), jnp.float32))
                dist_z = z_here - z0 - off_z
                dist_x = wrapped(x_here - atoms[i, 2], length) - off_x
                flat = dist_z * dist_z + dist_x * dist_x

                def row(y, inner):
                    dist_y = (y - y0).astype(jnp.float32) - off_y
                    bell = jnp.maximum(jnp.exp(-width * (flat + dist_y * dist_y)) - cut, 0.0)
                    field[y] += bell * factor
                    return inner

                lax.fori_loop(first, last, row, 0)

            return carry

        lax.fori_loop(0, count, deposit, 0)
        for i in range(fy // 2):
            span = slice(2 * i * length, (2 * i + 2) * length)
            out[:, span] = partial[:, span] + jnp.concatenate([field[2 * i], field[2 * i + 1]], 1)
        for item in fetch([(out, out_h)], sems, 3):
            item.wait()

    hbm = pl.BlockSpec(memory_space=pltpu.HBM)
    vmem = pl.BlockSpec(memory_space=pltpu.VMEM)
    return pl.pallas_call(
        kernel,
        name="finish",
        compiler_params=pltpu.CompilerParams(vmem_limit_bytes=VMEM_LIMIT),
        in_specs=[vmem, hbm, hbm],
        out_specs=hbm,
        out_shape=jax.ShapeDtypeStruct((fz, fy * length), jnp.float32),
        scratch_shapes=[
            pltpu.VMEM((fz, fy * length), jnp.float32),
            room(t["a"]),
            pltpu.VMEM((fz, fy * length), jnp.float32),
            pltpu.VMEM((fy, fz, length), jnp.float32),
            pltpu.VMEM((SUB * GROUP, LANES), jnp.float32),
            pltpu.VMEM((count, LANES), jnp.float32),
            pltpu.SMEM((count, LANES), jnp.float32),
            pltpu.SemaphoreType.DMA,
            pltpu.SemaphoreType.DMA((4,)),
        ],
        cost_estimate=pl.CostEstimate(flops=3_000_000_000, bytes_accessed=4_000_000, transcendentals=0),
    )


def part_c(plan, t, terms):
    length, fz, fy, count = plan.length, plan.fz, plan.fy, plan.count
    per = plan.rows_back
    wide = 3 * LANES

    def kernel(
        recv, table_h, history_h, potential_h, sums, tables_v, history, potential, sems
    ):
        first = fetch([(table_h, tables_v)], sems)
        copies = fetch([(history_h.at[i], history.at[i]) for i in range(terms)], sems, 2)
        first[0].wait()
        size = count * SUB
        xb = [
            [tables_v[(4 * h + i) * size : (4 * h + i + 1) * size, :] for i in range(4)]
            for h in range(2)
        ]
        def modes(t):
            return halves(recv[:, t * SUB : (t + 1) * SUB, :].reshape(count * SUB, LANES).T)

        def place(block, values):
            yo, zo = block // plan.zo, block % plan.zo
            for pair in range(GROUP // 2):
                at = (yo * GROUP + 2 * pair) * length
                rows = values[2 * pair * SUB : (2 * pair + 2) * SUB]
                potential[zo * SUB : (zo + 1) * SUB, at : at + 2 * length] = jnp.concatenate(
                    [rows[:SUB], rows[SUB:]], 1
                )

        given = [None, None]
        for t in range(per // SUB):
            left = modes(t)
            place(t, mm3(left, (xb[0][0], xb[1][0])))
            if t < 6:
                part = mm3(left, (xb[0][1 + t % 3], xb[1][1 + t % 3]))
                given[t // 3] = part if given[t // 3] is None else given[t // 3] + part
        place(7, given[0])
        place(8, given[1])
        out = fetch([(potential, potential_h)], sems, 2 + terms)
        acc = []
        for i in range(terms):
            def add(c, total, i=i):
                cut = pl.ds(pl.multiple_of(c * wide, LANES), wide)
                return total + history[i, :, cut] * potential[:, cut]

            copies[i].wait()
            acc.append(
                lax.fori_loop(
                    0, fy * length // wide, add, jnp.zeros((fz, wide), jnp.float32), unroll=4
                )
            )
        lane = lax.broadcasted_iota(jnp.int32, (1, LANES), 1)
        line = jnp.zeros((1, LANES), jnp.float32)
        for i in range(terms):
            line = jnp.where(lane == i, jnp.sum(acc[i]), line)
        own = jnp.sum(recv[:, TAIL[0] : TAIL[0] + 1, :], axis=0)
        line = jnp.where(lane == terms, own, line)
        sums[...] = jnp.broadcast_to(line * (1.0 / float(length) ** 3), (count, LANES))
        out[0].wait()

    hbm = pl.BlockSpec(memory_space=pltpu.HBM)
    vmem = pl.BlockSpec(memory_space=pltpu.VMEM)
    return pl.pallas_call(
        kernel,
        name="finish_potential",
        in_specs=[vmem, hbm, hbm],
        out_specs=[hbm, vmem],
        scratch_shapes=[
            room(t["c"]),
            pltpu.VMEM((terms, fz, fy * length), jnp.float32),
            pltpu.VMEM((fz, fy * length), jnp.float32),
            pltpu.SemaphoreType.DMA((3 + terms,)),
        ],
        out_shape=[
            jax.ShapeDtypeStruct((fz, fy * length), jnp.float32),
            jax.ShapeDtypeStruct((count, LANES), jnp.float32),
        ],
        compiler_params=pltpu.CompilerParams(vmem_limit_bytes=LATE_LIMIT),
        cost_estimate=pl.CostEstimate(flops=500_000_000, bytes_accessed=10_000_000, transcendentals=0),
    )


def exchange(sent, axes):
    return lax.all_to_all(sent, axes, 0, 0, tiled=True)


def local_fast(plan, coarse_density, density_in, history, atom_cell, atom_offset, atom_charge, atom_width):
    axes = ("gz", "gy")
    count = plan.count
    tables_ = fast_tables(plan)
    sent, partial = part_a(plan, tables_)(
        atom_cell.reshape(1),
        atom_offset.reshape(3),
        atom_charge.reshape(1),
        atom_width.reshape(1),
        coarse_density,
        density_in,
        tables_["a"],
    )
    spectra = exchange(sent, axes)
    solved = part_b(plan, tables_)(
        tables_["window"],
        spectra.reshape((plan.nz, plan.ny) + spectra.shape[1:]),
        tables_["b"],
    )
    back = exchange(solved.reshape((count,) + solved.shape[2:]), axes)
    residual = part_r(plan, tables_)(spectra, partial, tables_["a"])
    potential, sums = part_c(plan, tables_, history.shape[0])(back, tables_["c"], history)
    rows = lax.all_to_all(sums, axes, 0, 0, tiled=True)
    return residual, potential, jnp.sum(rows, 0)[: history.shape[0] + 1]


def solution(mesh):
    in_specs = (
        P(None, "gy", None),
        P("gz", "gy"),
        P(None, "gz", "gy"),
        P("gz", "gy", None),
        P(None, "gz", "gy", None),
        P("gz", "gy", None),
        P("gz", "gy", None),
    )
    out_specs = (P("gz", "gy"), P("gz", "gy"), P())

    def body(*arguments):
        coarse_density, density_in = arguments[:2]
        plan = Plan(
            (mesh.shape["gz"], mesh.shape["gy"]),
            2 * coarse_density.shape[0],
            coarse_density.shape[0],
            density_in.shape[0],
            2 * coarse_density.shape[1],
        )
        if plan.ok():
            return local_fast(plan, *arguments)
        return local(*arguments)

    return jax.shard_map(body, mesh=mesh, in_specs=in_specs, out_specs=out_specs, check_vma=False)
```

```python
import math

import jax
import jax.numpy as jnp
import numpy as np
from jax import lax
from jax.experimental import pallas as pl
from jax.experimental.pallas import tpu as pltpu
from jax.sharding import PartitionSpec as P

RC = 4
NF = 192


def with_halo(block, sides, width):
    for axis, dim in sides:
        count = lax.axis_size(axis)
        forward = [(i, i + 1) for i in range(count - 1)]
        forward.append((count - 1, 0))
        backward = [(target, source) for source, target in forward]
        low = lax.ppermute(
            lax.slice_in_dim(block, block.shape[dim] - width, None, axis=dim), axis, forward
        )
        high = lax.ppermute(lax.slice_in_dim(block, 0, width, axis=dim), axis, backward)
        block = jnp.concatenate([low, block, high], axis=dim)
    return block


def midpoint(extended, dimension, cells_in):

    def window(offset):
        return lax.slice_in_dim(extended, offset, offset + cells_in, axis=dimension)

    even_cells = window(2)
    odd_cells = (9.0 * (window(2) + window(3)) - window(1) - window(4)) / 16.0
    merged = jnp.stack([even_cells, odd_cells], dimension + 1)
    new_shape = list(even_cells.shape)
    new_shape[dimension] = 2 * cells_in
    return merged.reshape(new_shape)


def signed(counter, length):
    return jnp.where(counter < length // 2, counter, counter - length)


def shape_value(squared, charge, exponent):
    factor = charge * (exponent / jnp.pi) ** 1.5
    return factor * jnp.maximum(
        jnp.exp(-exponent * squared) - jnp.exp(-exponent * float(RC * RC)), 0.0
    )


def gaussians(dist_z, dist_y, dist_x, charge, exponent):
    squared = (
        dist_z[:, :, None, None] ** 2
        + dist_y[:, None, :, None] ** 2
        + dist_x[:, None, None, :] ** 2
    )
    return jnp.sum(
        shape_value(squared, charge[:, None, None, None], exponent[:, None, None, None]), 0
    )


def tables(length):
    counter = jnp.arange(length, dtype=jnp.int32)
    phase = counter[:, None] * counter[None, :] % length
    angle = 2.0 * jnp.pi / length * phase.astype(jnp.float32)
    return (jnp.cos(angle), jnp.sin(angle))


def contract(values, table, dimension):
    product = jnp.tensordot(values, table, axes=([dimension], [0]), precision=lax.Precision.HIGHEST)
    return jnp.moveaxis(product, -1, dimension)


def transform(spectra, dimension, direction):
    cosine, sine_table = tables(spectra.shape[dimension])
    inner_dim = dimension - 1
    real_part = spectra[:, 0]
    imag_part = spectra[:, 1]
    new_real = contract(real_part, cosine, inner_dim) - direction * contract(
        imag_part, sine_table, inner_dim
    )
    new_imag = contract(imag_part, cosine, inner_dim) + direction * contract(
        real_part, sine_table, inner_dim
    )
    result = jnp.stack([new_real, new_imag], 1)
    if direction > 0:
        result = result / spectra.shape[dimension]
    return result


def transform_y(pieces):
    return transform(pieces, 3, -1.0)


def transform_z(pieces):
    return transform(pieces, 2, -1.0)


def inverse_y(pieces):
    return transform(pieces, 3, 1.0)


def inverse_x_real(pieces):
    cosine, sine_table = tables(pieces.shape[4])
    real_part = contract(pieces[:, 0], cosine, 3) - contract(pieces[:, 1], sine_table, 3)
    return real_part / pieces.shape[4]


def forward(fields):
    cosine, sine_table = tables(fields.shape[3])
    spectra = jnp.stack([contract(fields, cosine, 3), -contract(fields, sine_table, 3)], 1)
    columns = transform_y(lax.all_to_all(spectra, "gy", split_axis=4, concat_axis=3, tiled=True))
    return transform_z(lax.all_to_all(columns, "gz", split_axis=3, concat_axis=2, tiled=True))


def inverse(spectra):
    local_z = transform(spectra, 2, 1.0)
    rows_back = inverse_y(lax.all_to_all(local_z, "gz", split_axis=2, concat_axis=3, tiled=True))
    return inverse_x_real(lax.all_to_all(rows_back, "gy", split_axis=3, concat_axis=4, tiled=True))


def poisson_weight(spectra):
    length = spectra.shape[2]
    y_block = spectra.shape[3]
    x_block = spectra.shape[4]
    wave_z = signed(jnp.arange(length, dtype=jnp.int32), length)
    wave_y = signed(lax.axis_index("gz") * y_block + jnp.arange(y_block, dtype=jnp.int32), length)
    wave_x = signed(lax.axis_index("gy") * x_block + jnp.arange(x_block, dtype=jnp.int32), length)
    squares = (
        wave_z[:, None, None] * wave_z[:, None, None]
        + wave_y[None, :, None] * wave_y[None, :, None]
        + wave_x[None, None, :] * wave_x[None, None, :]
    )
    scaled = (2.0 * jnp.pi / length) ** 2 * jnp.maximum(squares, 1).astype(jnp.float32)
    return jnp.where(squares > 0, 4.0 * jnp.pi / scaled, 0.0)


def total_intersections(own_terms):
    return lax.psum(own_terms, ("gz", "gy"))


def deposit_rims(atom_cell, atom_offset, atom_charge, atom_width, slab_z, slab_y, length):
    cell_ids = atom_cell.reshape(-1)
    local_z = cell_ids // (slab_y * length)
    local_y = cell_ids // length % slab_y
    local_x = cell_ids % length
    offsets = atom_offset.reshape(3, -1)
    dist_z = (jnp.arange(slab_z + 2 * RC, dtype=jnp.int32)[None, :] - RC - local_z[:, None]).astype(
        jnp.float32
    ) - offsets[0][:, None]
    dist_y = (jnp.arange(slab_y + 2 * RC, dtype=jnp.int32)[None, :] - RC - local_y[:, None]).astype(
        jnp.float32
    ) - offsets[1][:, None]
    dist_x = (
        signed(
            (jnp.arange(length, dtype=jnp.int32)[None, :] - local_x[:, None]) % length, length
        ).astype(jnp.float32)
        - offsets[2][:, None]
    )
    buffer_sum = gaussians(dist_z, dist_y, dist_x, atom_charge.reshape(-1), atom_width.reshape(-1))
    rims_z = jnp.concatenate([buffer_sum[:RC], buffer_sum[-RC:]], 0)
    near_z = with_halo(rims_z, (("gz", 0),), RC)
    middle = buffer_sum[RC : RC + slab_z]
    middle = middle.at[:RC].add(near_z[:RC]).at[slab_z - RC :].add(near_z[3 * RC :])
    rims_y = jnp.concatenate([middle[:, :RC], middle[:, -RC:]], 1)
    near_y = with_halo(rims_y, (("gy", 1),), RC)
    inside = middle[:, RC : RC + slab_y]
    return inside.at[:, :RC].add(near_y[:, :RC]).at[:, slab_y - RC :].add(near_y[:, 3 * RC :])


def local(coarse_density, density_in, history, atom_cell, atom_offset, atom_charge, atom_width):
    length = NF
    slab_z = density_in.shape[0]
    slab_y = density_in.shape[1] // length
    density_cube = density_in.reshape(slab_z, slab_y, length)
    history_cube = history.reshape(history.shape[0], slab_z, slab_y, length)
    extended = with_halo(coarse_density, (("gy", 1),), 2)
    coarse_rows = coarse_density.shape[0] // lax.axis_size("gz")
    beside_all = jnp.concatenate([extended[-2:], extended, extended[:2]], 0)
    start = lax.axis_index("gz") * coarse_rows
    own_planes = lax.dynamic_slice_in_dim(beside_all, start, coarse_rows + 4, 0)
    wrapped = jnp.concatenate([own_planes[:, :, -2:], own_planes, own_planes[:, :, :2]], 2)
    smooth = midpoint(wrapped, 2, coarse_density.shape[2])
    smooth = midpoint(smooth, 1, coarse_density.shape[1])
    smooth = midpoint(smooth, 0, coarse_rows)
    charge_field = deposit_rims(
        atom_cell, atom_offset, atom_charge, atom_width, slab_z, slab_y, length
    )
    residual = smooth + charge_field - density_cube
    cells_all = float(length) ** 3
    spectra = forward(residual[None])
    weight = poisson_weight(spectra)
    potential = inverse(weight * spectra)[0]
    own_terms = (
        jnp.concatenate(
            [
                jnp.sum(history_cube * potential[None], axis=(1, 2, 3)),
                jnp.sum(residual * potential)[None],
            ]
        )
        / cells_all
    )
    intersections = total_intersections(own_terms)
    return (
        residual.reshape(slab_z, slab_y * length),
        potential.reshape(slab_z, slab_y * length),
        intersections,
    )


GROUP = 16
LANES = 128
SUB = 8


def basis(length):
    half = length // 2
    wave = np.concatenate([np.arange(half + 1), np.arange(1, half)])
    angle = 2.0 * np.pi / length * (np.outer(wave, np.arange(length)) % length)
    rows = np.where(np.arange(length)[:, None] <= half, np.cos(angle), np.sin(angle))
    scale = np.where((wave == 0) | (wave == half), 1.0, np.sqrt(2.0)) / np.sqrt(length)
    return rows * scale[:, None], wave


def halves(values):
    high = values.astype(jnp.bfloat16)
    return high, (values - high.astype(jnp.float32)).astype(jnp.bfloat16)


def thirds(values):
    high = values.astype(jnp.bfloat16)
    rest = values - high.astype(jnp.float32)
    middle = rest.astype(jnp.bfloat16)
    return high, middle, (rest - middle.astype(jnp.float32)).astype(jnp.bfloat16)


NN = (((1,), (0,)), ((), ()))
NT = (((1,), (1,)), ((), ()))


def mm(left, right, dims):
    return lax.dot_general(left, right, dims, preferred_element_type=jnp.float32)


def mm3(left, right, dims=NN):
    rows = left[0].shape[0]
    both = mm(jnp.concatenate(left, 0), right[0], dims)
    return mm(left[0], right[1], dims) + both[rows:] + both[:rows]


def turn_tiles(tiles):
    row = lax.broadcasted_iota(jnp.int32, (SUB, LANES), 0)
    tiles = list(tiles)
    for step in (4, 2, 1):
        own = (row & step) == 0
        for i in range(SUB):
            if i & step == 0:
                first, second = tiles[i], tiles[i + step]
                tiles[i] = jnp.where(own, first, pltpu.roll(second, step, 0))
                tiles[i + step] = jnp.where(own, pltpu.roll(first, SUB - step, 0), second)
    return tiles


def slot(g, pair, k):
    if g < 7:
        return SUB * g + 2 * pair + k
    return SUB * (3 * (g - 7) + pair) + 6 + k


def fetch(pairs, sems, first=0):
    copies = [
        pltpu.make_async_copy(source, target, sems.at[first + i])
        for i, (source, target) in enumerate(pairs)
    ]
    for copy in copies:
        copy.start()
    return copies


def room(array):
    return pltpu.VMEM(array.shape, array.dtype)


SPARE = 54
PIECE = 40
FACTS = 3 * PIECE
VMEM_LIMIT = 60 * 1024 * 1024
LATE_LIMIT = 48 * 1024 * 1024


def tile_masks():
    row = lax.broadcasted_iota(jnp.int32, (SUB, LANES), 0)
    group = lax.broadcasted_iota(jnp.int32, (SUB, LANES), 1) // SUB
    return row, group


def rotate_up(upper, lower, masks):
    row, group = masks
    bit = (group & 8) != 0
    upper, lower = jnp.where(bit, lower, upper), jnp.where(bit, upper, lower)
    for shift in (4, 2, 1):
        bit = (group & shift) != 0
        roll_u = pltpu.roll(upper, SUB - shift, 0)
        roll_l = pltpu.roll(lower, SUB - shift, 0)
        stay = row < SUB - shift
        new_u = jnp.where(stay, roll_u, roll_l)
        new_l = jnp.where(stay, roll_l, roll_u)
        upper, lower = jnp.where(bit, new_u, upper), jnp.where(bit, new_l, lower)
    return upper, lower


def skew(values, start):
    return pltpu.roll(values, start, 1, stride=SUB, stride_axis=0)


def block_turn(upper, lower, masks):
    upper, lower = rotate_up(skew(upper, 0), skew(lower, 64), masks)
    return skew(upper, 0), skew(lower, 64)


class Plan:
    def __init__(self, mesh_shape, length, coarse, fz, fy):
        self.nz, self.ny = mesh_shape
        self.count = self.nz * self.ny
        self.length, self.coarse, self.fz, self.fy = length, coarse, fz, fy
        self.j = length // self.count
        self.zo, self.yo = fz // SUB, fy // GROUP
        self.rows_out = 56
        self.rows_back = 56
        self.ext = length + 32

    def ok(self):
        return (
            (self.nz, self.ny, self.zo, self.yo, self.j) == (8, 4, 3, 3, 6)
            and self.fz % SUB == 0
            and self.fy % GROUP == 0
            and self.length == self.coarse * 2
        )


def fast_tables(plan):
    length, nz = plan.length, plan.nz
    rows, wave = basis(length)
    fine_of = np.zeros((plan.coarse, length), np.float32)
    for i in range(plan.coarse):
        fine_of[i, 2 * i] += 1.0
        for step, value in ((0, 9), (1, 9), (-1, -1), (2, -1)):
            fine_of[(i + step) % plan.coarse, 2 * i + 1] += value / 16.0
    local_z = np.zeros((plan.fz, GROUP), np.float32)
    for i in range(plan.fz // 2):
        local_z[2 * i, i + 1] = 1.0
        for step, value in ((1, 9), (2, 9), (0, -1), (3, -1)):
            local_z[2 * i + 1, i + step] += value / 16.0

    def along_z(turn):
        half_of, owner = turn // SUB, turn % SUB
        lane = np.arange(SUB)
        z_main = (owner[:, None] * plan.fz + half_of[:, None] * SUB + lane[None]).reshape(-1)
        z_shared = (owner[:, None] * plan.fz + 2 * SUB + lane[None]).reshape(-1)
        odd = np.repeat(half_of, SUB)
        tables_z = []
        for parity in (0, 1):
            table = np.zeros((2 * LANES, length))
            table[:LANES] = rows[:, z_main].T
            table[LANES:] = np.where((odd == parity)[:, None], rows[:, z_shared].T, 0.0)
            tables_z.append(table)
        return tables_z

    z_tables = along_z(np.arange(GROUP))
    y_of_row = (np.arange(plan.ext) - SUB) % length
    count = plan.count
    x_window = np.zeros((count, length + GROUP, SUB), np.float32)
    x_of_row = (np.arange(length + GROUP) - SUB) % length
    padded = np.zeros((count, SUB, length))
    kept = np.zeros((count, SUB, length))
    donors = np.zeros((3, count, SUB, length))
    for d in range(count):
        for j in range(plan.j):
            mode = rows[j * count + d]
            x_window[d, :, j] = mode[x_of_row]
            padded[d, j] = kept[d, j] = mode
            donors[j // 2, d, 6 + j % 2] = mode
        padded[d, 6:] = padded[d, 4:6]
    flat = lambda table: table.reshape(count * SUB, length)
    def halves_of(table):
        table = np.asarray(table, np.float32)
        high = table.astype(jnp.bfloat16)
        return [high, (table - high.astype(np.float32)).astype(jnp.bfloat16)]

    def pack(tables_in):
        width = max(table.shape[-1] for table in tables_in)
        return jnp.asarray(
            np.concatenate(
                [
                    np.pad(table, ((0, 0), (0, width - table.shape[-1])))
                    for table in tables_in
                ],
                0,
            )
        )

    z_all = np.stack(z_tables).reshape(-1, length)
    coarse_z = fine_of.astype(np.float64) @ rows.T
    own = plan.coarse // nz
    edge_z = np.zeros((3, LANES, length))
    for a in range(nz):
        for edge in range(3):
            at = PIECE * (a % 3) + own * edge
            edge_z[a // 3, at : at + own] = coarse_z[a * own : (a + 1) * own]
    y_table = np.zeros((length, plan.ext + GROUP))
    y_table[:, : plan.ext] = rows[:, y_of_row]
    for b in range(plan.ny):
        at, y = plan.ext + 4 * b, b * plan.fy
        y_table[:, at] = (9.0 * rows[:, y - 1] - rows[:, y - 3]) / 16.0
        y_table[:, at + 1] = -rows[:, y - 1] / 16.0
        y_table[:, at + 2] = -rows[:, (y + plan.fy + 1) % length] / 16.0
    near = [np.kron(np.eye(SUB), local_z), fine_of]
    return {
        "a": pack(halves_of(flat(padded)) + [table.astype(jnp.bfloat16) for table in near]),
        "b": pack(
            halves_of(z_all)
            + halves_of(edge_z.reshape(-1, length))
            + halves_of(y_table)
            + halves_of(rows.T)
        ),
        "c": pack(halves_of(np.stack([flat(kept)] + [flat(donors[i]) for i in range(3)]).reshape(-1, length))),
        "window": jnp.asarray(x_window.reshape(count, 1, -1)),
    }


def near_tables(plan, near, first):
    kron_rows = SUB * plan.fz
    kron = near[first : first + kron_rows, :LANES]
    return kron, near[first + kron_rows : first + kron_rows + plan.coarse, :]


def part_a(plan, t):
    length, fz, fy, count = plan.length, plan.fz, plan.fy, plan.count
    rows_c = fy // 2
    per = plan.rows_out

    def kernel(
        cell_h, offset_h, charge_h, width_h, coarse_h, density_h, table_h, send_h, partial_h, after_h, before_h,
        cell, offset, charge, width, density, tables_v, send, partial, planes, smooth, field, after, before, sems,
    ):
        a = lax.axis_index("gz")
        b = lax.axis_index("gy")
        own = plan.coarse // plan.nz
        first = fetch(
            [
                (
                    coarse_h.at[lax.rem(own * a + plan.coarse - 1 + i, plan.coarse)],
                    planes.at[pl.ds(i * rows_c, rows_c), :],
                )
                for i in range(GROUP)
            ]
            + [(table_h, tables_v)],
            sems,
            10,
        )
        third = fy // plan.yo * length
        cuts = [slice(yo * third, (yo + 1) * third) for yo in range(plan.yo)]
        order = (2, 0, 1)
        second = {
            yo: fetch([(density_h.at[:, cuts[yo]], density.at[:, cuts[yo]])], sems, 30 + yo)[0]
            for yo in order
        }
        facts_in = fetch(
            [(cell_h, cell), (offset_h, offset), (charge_h, charge), (width_h, width)], sems, 4
        )
        for copy in first:
            copy.wait()
        kron, fine = near_tables(plan, tables_v, 2 * count * SUB)
        after[...] = planes[pl.ds(rows_c - 1, GROUP, stride=rows_c), :]
        for i in range(2):
            before[i * GROUP : (i + 1) * GROUP, :] = planes[pl.ds(i, GROUP, stride=rows_c), :]
        out_halo = fetch([(after, after_h), (before, before_h)], sems, 0)
        for part in range(rows_c // SUB):
            block = jnp.concatenate(
                [planes[pl.ds(part * SUB + y, GROUP, stride=rows_c), :] for y in range(SUB)], 0
            )
            wide = sum(mm(piece, fine, NN) for piece in thirds(block)[::-1])
            if part == 0:
                edges = [wide[i * GROUP + 1 : i * GROUP + 1 + own] for i in (0, 1)]
            if part == rows_c // SUB - 1:
                edges.append(wide[(SUB - 1) * GROUP + 1 : (SUB - 1) * GROUP + 1 + own])
            tall = sum(mm(kron, piece, NN) for piece in thirds(wide)[::-1])
            for y in range(SUB):
                smooth[part * SUB + y] = tall[y * fz : (y + 1) * fz]

        def row(i):
            return smooth[i] if 0 <= i < rows_c else jnp.zeros((fz, length), jnp.float32)

        def rows_of(yo):
            second[yo].wait()
            for i in range(yo * rows_c // plan.yo, (yo + 1) * rows_c // plan.yo):
                odd_row = (9.0 * (row(i) + row(i + 1)) - row(i - 1) - row(i + 2)) * (1.0 / 16.0)
                span = slice(2 * i * length, (2 * i + 2) * length)
                old = density[:, span]
                even_out = smooth[i] - old[:, :length]
                odd_out = odd_row - old[:, length:]
                field[2 * i] = even_out
                field[2 * i + 1] = odd_out
                partial[:, span] = jnp.concatenate([even_out, odd_out], 1)
            return fetch([(partial.at[:, cuts[yo]], partial_h.at[:, cuts[yo]])], sems, 33 + yo)

        table = (tables_v[: count * SUB, :], tables_v[count * SUB : 2 * count * SUB, :])
        sub_row = lax.broadcasted_iota(jnp.int32, (count, SUB, LANES), 1)

        def modes(block):
            out = mm3(table, halves(block), NT)
            return [
                out[:, g * LANES : (g + 1) * LANES].reshape(count, SUB, LANES)
                for g in range(out.shape[1] // LANES)
            ]

        for copy in facts_in:
            copy.wait()
        number = cell[0]
        plane = fy * length
        facts = (
            (a * fz + number // plane).astype(jnp.float32),
            (b * fy + lax.rem(number // length, fy)).astype(jnp.float32),
            lax.rem(number, length).astype(jnp.float32),
            offset[0],
            offset[1],
            offset[2],
            charge[0],
            width[0],
        )
        lane = lax.broadcasted_iota(jnp.int32, (count, SUB, LANES), 2)
        spare = jnp.zeros((count, SUB, LANES), jnp.float32)
        for i, fact in enumerate(facts):
            spare = jnp.where(lane == FACTS + i, fact, spare)
        gap = jnp.zeros((PIECE - 3 * own, length), jnp.float32)
        rest = jnp.zeros((LANES - FACTS, length), jnp.float32)
        edge_modes = modes(jnp.concatenate((edges + [gap]) * 3 + [rest], 0))[0]
        for j in range(plan.j):
            into = 6 + j // 3
            here = (lane // PIECE == j % 3) & (sub_row == into)
            spare = jnp.where(here, pltpu.roll(edge_modes, (into - j) % SUB, 1), spare)
        donor = None
        outs = []
        for yo in order:
            outs += rows_of(yo)
            block = jnp.concatenate(
                [
                    field[yo * GROUP + (-g) % GROUP, zo * SUB : (zo + 1) * SUB, :]
                    for zo in range(plan.zo)
                    for g in range(GROUP)
                ],
                0,
            )
            found = modes(block)
            if yo == 2:
                send[:, 48:56, :] = jnp.where(sub_row < 6, found[0], spare)
                donor = found[1:]
            else:
                for pair in range(3):
                    other = donor[yo]
                    if pair < 2:
                        other = pltpu.roll(other, 6 - 2 * pair, 1)
                    at = SUB * (3 * yo + pair)
                    send[:, at : at + SUB, :] = jnp.where(sub_row < 6, found[pair], other)
            span = slice(48, 56) if yo == 2 else slice(24 * yo, 24 * yo + 24)
            outs += fetch([(send.at[:, span, :], send_h.at[:, span, :])], sems, 27 + yo)
        for copy in out_halo + outs:
            copy.wait()

    hbm = pl.BlockSpec(memory_space=pltpu.HBM)
    return pl.pallas_call(
        kernel,
        name="spread",
        in_specs=[hbm] * 7,
        out_specs=[hbm] * 4,
        out_shape=[
            jax.ShapeDtypeStruct((count, per, LANES), jnp.float32),
            jax.ShapeDtypeStruct((fz, fy * length), jnp.float32),
            jax.ShapeDtypeStruct((GROUP, plan.coarse), jnp.float32),
            jax.ShapeDtypeStruct((2 * GROUP, plan.coarse), jnp.float32),
        ],
        compiler_params=pltpu.CompilerParams(vmem_limit_bytes=VMEM_LIMIT),
        scratch_shapes=[
            pltpu.SMEM((1,), jnp.int32),
            pltpu.SMEM((3,), jnp.float32),
            pltpu.SMEM((1,), jnp.float32),
            pltpu.SMEM((1,), jnp.float32),
            pltpu.VMEM((fz, fy * length), jnp.float32),
            room(t["a"]),
            pltpu.VMEM((count, per, LANES), jnp.float32),
            pltpu.VMEM((fz, fy * length), jnp.float32),
            pltpu.VMEM((GROUP * rows_c, plan.coarse), jnp.float32),
            pltpu.VMEM((rows_c, fz, length), jnp.float32),
            pltpu.VMEM((fy, fz, length), jnp.float32),
            pltpu.VMEM((GROUP, plan.coarse), jnp.float32),
            pltpu.VMEM((2 * GROUP, plan.coarse), jnp.float32),
            pltpu.SemaphoreType.DMA((36,)),
        ],
        cost_estimate=pl.CostEstimate(flops=500_000_000, bytes_accessed=4_000_000, transcendentals=0),
    )


def wrapped(distance, length):
    half = length // 2
    distance = jnp.where(distance >= half, distance - length, distance)
    return jnp.where(distance < -half, distance + length, distance)


def part_b(plan, t):
    length, count, ext = plan.length, plan.count, plan.ext
    per, per_back = plan.rows_out, plan.rows_back

    def kernel(
        window_h, recv_h, table_h, send_h,
        window, recv, tables_v, send, main, shared, bells, turned, ready, atoms_v, atoms, sem, sems, sems_in, sems_out,
    ):
        device = lax.axis_index("gz") * plan.ny + lax.axis_index("gy")

        def incoming(b):
            return pltpu.make_async_copy(recv_h.at[:, b], recv.at[:, b], sems_in.at[b])

        def outgoing(b):
            return pltpu.make_async_copy(send.at[:, b], send_h.at[:, b], sems_out.at[b])

        for b in range(plan.ny):
            incoming(b).start()
        copies = fetch(
            [
                (window_h.at[device], window),
                (table_h, tables_v),
            ],
            sems,
        )
        def unpack(b, carry):
            incoming(b).wait()
            for t in range(per // SUB):
                tiles = turn_tiles(
                    [recv[a, b, t * SUB : (t + 1) * SUB, :] for a in range(plan.nz)]
                )
                for i, tile in enumerate(tiles):
                    turned[b, t * SUB + i] = tile
            atoms_v[pl.ds(pl.multiple_of(b * SUB, SUB), SUB), :] = turned[b, SPARE]
            return carry

        lax.fori_loop(0, plan.ny, unpack, 0)
        copy = pltpu.make_async_copy(atoms_v, atoms, sem)
        copy.start()
        masks = tile_masks()
        bells[...] = jnp.zeros_like(bells)
        def gather(jp, b):
            for yo in range(plan.yo):
                tiles = []
                for k in (0, 1):
                    for zo in range(plan.zo):
                        tile = turned[b, slot(yo * plan.zo + zo, jp, k)]
                        tiles.append(tile)
                at = pl.multiple_of(b * plan.fy + yo * GROUP, SUB)
                for k in (0, 1):
                    upper, lower = block_turn(tiles[3 * k], tiles[3 * k + 1], masks)
                    main[2 * jp + k, pl.ds(at, SUB), :] = upper
                    main[2 * jp + k, pl.ds(at + SUB, SUB), :] = lower
                upper, lower = block_turn(tiles[2], tiles[5], masks)
                shared[jp, pl.ds(at, SUB), :] = upper
                shared[jp, pl.ds(at + SUB, SUB), :] = lower
        def gather_alone(b, carry):
            gather(0, b)
            return carry

        lax.fori_loop(0, plan.ny, gather_alone, 0)
        copy.wait()
        copies[0].wait()
        lane = lax.broadcasted_iota(jnp.int32, (1, LANES), 1)
        block = lane // SUB
        odd = block >= SUB
        z_first = (block & (SUB - 1)) * plan.fz + (lane & (SUB - 1))
        z_main = (z_first + jnp.where(odd, SUB, 0)).astype(jnp.float32)
        z_shared = (z_first + 2 * SUB).astype(jnp.float32)
        window_rows = lax.broadcasted_iota(jnp.int32, (GROUP, LANES), 0).astype(jnp.float32) - RC

        def deposit(i):
            z0, y0, x0, off_z, off_y, off_x, charge, width = (atoms[i, FACTS + f] for f in range(8))
            ratio = jnp.full((SUB, LANES), width / jnp.pi, jnp.float32)
            factor = ratio * jnp.sqrt(ratio) * charge
            factor = factor[0:1]
            cut = jnp.exp(jnp.full((SUB, LANES), -width * float(RC * RC), jnp.float32))[0:1]
            profile_y = jnp.exp(-width * (window_rows - off_y) ** 2)
            profile_x = jnp.exp(-width * (window_rows - off_x) ** 2)
            planes = []
            for z in (z_main, z_shared):
                profile_z = jnp.exp(-width * (wrapped(z - z0, length) - off_z) ** 2)
                planes.append(profile_y * profile_z)
            base = (x0.astype(jnp.int32) - RC + SUB) * SUB
            zero = jnp.zeros((GROUP, LANES), jnp.float32)
            sums = [[zero, zero, zero] for _ in range(plan.j // 2)]
            for dx in range(2 * RC + 2):
                line = profile_x[dx : dx + 1]
                bell = [jnp.maximum(plane * line - cut, 0.0) for plane in planes]
                for jp in range(plan.j // 2):
                    even = window[0, base + dx * SUB + 2 * jp]
                    odd_value = window[0, base + dx * SUB + 2 * jp + 1]
                    sums[jp][0] += bell[0] * even
                    sums[jp][1] += bell[0] * odd_value
                    sums[jp][2] += bell[1] * jnp.where(odd, odd_value, even)
            at = y0.astype(jnp.int32) - RC + SUB
            for jp in range(plan.j // 2):
                for k in (0, 1):
                    bells[2 * jp + k, pl.ds(at, GROUP), :] += sums[jp][k] * factor
                bells[plan.j + jp, pl.ds(at, GROUP), :] += sums[jp][2] * factor

        steps = plan.ny * (plan.j // 2 - 1)

        def gather_and_deposit(step, carry):
            for i in range(count // steps):
                deposit(step * (count // steps) + i)
            gather(1 + step // plan.ny, lax.rem(step, plan.ny))
            return carry

        lax.fori_loop(0, steps, gather_and_deposit, 0)
        for item in copies[1:]:
            item.wait()
        scale = float(length) ** 2 / math.pi
        half = length // 2

        def square(mode):
            wave = jnp.where(mode <= half, mode, mode - half)
            return (wave * wave).astype(jnp.float32)

        plane = square(lax.broadcasted_iota(jnp.int32, (length, length), 0)) + square(
            lax.broadcasted_iota(jnp.int32, (length, length), 1)
        )
        zt, et, yt, yti = [], [], [], []
        at = 0
        for into, size, width, parts in (
            (zt, 2 * LANES, length, 2),
            (et, 3 * LANES, length, 1),
            (yt, length, ext + GROUP, 1),
            (yti, length, length, 1),
        ):
            for half_index in range(2):
                into.append(
                    [tables_v[at + i * size : at + (i + 1) * size, :width] for i in range(parts)]
                )
                at += parts * size
        edge_row = lax.broadcasted_iota(jnp.int32, (GROUP, LANES), 0)
        edge_lane = lax.broadcasted_iota(jnp.int32, (GROUP, LANES), 1)
        own = plan.coarse // plan.nz
        first_lane = own * (edge_row & 3)
        lines = []
        for row in range(2):
            spread = [turned[b, SPARE + row] for b in range(plan.ny)]
            for q in range(3):
                blocks = []
                for a in range(plan.nz):
                    if a % 3 == 0:
                        blocks.append(jnp.zeros((GROUP, LANES), jnp.float32))
                    line = jnp.concatenate(
                        [jnp.broadcast_to(tile[a : a + 1], (4, LANES)) for tile in spread], 0
                    )
                    shift = (PIECE * (a % 3 - q)) % LANES
                    line = pltpu.roll(line, shift, 1) if shift else line
                    start = first_lane + PIECE * (a % 3)
                    keep = (edge_lane >= start) & (edge_lane < start + own) & ((edge_row & 3) < 3)
                    blocks[-1] = jnp.where(keep, line, blocks[-1])
                lines.append(jnp.concatenate(blocks, 1))
        edges_z = mm3(halves(jnp.concatenate(lines, 0)), (et[0][0], et[1][0]))
        def with_bells(block, index):
            top, last = SUB, SUB + length
            return jnp.concatenate(
                [
                    bells[index, :top, :],
                    block + bells[index, top:last, :],
                    bells[index, last:, :],
                ],
                0,
            )

        backs = []
        energy = jnp.zeros((SUB, length), jnp.float32)
        for k in (0, 1):
            left = jnp.concatenate(
                [
                    jnp.concatenate(
                        [with_bells(main[2 * jp + k], 2 * jp + k), with_bells(shared[jp], plan.j + jp)],
                        1,
                    )
                    for jp in range(plan.j // 2)
                ],
                0,
            )
            rows_z = mm3(halves(left), (zt[0][k], zt[1][k]))
            rows_y = []
            for jp in range(plan.j // 2):
                j = 2 * jp + k
                column = jnp.concatenate(
                    [rows_z[jp * ext : (jp + 1) * ext], edges_z[j * GROUP : (j + 1) * GROUP]], 0
                )
                full = mm3((yt[0][0], yt[1][0]), halves(column))
                squares = plane + square((2 * jp + k) * count + device)
                weight = jnp.where(squares > 0.0, scale / jnp.maximum(squares, 1.0), 0.0)
                weighted = full * weight
                product = full * weighted
                for i in range(length // SUB):
                    energy += product[i * SUB : (i + 1) * SUB]
                rows_y.append(mm3((yti[0][0], yti[1][0]), halves(weighted)))
            backs.append(mm3(halves(jnp.concatenate(rows_y, 0)), (zt[0][k], zt[1][k]), NT))
        for jp in range(plan.j // 2):
            here = slice(jp * length, (jp + 1) * length)
            for k in (0, 1):
                main[2 * jp + k] = backs[k][here, :LANES]
            shared[jp] = backs[0][here, LANES:] + backs[1][here, LANES:]

        first = masks[0] == 0

        def scatter(step, carry):
            jp = step // plan.ny
            b = lax.rem(step, plan.ny)
            for yo in range(plan.yo):
                at = pl.multiple_of(b * plan.fy + yo * GROUP, SUB)
                found = []
                for source in (main.at[2 * jp], main.at[2 * jp + 1], shared.at[jp]):
                    upper, lower = block_turn(
                        source[pl.ds(at, SUB), :], source[pl.ds(at + SUB, SUB), :], masks
                    )
                    found.append(
                        (jnp.where(first, upper, lower), jnp.where(first, lower, upper))
                    )
                for k in (0, 1):
                    for zo, tile in enumerate((found[k][0], found[k][1], found[2][k])):
                        ready[b, slot(yo * plan.zo + zo, jp, k)] = tile
            return carry

        lax.fori_loop(0, plan.ny * (plan.j // 2), scatter, 0)

        share = jnp.sum(energy) * (1.0 / count)

        def pack(b, carry):
            for row in (SPARE, SPARE + 1):
                ready[b, row] = jnp.full((SUB, LANES), share, jnp.float32)
            for t in range(per_back // SUB):
                tiles = turn_tiles([ready[b, t * SUB + i] for i in range(SUB)])
                for i, tile in enumerate(tiles):
                    a = (SUB - i) % SUB
                    send[a, b, t * SUB : (t + 1) * SUB, :] = tile
            outgoing(b).start()
            return carry

        lax.fori_loop(0, plan.ny, pack, 0)
        for b in range(plan.ny):
            outgoing(b).wait()

    hbm = pl.BlockSpec(memory_space=pltpu.HBM)
    vmem = pl.BlockSpec(memory_space=pltpu.VMEM)
    return pl.pallas_call(
        kernel,
        name="solve",
        in_specs=[hbm, hbm, hbm],
        out_specs=hbm,
        out_shape=jax.ShapeDtypeStruct((plan.nz, plan.ny, per_back, LANES), jnp.float32),
        compiler_params=pltpu.CompilerParams(vmem_limit_bytes=VMEM_LIMIT),
        scratch_shapes=[
            pltpu.SMEM(t["window"].shape[1:], jnp.float32),
            pltpu.VMEM((plan.nz, plan.ny, per, LANES), jnp.float32),
            room(t["b"]),
            pltpu.VMEM((plan.nz, plan.ny, per_back, LANES), jnp.float32),
            pltpu.VMEM((plan.j, length, LANES), jnp.float32),
            pltpu.VMEM((plan.j // 2, length, LANES), jnp.float32),
            pltpu.VMEM((plan.j + plan.j // 2, ext, LANES), jnp.float32),
            pltpu.VMEM((plan.ny, per, SUB, LANES), jnp.float32),
            pltpu.VMEM((plan.ny, per_back, SUB, LANES), jnp.float32),
            pltpu.VMEM((count, LANES), jnp.float32),
            pltpu.SMEM((count, LANES), jnp.float32),
            pltpu.SemaphoreType.DMA,
            pltpu.SemaphoreType.DMA((2,)),
            pltpu.SemaphoreType.DMA((plan.ny,)),
            pltpu.SemaphoreType.DMA((plan.ny,)),
        ],
        cost_estimate=pl.CostEstimate(flops=2_000_000_000, bytes_accessed=4_000_000, transcendentals=0),
    )


def part_r(plan, t):
    length, fz, fy, count = plan.length, plan.fz, plan.fy, plan.count
    per = plan.rows_out

    def kernel(
        recv, partial_h, below_h, above_h, table_h, out_h,
        partial, tables_v, out, field, lines, atoms_v, atoms, sem, sems,
    ):
        lines[...] = jnp.zeros_like(lines)
        copies = fetch(
            [
                (partial_h, partial),
                (table_h, tables_v),
                (below_h, lines.at[pl.ds(0, GROUP), :]),
                (above_h, lines.at[pl.ds(GROUP, 2 * GROUP), :]),
            ],
            sems,
        )
        a = lax.axis_index("gz")
        b = lax.axis_index("gy")
        for i in range(count):
            atoms_v[i : i + 1, :] = recv[i, SPARE : SPARE + 1, :]
        copy = pltpu.make_async_copy(atoms_v, atoms, sem)
        copy.start()
        for item in copies:
            item.wait()
        kron, fine = near_tables(plan, tables_v, 2 * count * SUB)
        block = lines[...]
        wide = sum(mm(piece, fine, NN) for piece in thirds(block)[::-1])
        tall = sum(mm(kron, piece, NN) for piece in thirds(wide)[::-1])
        below, above, above2 = (tall[i * fz : (i + 1) * fz] for i in range(3))
        field[...] = jnp.zeros_like(field)
        field[1] = below * (-1.0 / 16.0)
        field[fy - 3] = above * (-1.0 / 16.0)
        field[fy - 1] = (9.0 * above - above2) * (1.0 / 16.0)
        copy.wait()
        z_here = lax.broadcasted_iota(jnp.int32, (fz, length), 0).astype(jnp.float32)
        x_here = lax.broadcasted_iota(jnp.int32, (fz, length), 1).astype(jnp.float32)

        def deposit(i, carry):
            z0 = wrapped(atoms[i, FACTS + 0] - (a * fz).astype(jnp.float32), length)
            y0 = wrapped(atoms[i, FACTS + 1] - (b * fy).astype(jnp.float32), length).astype(jnp.int32)
            first = jnp.maximum(y0 - RC, 0)
            last = jnp.minimum(y0 + RC + 2, fy)
            near_z = (z0 > -RC - 2.0) & (z0 < fz + RC + 1.0)

            @pl.when(near_z & (first < last))
            def _():
                off_z, off_y, off_x = atoms[i, FACTS + 3], atoms[i, FACTS + 4], atoms[i, FACTS + 5]
                charge, width = atoms[i, FACTS + 6], atoms[i, FACTS + 7]
                ratio = jnp.full((fz, length), width / jnp.pi, jnp.float32)
                factor = ratio * jnp.sqrt(ratio) * charge
                cut = jnp.exp(jnp.full((fz, length), -width * float(RC * RC), jnp.float32))
                dist_z = z_here - z0 - off_z
                dist_x = wrapped(x_here - atoms[i, FACTS + 2], length) - off_x
                flat = dist_z * dist_z + dist_x * dist_x

                def row(y, inner):
                    dist_y = (y - y0).astype(jnp.float32) - off_y
                    bell = jnp.maximum(jnp.exp(-width * (flat + dist_y * dist_y)) - cut, 0.0)
                    field[y] += bell * factor
                    return inner

                lax.fori_loop(first, last, row, 0)

            return carry

        lax.fori_loop(0, count, deposit, 0)
        for i in range(fy // 2):
            span = slice(2 * i * length, (2 * i + 2) * length)
            out[:, span] = partial[:, span] + jnp.concatenate([field[2 * i], field[2 * i + 1]], 1)
        for item in fetch([(out, out_h)], sems, 4):
            item.wait()

    hbm = pl.BlockSpec(memory_space=pltpu.HBM)
    vmem = pl.BlockSpec(memory_space=pltpu.VMEM)
    return pl.pallas_call(
        kernel,
        name="finish",
        compiler_params=pltpu.CompilerParams(vmem_limit_bytes=VMEM_LIMIT),
        in_specs=[vmem] + [hbm] * 4,
        out_specs=hbm,
        out_shape=jax.ShapeDtypeStruct((fz, fy * length), jnp.float32),
        scratch_shapes=[
            pltpu.VMEM((fz, fy * length), jnp.float32),
            room(t["a"]),
            pltpu.VMEM((fz, fy * length), jnp.float32),
            pltpu.VMEM((fy, fz, length), jnp.float32),
            pltpu.VMEM((SUB * GROUP, plan.coarse), jnp.float32),
            pltpu.VMEM((count, LANES), jnp.float32),
            pltpu.SMEM((count, LANES), jnp.float32),
            pltpu.SemaphoreType.DMA,
            pltpu.SemaphoreType.DMA((5,)),
        ],
        cost_estimate=pl.CostEstimate(flops=3_000_000_000, bytes_accessed=4_000_000, transcendentals=0),
    )


def part_c(plan, t, terms):
    length, fz, fy, count = plan.length, plan.fz, plan.fy, plan.count
    per = plan.rows_back
    wide = 3 * LANES

    def kernel(
        recv, table_h, history_h, potential_h, sums, tables_v, history, potential, sems
    ):
        first = fetch([(table_h, tables_v)], sems)
        copies = fetch([(history_h.at[i], history.at[i]) for i in range(terms)], sems, 2)
        first[0].wait()
        size = count * SUB
        xb = [
            [tables_v[(4 * h + i) * size : (4 * h + i + 1) * size, :] for i in range(4)]
            for h in range(2)
        ]
        def modes(t):
            return halves(recv[:, t * SUB : (t + 1) * SUB, :].reshape(count * SUB, LANES).T)

        def place(block, values):
            yo, zo = block // plan.zo, block % plan.zo
            for pair in range(GROUP // 2):
                at = (yo * GROUP + 2 * pair) * length
                rows = values[2 * pair * SUB : (2 * pair + 2) * SUB]
                potential[zo * SUB : (zo + 1) * SUB, at : at + 2 * length] = jnp.concatenate(
                    [rows[:SUB], rows[SUB:]], 1
                )

        given = [None, None]
        for t in range(per // SUB):
            left = modes(t)
            place(t, mm3(left, (xb[0][0], xb[1][0])))
            if t < 6:
                part = mm3(left, (xb[0][1 + t % 3], xb[1][1 + t % 3]))
                given[t // 3] = part if given[t // 3] is None else given[t // 3] + part
        place(7, given[0])
        place(8, given[1])
        out = fetch([(potential, potential_h)], sems, 2 + terms)
        acc = []
        for i in range(terms):
            def add(c, total, i=i):
                cut = pl.ds(pl.multiple_of(c * wide, LANES), wide)
                return total + history[i, :, cut] * potential[:, cut]

            copies[i].wait()
            acc.append(
                lax.fori_loop(
                    0, fy * length // wide, add, jnp.zeros((fz, wide), jnp.float32), unroll=4
                )
            )
        lane = lax.broadcasted_iota(jnp.int32, (1, LANES), 1)
        line = jnp.zeros((1, LANES), jnp.float32)
        for i in range(terms):
            line = jnp.where(lane == i, jnp.sum(acc[i]), line)
        own = jnp.sum(recv[:, SPARE : SPARE + 1, :], axis=0)
        line = jnp.where(lane == terms, own, line)
        sums[...] = jnp.broadcast_to(line * (1.0 / float(length) ** 3), (count, LANES))
        out[0].wait()

    hbm = pl.BlockSpec(memory_space=pltpu.HBM)
    vmem = pl.BlockSpec(memory_space=pltpu.VMEM)
    return pl.pallas_call(
        kernel,
        name="finish_potential",
        in_specs=[vmem, hbm, hbm],
        out_specs=[hbm, vmem],
        scratch_shapes=[
            room(t["c"]),
            pltpu.VMEM((terms, fz, fy * length), jnp.float32),
            pltpu.VMEM((fz, fy * length), jnp.float32),
            pltpu.SemaphoreType.DMA((3 + terms,)),
        ],
        out_shape=[
            jax.ShapeDtypeStruct((fz, fy * length), jnp.float32),
            jax.ShapeDtypeStruct((count, LANES), jnp.float32),
        ],
        compiler_params=pltpu.CompilerParams(vmem_limit_bytes=LATE_LIMIT),
        cost_estimate=pl.CostEstimate(flops=500_000_000, bytes_accessed=10_000_000, transcendentals=0),
    )


def exchange(sent, axes):
    return lax.all_to_all(sent, axes, 0, 0, tiled=True)


def local_fast(plan, coarse_density, density_in, history, atom_cell, atom_offset, atom_charge, atom_width):
    axes = ("gz", "gy")
    count = plan.count
    tables_ = fast_tables(plan)
    sent, partial, after, before = part_a(plan, tables_)(
        atom_cell.reshape(1),
        atom_offset.reshape(3),
        atom_charge.reshape(1),
        atom_width.reshape(1),
        coarse_density,
        density_in,
        tables_["a"],
    )
    spectra = exchange(sent, axes)
    solved = part_b(plan, tables_)(
        tables_["window"],
        spectra.reshape((plan.nz, plan.ny) + spectra.shape[1:]),
        tables_["b"],
    )
    back = exchange(solved.reshape((count,) + solved.shape[2:]), axes)
    ring = [(i, (i + 1) % plan.ny) for i in range(plan.ny)]
    below = lax.ppermute(after, "gy", ring)
    above = lax.ppermute(before, "gy", [(target, source) for source, target in ring])
    residual = part_r(plan, tables_)(spectra, partial, below, above, tables_["a"])
    potential, sums = part_c(plan, tables_, history.shape[0])(back, tables_["c"], history)
    rows = lax.all_to_all(sums, axes, 0, 0, tiled=True)
    return residual, potential, jnp.sum(rows, 0)[: history.shape[0] + 1]


def solution(mesh):
    in_specs = (
        P(None, "gy", None),
        P("gz", "gy"),
        P(None, "gz", "gy"),
        P("gz", "gy", None),
        P(None, "gz", "gy", None),
        P("gz", "gy", None),
        P("gz", "gy", None),
    )
    out_specs = (P("gz", "gy"), P("gz", "gy"), P())

    def body(*arguments):
        coarse_density, density_in = arguments[:2]
        plan = Plan(
            (mesh.shape["gz"], mesh.shape["gy"]),
            2 * coarse_density.shape[0],
            coarse_density.shape[0],
            density_in.shape[0],
            2 * coarse_density.shape[1],
        )
        if plan.ok():
            return local_fast(plan, *arguments)
        return local(*arguments)

    return jax.shard_map(body, mesh=mesh, in_specs=in_specs, out_specs=out_specs, check_vma=False)
```

```python
import math

import jax
import jax.numpy as jnp
import numpy as np
from jax import lax
from jax.experimental import pallas as pl
from jax.experimental.pallas import tpu as pltpu
from jax.sharding import PartitionSpec as P

RC = 4
NF = 192


def with_halo(block, sides, width):
    for axis, dim in sides:
        count = lax.axis_size(axis)
        forward = [(i, i + 1) for i in range(count - 1)]
        forward.append((count - 1, 0))
        backward = [(target, source) for source, target in forward]
        low = lax.ppermute(
            lax.slice_in_dim(block, block.shape[dim] - width, None, axis=dim), axis, forward
        )
        high = lax.ppermute(lax.slice_in_dim(block, 0, width, axis=dim), axis, backward)
        block = jnp.concatenate([low, block, high], axis=dim)
    return block


def midpoint(extended, dimension, cells_in):

    def window(offset):
        return lax.slice_in_dim(extended, offset, offset + cells_in, axis=dimension)

    even_cells = window(2)
    odd_cells = (9.0 * (window(2) + window(3)) - window(1) - window(4)) / 16.0
    merged = jnp.stack([even_cells, odd_cells], dimension + 1)
    new_shape = list(even_cells.shape)
    new_shape[dimension] = 2 * cells_in
    return merged.reshape(new_shape)


def signed(counter, length):
    return jnp.where(counter < length // 2, counter, counter - length)


def shape_value(squared, charge, exponent):
    factor = charge * (exponent / jnp.pi) ** 1.5
    return factor * jnp.maximum(
        jnp.exp(-exponent * squared) - jnp.exp(-exponent * float(RC * RC)), 0.0
    )


def gaussians(dist_z, dist_y, dist_x, charge, exponent):
    squared = (
        dist_z[:, :, None, None] ** 2
        + dist_y[:, None, :, None] ** 2
        + dist_x[:, None, None, :] ** 2
    )
    return jnp.sum(
        shape_value(squared, charge[:, None, None, None], exponent[:, None, None, None]), 0
    )


def tables(length):
    counter = jnp.arange(length, dtype=jnp.int32)
    phase = counter[:, None] * counter[None, :] % length
    angle = 2.0 * jnp.pi / length * phase.astype(jnp.float32)
    return (jnp.cos(angle), jnp.sin(angle))


def contract(values, table, dimension):
    product = jnp.tensordot(values, table, axes=([dimension], [0]), precision=lax.Precision.HIGHEST)
    return jnp.moveaxis(product, -1, dimension)


def transform(spectra, dimension, direction):
    cosine, sine_table = tables(spectra.shape[dimension])
    inner_dim = dimension - 1
    real_part = spectra[:, 0]
    imag_part = spectra[:, 1]
    new_real = contract(real_part, cosine, inner_dim) - direction * contract(
        imag_part, sine_table, inner_dim
    )
    new_imag = contract(imag_part, cosine, inner_dim) + direction * contract(
        real_part, sine_table, inner_dim
    )
    result = jnp.stack([new_real, new_imag], 1)
    if direction > 0:
        result = result / spectra.shape[dimension]
    return result


def transform_y(pieces):
    return transform(pieces, 3, -1.0)


def transform_z(pieces):
    return transform(pieces, 2, -1.0)


def inverse_y(pieces):
    return transform(pieces, 3, 1.0)


def inverse_x_real(pieces):
    cosine, sine_table = tables(pieces.shape[4])
    real_part = contract(pieces[:, 0], cosine, 3) - contract(pieces[:, 1], sine_table, 3)
    return real_part / pieces.shape[4]


def forward(fields):
    cosine, sine_table = tables(fields.shape[3])
    spectra = jnp.stack([contract(fields, cosine, 3), -contract(fields, sine_table, 3)], 1)
    columns = transform_y(lax.all_to_all(spectra, "gy", split_axis=4, concat_axis=3, tiled=True))
    return transform_z(lax.all_to_all(columns, "gz", split_axis=3, concat_axis=2, tiled=True))


def inverse(spectra):
    local_z = transform(spectra, 2, 1.0)
    rows_back = inverse_y(lax.all_to_all(local_z, "gz", split_axis=2, concat_axis=3, tiled=True))
    return inverse_x_real(lax.all_to_all(rows_back, "gy", split_axis=3, concat_axis=4, tiled=True))


def poisson_weight(spectra):
    length = spectra.shape[2]
    y_block = spectra.shape[3]
    x_block = spectra.shape[4]
    wave_z = signed(jnp.arange(length, dtype=jnp.int32), length)
    wave_y = signed(lax.axis_index("gz") * y_block + jnp.arange(y_block, dtype=jnp.int32), length)
    wave_x = signed(lax.axis_index("gy") * x_block + jnp.arange(x_block, dtype=jnp.int32), length)
    squares = (
        wave_z[:, None, None] * wave_z[:, None, None]
        + wave_y[None, :, None] * wave_y[None, :, None]
        + wave_x[None, None, :] * wave_x[None, None, :]
    )
    scaled = (2.0 * jnp.pi / length) ** 2 * jnp.maximum(squares, 1).astype(jnp.float32)
    return jnp.where(squares > 0, 4.0 * jnp.pi / scaled, 0.0)


def total_intersections(own_terms):
    return lax.psum(own_terms, ("gz", "gy"))


def deposit_rims(atom_cell, atom_offset, atom_charge, atom_width, slab_z, slab_y, length):
    cell_ids = atom_cell.reshape(-1)
    local_z = cell_ids // (slab_y * length)
    local_y = cell_ids // length % slab_y
    local_x = cell_ids % length
    offsets = atom_offset.reshape(3, -1)
    dist_z = (jnp.arange(slab_z + 2 * RC, dtype=jnp.int32)[None, :] - RC - local_z[:, None]).astype(
        jnp.float32
    ) - offsets[0][:, None]
    dist_y = (jnp.arange(slab_y + 2 * RC, dtype=jnp.int32)[None, :] - RC - local_y[:, None]).astype(
        jnp.float32
    ) - offsets[1][:, None]
    dist_x = (
        signed(
            (jnp.arange(length, dtype=jnp.int32)[None, :] - local_x[:, None]) % length, length
        ).astype(jnp.float32)
        - offsets[2][:, None]
    )
    buffer_sum = gaussians(dist_z, dist_y, dist_x, atom_charge.reshape(-1), atom_width.reshape(-1))
    rims_z = jnp.concatenate([buffer_sum[:RC], buffer_sum[-RC:]], 0)
    near_z = with_halo(rims_z, (("gz", 0),), RC)
    middle = buffer_sum[RC : RC + slab_z]
    middle = middle.at[:RC].add(near_z[:RC]).at[slab_z - RC :].add(near_z[3 * RC :])
    rims_y = jnp.concatenate([middle[:, :RC], middle[:, -RC:]], 1)
    near_y = with_halo(rims_y, (("gy", 1),), RC)
    inside = middle[:, RC : RC + slab_y]
    return inside.at[:, :RC].add(near_y[:, :RC]).at[:, slab_y - RC :].add(near_y[:, 3 * RC :])


def local(coarse_density, density_in, history, atom_cell, atom_offset, atom_charge, atom_width):
    length = NF
    slab_z = density_in.shape[0]
    slab_y = density_in.shape[1] // length
    density_cube = density_in.reshape(slab_z, slab_y, length)
    history_cube = history.reshape(history.shape[0], slab_z, slab_y, length)
    extended = with_halo(coarse_density, (("gy", 1),), 2)
    coarse_rows = coarse_density.shape[0] // lax.axis_size("gz")
    beside_all = jnp.concatenate([extended[-2:], extended, extended[:2]], 0)
    start = lax.axis_index("gz") * coarse_rows
    own_planes = lax.dynamic_slice_in_dim(beside_all, start, coarse_rows + 4, 0)
    wrapped = jnp.concatenate([own_planes[:, :, -2:], own_planes, own_planes[:, :, :2]], 2)
    smooth = midpoint(wrapped, 2, coarse_density.shape[2])
    smooth = midpoint(smooth, 1, coarse_density.shape[1])
    smooth = midpoint(smooth, 0, coarse_rows)
    charge_field = deposit_rims(
        atom_cell, atom_offset, atom_charge, atom_width, slab_z, slab_y, length
    )
    residual = smooth + charge_field - density_cube
    cells_all = float(length) ** 3
    spectra = forward(residual[None])
    weight = poisson_weight(spectra)
    potential = inverse(weight * spectra)[0]
    own_terms = (
        jnp.concatenate(
            [
                jnp.sum(history_cube * potential[None], axis=(1, 2, 3)),
                jnp.sum(residual * potential)[None],
            ]
        )
        / cells_all
    )
    intersections = total_intersections(own_terms)
    return (
        residual.reshape(slab_z, slab_y * length),
        potential.reshape(slab_z, slab_y * length),
        intersections,
    )


GROUP = 16
LANES = 128
SUB = 8


def basis(length):
    half = length // 2
    wave = np.concatenate([np.arange(half + 1), np.arange(1, half)])
    angle = 2.0 * np.pi / length * (np.outer(wave, np.arange(length)) % length)
    rows = np.where(np.arange(length)[:, None] <= half, np.cos(angle), np.sin(angle))
    scale = np.where((wave == 0) | (wave == half), 1.0, np.sqrt(2.0)) / np.sqrt(length)
    return rows * scale[:, None], wave


def halves(values):
    high = values.astype(jnp.bfloat16)
    return high, (values - high.astype(jnp.float32)).astype(jnp.bfloat16)


def thirds(values):
    high = values.astype(jnp.bfloat16)
    rest = values - high.astype(jnp.float32)
    middle = rest.astype(jnp.bfloat16)
    return high, middle, (rest - middle.astype(jnp.float32)).astype(jnp.bfloat16)


NN = (((1,), (0,)), ((), ()))
NT = (((1,), (1,)), ((), ()))


def mm(left, right, dims):
    return lax.dot_general(left, right, dims, preferred_element_type=jnp.float32)


def mm3(left, right, dims=NN):
    rows = left[0].shape[0]
    both = mm(jnp.concatenate(left, 0), right[0], dims)
    return mm(left[0], right[1], dims) + both[rows:] + both[:rows]


def turn_tiles(tiles):
    row = lax.broadcasted_iota(jnp.int32, (SUB, LANES), 0)
    tiles = list(tiles)
    for step in (4, 2, 1):
        own = (row & step) == 0
        for i in range(SUB):
            if i & step == 0:
                first, second = tiles[i], tiles[i + step]
                tiles[i] = jnp.where(own, first, pltpu.roll(second, step, 0))
                tiles[i + step] = jnp.where(own, pltpu.roll(first, SUB - step, 0), second)
    return tiles


def slot(g, pair, k):
    if g < 7:
        return SUB * g + 2 * pair + k
    return SUB * (3 * (g - 7) + pair) + 6 + k


def fetch(pairs, sems, first=0):
    copies = [
        pltpu.make_async_copy(source, target, sems.at[first + i])
        for i, (source, target) in enumerate(pairs)
    ]
    for copy in copies:
        copy.start()
    return copies


def room(array):
    return pltpu.VMEM(array.shape, array.dtype)


SPARE = 54
PIECE = 40
FACTS = 3 * PIECE
VMEM_LIMIT = 60 * 1024 * 1024
EARLY = 2
LATE_LIMIT = 48 * 1024 * 1024


def tile_masks():
    row = lax.broadcasted_iota(jnp.int32, (SUB, LANES), 0)
    group = lax.broadcasted_iota(jnp.int32, (SUB, LANES), 1) // SUB
    return row, group


def rotate_up(upper, lower, masks):
    row, group = masks
    bit = (group & 8) != 0
    upper, lower = jnp.where(bit, lower, upper), jnp.where(bit, upper, lower)
    for shift in (4, 2, 1):
        bit = (group & shift) != 0
        roll_u = pltpu.roll(upper, SUB - shift, 0)
        roll_l = pltpu.roll(lower, SUB - shift, 0)
        stay = row < SUB - shift
        new_u = jnp.where(stay, roll_u, roll_l)
        new_l = jnp.where(stay, roll_l, roll_u)
        upper, lower = jnp.where(bit, new_u, upper), jnp.where(bit, new_l, lower)
    return upper, lower


def skew(values, start):
    return pltpu.roll(values, start, 1, stride=SUB, stride_axis=0)


def block_turn(upper, lower, masks):
    upper, lower = rotate_up(skew(upper, 0), skew(lower, 64), masks)
    return skew(upper, 0), skew(lower, 64)


class Plan:
    def __init__(self, mesh_shape, length, coarse, fz, fy):
        self.nz, self.ny = mesh_shape
        self.count = self.nz * self.ny
        self.length, self.coarse, self.fz, self.fy = length, coarse, fz, fy
        self.j = length // self.count
        self.zo, self.yo = fz // SUB, fy // GROUP
        self.rows_out = 56
        self.rows_back = 56
        self.ext = length + 32

    def ok(self):
        return (
            (self.nz, self.ny, self.zo, self.yo, self.j) == (8, 4, 3, 3, 6)
            and self.fz % SUB == 0
            and self.fy % GROUP == 0
            and self.length == self.coarse * 2
        )


def fast_tables(plan):
    length, nz = plan.length, plan.nz
    rows, wave = basis(length)
    fine_of = np.zeros((plan.coarse, length), np.float32)
    for i in range(plan.coarse):
        fine_of[i, 2 * i] += 1.0
        for step, value in ((0, 9), (1, 9), (-1, -1), (2, -1)):
            fine_of[(i + step) % plan.coarse, 2 * i + 1] += value / 16.0
    local_z = np.zeros((plan.fz, GROUP), np.float32)
    for i in range(plan.fz // 2):
        local_z[2 * i, i + 1] = 1.0
        for step, value in ((1, 9), (2, 9), (0, -1), (3, -1)):
            local_z[2 * i + 1, i + step] += value / 16.0

    def along_z(turn):
        half_of, owner = turn // SUB, turn % SUB
        lane = np.arange(SUB)
        z_main = (owner[:, None] * plan.fz + half_of[:, None] * SUB + lane[None]).reshape(-1)
        z_shared = (owner[:, None] * plan.fz + 2 * SUB + lane[None]).reshape(-1)
        odd = np.repeat(half_of, SUB)
        tables_z = []
        for parity in (0, 1):
            table = np.zeros((2 * LANES, length))
            table[:LANES] = rows[:, z_main].T
            table[LANES:] = np.where((odd == parity)[:, None], rows[:, z_shared].T, 0.0)
            tables_z.append(table)
        return tables_z

    z_tables = along_z(np.arange(GROUP))
    y_of_row = (np.arange(plan.ext) - SUB) % length
    count = plan.count
    x_window = np.zeros((count, length + GROUP, SUB), np.float32)
    x_of_row = (np.arange(length + GROUP) - SUB) % length
    padded = np.zeros((count, SUB, length))
    for d in range(count):
        for j in range(plan.j):
            mode = rows[j * count + d]
            x_window[d, :, j] = mode[x_of_row]
            padded[d, j] = mode
        padded[d, 6:] = padded[d, 4:6]
    flat = lambda table: table.reshape(count * SUB, length)
    def halves_of(table):
        table = np.asarray(table, np.float32)
        high = table.astype(jnp.bfloat16)
        return [high, (table - high.astype(np.float32)).astype(jnp.bfloat16)]

    def pack(tables_in):
        width = max(table.shape[-1] for table in tables_in)
        return jnp.asarray(
            np.concatenate(
                [
                    np.pad(table, ((0, 0), (0, width - table.shape[-1])))
                    for table in tables_in
                ],
                0,
            )
        )

    z_all = np.stack(z_tables).reshape(-1, length)
    coarse_z = fine_of.astype(np.float64) @ rows.T
    own = plan.coarse // nz
    edge_z = np.zeros((3, LANES, length))
    for a in range(nz):
        for edge in range(3):
            at = PIECE * (a % 3) + own * edge
            edge_z[a // 3, at : at + own] = coarse_z[a * own : (a + 1) * own]
    y_table = np.zeros((length, plan.ext + GROUP))
    y_table[:, : plan.ext] = rows[:, y_of_row]
    for b in range(plan.ny):
        at, y = plan.ext + 4 * b, b * plan.fy
        y_table[:, at] = (9.0 * rows[:, y - 1] - rows[:, y - 3]) / 16.0
        y_table[:, at + 1] = -rows[:, y - 1] / 16.0
        y_table[:, at + 2] = -rows[:, (y + plan.fy + 1) % length] / 16.0
    near = [np.kron(np.eye(SUB), local_z), fine_of]
    return {
        "a": pack(halves_of(flat(padded)) + [table.astype(jnp.bfloat16) for table in near]),
        "b": pack(
            halves_of(z_all)
            + halves_of(edge_z.reshape(-1, length))
            + halves_of(y_table)
            + halves_of(rows.T)
        ),
        "window": jnp.asarray(x_window.reshape(count, 1, -1)),
    }


def near_tables(plan, near, first):
    kron_rows = SUB * plan.fz
    kron = near[first : first + kron_rows, :LANES]
    return kron, near[first + kron_rows : first + kron_rows + plan.coarse, :]


def part_a(plan, t):
    length, fz, fy, count = plan.length, plan.fz, plan.fy, plan.count
    rows_c = fy // 2
    per = plan.rows_out

    def kernel(
        cell_h, offset_h, charge_h, width_h, coarse_h, density_h, table_h, send_h, partial_h, after_h, before_h,
        cell, offset, charge, width, density, tables_v, send, partial, planes, smooth, field, after, before, sems,
    ):
        a = lax.axis_index("gz")
        b = lax.axis_index("gy")
        own = plan.coarse // plan.nz
        first = fetch(
            [
                (
                    coarse_h.at[lax.rem(own * a + plan.coarse - 1 + i, plan.coarse)],
                    planes.at[pl.ds(i * rows_c, rows_c), :],
                )
                for i in range(GROUP)
            ]
            + [(table_h, tables_v)],
            sems,
            10,
        )
        third = fy // plan.yo * length
        cuts = [slice(yo * third, (yo + 1) * third) for yo in range(plan.yo)]
        order = (2, 0, 1)
        second = {
            yo: fetch([(density_h.at[:, cuts[yo]], density.at[:, cuts[yo]])], sems, 30 + yo)[0]
            for yo in order
        }
        facts_in = fetch(
            [(cell_h, cell), (offset_h, offset), (charge_h, charge), (width_h, width)], sems, 4
        )
        for copy in first:
            copy.wait()
        kron, fine = near_tables(plan, tables_v, 2 * count * SUB)
        after[...] = planes[pl.ds(rows_c - 1, GROUP, stride=rows_c), :]
        for i in range(2):
            before[i * GROUP : (i + 1) * GROUP, :] = planes[pl.ds(i, GROUP, stride=rows_c), :]
        out_halo = fetch([(after, after_h), (before, before_h)], sems, 0)
        for part in range(rows_c // SUB):
            block = jnp.concatenate(
                [planes[pl.ds(part * SUB + y, GROUP, stride=rows_c), :] for y in range(SUB)], 0
            )
            wide = sum(mm(piece, fine, NN) for piece in thirds(block)[::-1])
            if part == 0:
                edges = [wide[i * GROUP + 1 : i * GROUP + 1 + own] for i in (0, 1)]
            if part == rows_c // SUB - 1:
                edges.append(wide[(SUB - 1) * GROUP + 1 : (SUB - 1) * GROUP + 1 + own])
            tall = sum(mm(kron, piece, NN) for piece in thirds(wide)[::-1])
            for y in range(SUB):
                smooth[part * SUB + y] = tall[y * fz : (y + 1) * fz]

        def row(i):
            return smooth[i] if 0 <= i < rows_c else jnp.zeros((fz, length), jnp.float32)

        def rows_of(yo):
            second[yo].wait()
            for i in range(yo * rows_c // plan.yo, (yo + 1) * rows_c // plan.yo):
                odd_row = (9.0 * (row(i) + row(i + 1)) - row(i - 1) - row(i + 2)) * (1.0 / 16.0)
                span = slice(2 * i * length, (2 * i + 2) * length)
                old = density[:, span]
                even_out = smooth[i] - old[:, :length]
                odd_out = odd_row - old[:, length:]
                field[2 * i] = even_out
                field[2 * i + 1] = odd_out
                partial[:, span] = jnp.concatenate([even_out, odd_out], 1)
            return fetch([(partial.at[:, cuts[yo]], partial_h.at[:, cuts[yo]])], sems, 33 + yo)

        table = (tables_v[: count * SUB, :], tables_v[count * SUB : 2 * count * SUB, :])
        sub_row = lax.broadcasted_iota(jnp.int32, (count, SUB, LANES), 1)

        def modes(block):
            out = mm3(table, halves(block), NT)
            return [
                out[:, g * LANES : (g + 1) * LANES].reshape(count, SUB, LANES)
                for g in range(out.shape[1] // LANES)
            ]

        for copy in facts_in:
            copy.wait()
        number = cell[0]
        plane = fy * length
        facts = (
            (a * fz + number // plane).astype(jnp.float32),
            (b * fy + lax.rem(number // length, fy)).astype(jnp.float32),
            lax.rem(number, length).astype(jnp.float32),
            offset[0],
            offset[1],
            offset[2],
            charge[0],
            width[0],
        )
        lane = lax.broadcasted_iota(jnp.int32, (count, SUB, LANES), 2)
        spare = jnp.zeros((count, SUB, LANES), jnp.float32)
        for i, fact in enumerate(facts):
            spare = jnp.where(lane == FACTS + i, fact, spare)
        gap = jnp.zeros((PIECE - 3 * own, length), jnp.float32)
        rest = jnp.zeros((LANES - FACTS, length), jnp.float32)
        edge_modes = modes(jnp.concatenate((edges + [gap]) * 3 + [rest], 0))[0]
        for j in range(plan.j):
            into = 6 + j // 3
            here = (lane // PIECE == j % 3) & (sub_row == into)
            spare = jnp.where(here, pltpu.roll(edge_modes, (into - j) % SUB, 1), spare)
        donor = None
        outs = []
        for yo in order:
            outs += rows_of(yo)
            block = jnp.concatenate(
                [
                    field[yo * GROUP + (-g) % GROUP, zo * SUB : (zo + 1) * SUB, :]
                    for zo in range(plan.zo)
                    for g in range(GROUP)
                ],
                0,
            )
            found = modes(block)
            if yo == 2:
                send[:, 48:56, :] = jnp.where(sub_row < 6, found[0], spare)
                donor = found[1:]
            else:
                for pair in range(3):
                    other = donor[yo]
                    if pair < 2:
                        other = pltpu.roll(other, 6 - 2 * pair, 1)
                    at = SUB * (3 * yo + pair)
                    send[:, at : at + SUB, :] = jnp.where(sub_row < 6, found[pair], other)
            span = slice(48, 56) if yo == 2 else slice(24 * yo, 24 * yo + 24)
            outs += fetch([(send.at[:, span, :], send_h.at[:, span, :])], sems, 27 + yo)
        for copy in out_halo + outs:
            copy.wait()

    hbm = pl.BlockSpec(memory_space=pltpu.HBM)
    return pl.pallas_call(
        kernel,
        name="spread",
        in_specs=[hbm] * 7,
        out_specs=[hbm] * 4,
        out_shape=[
            jax.ShapeDtypeStruct((count, per, LANES), jnp.float32),
            jax.ShapeDtypeStruct((fz, fy * length), jnp.float32),
            jax.ShapeDtypeStruct((GROUP, plan.coarse), jnp.float32),
            jax.ShapeDtypeStruct((2 * GROUP, plan.coarse), jnp.float32),
        ],
        compiler_params=pltpu.CompilerParams(vmem_limit_bytes=VMEM_LIMIT),
        scratch_shapes=[
            pltpu.SMEM((1,), jnp.int32),
            pltpu.SMEM((3,), jnp.float32),
            pltpu.SMEM((1,), jnp.float32),
            pltpu.SMEM((1,), jnp.float32),
            pltpu.VMEM((fz, fy * length), jnp.float32),
            room(t["a"]),
            pltpu.VMEM((count, per, LANES), jnp.float32),
            pltpu.VMEM((fz, fy * length), jnp.float32),
            pltpu.VMEM((GROUP * rows_c, plan.coarse), jnp.float32),
            pltpu.VMEM((rows_c, fz, length), jnp.float32),
            pltpu.VMEM((fy, fz, length), jnp.float32),
            pltpu.VMEM((GROUP, plan.coarse), jnp.float32),
            pltpu.VMEM((2 * GROUP, plan.coarse), jnp.float32),
            pltpu.SemaphoreType.DMA((36,)),
        ],
        cost_estimate=pl.CostEstimate(flops=500_000_000, bytes_accessed=4_000_000, transcendentals=0),
    )


def wrapped(distance, length):
    half = length // 2
    distance = jnp.where(distance >= half, distance - length, distance)
    return jnp.where(distance < -half, distance + length, distance)


def part_b(plan, t):
    length, count, ext = plan.length, plan.count, plan.ext
    per, per_back = plan.rows_out, plan.rows_back

    def kernel(
        window_h, recv_h, table_h, send_h,
        window, recv, tables_v, send, main, shared, bells, turned, ready, atoms_v, atoms, sem, sems, sems_in, sems_out,
    ):
        device = lax.axis_index("gz") * plan.ny + lax.axis_index("gy")

        def incoming(b):
            return pltpu.make_async_copy(recv_h.at[:, b], recv.at[:, b], sems_in.at[b])

        def outgoing(b):
            return pltpu.make_async_copy(send.at[:, b], send_h.at[:, b], sems_out.at[b])

        for b in range(plan.ny):
            incoming(b).start()
        copies = fetch(
            [
                (window_h.at[device], window),
                (table_h, tables_v),
            ],
            sems,
        )
        def unpack(b, carry):
            incoming(b).wait()
            for t in range(per // SUB):
                tiles = turn_tiles(
                    [recv[a, b, t * SUB : (t + 1) * SUB, :] for a in range(plan.nz)]
                )
                for i, tile in enumerate(tiles):
                    turned[b, t * SUB + i] = tile
            atoms_v[pl.ds(pl.multiple_of(b * SUB, SUB), SUB), :] = turned[b, SPARE]
            return carry

        lax.fori_loop(0, plan.ny, unpack, 0)
        copy = pltpu.make_async_copy(atoms_v, atoms, sem)
        copy.start()
        masks = tile_masks()
        bells[...] = jnp.zeros_like(bells)
        def gather(jp, b):
            for yo in range(plan.yo):
                tiles = []
                for k in (0, 1):
                    for zo in range(plan.zo):
                        tile = turned[b, slot(yo * plan.zo + zo, jp, k)]
                        tiles.append(tile)
                at = pl.multiple_of(b * plan.fy + yo * GROUP, SUB)
                for k in (0, 1):
                    upper, lower = block_turn(tiles[3 * k], tiles[3 * k + 1], masks)
                    main[2 * jp + k, pl.ds(at, SUB), :] = upper
                    main[2 * jp + k, pl.ds(at + SUB, SUB), :] = lower
                upper, lower = block_turn(tiles[2], tiles[5], masks)
                shared[jp, pl.ds(at, SUB), :] = upper
                shared[jp, pl.ds(at + SUB, SUB), :] = lower
        def gather_alone(b, carry):
            gather(0, b)
            return carry

        lax.fori_loop(0, plan.ny, gather_alone, 0)
        copy.wait()
        copies[0].wait()
        lane = lax.broadcasted_iota(jnp.int32, (1, LANES), 1)
        block = lane // SUB
        odd = block >= SUB
        z_first = (block & (SUB - 1)) * plan.fz + (lane & (SUB - 1))
        z_main = (z_first + jnp.where(odd, SUB, 0)).astype(jnp.float32)
        z_shared = (z_first + 2 * SUB).astype(jnp.float32)
        window_rows = lax.broadcasted_iota(jnp.int32, (GROUP, LANES), 0).astype(jnp.float32) - RC

        def deposit(i):
            z0, y0, x0, off_z, off_y, off_x, charge, width = (atoms[i, FACTS + f] for f in range(8))
            ratio = jnp.full((SUB, LANES), width / jnp.pi, jnp.float32)
            factor = ratio * jnp.sqrt(ratio) * charge
            factor = factor[0:1]
            cut = jnp.exp(jnp.full((SUB, LANES), -width * float(RC * RC), jnp.float32))[0:1]
            profile_y = jnp.exp(-width * (window_rows - off_y) ** 2)
            profile_x = jnp.exp(-width * (window_rows - off_x) ** 2)
            planes = []
            for z in (z_main, z_shared):
                profile_z = jnp.exp(-width * (wrapped(z - z0, length) - off_z) ** 2)
                planes.append(profile_y * profile_z)
            base = (x0.astype(jnp.int32) - RC + SUB) * SUB
            zero = jnp.zeros((GROUP, LANES), jnp.float32)
            sums = [[zero, zero, zero] for _ in range(plan.j // 2)]
            for dx in range(2 * RC + 2):
                line = profile_x[dx : dx + 1]
                bell = [jnp.maximum(plane * line - cut, 0.0) for plane in planes]
                for jp in range(plan.j // 2):
                    even = window[0, base + dx * SUB + 2 * jp]
                    odd_value = window[0, base + dx * SUB + 2 * jp + 1]
                    sums[jp][0] += bell[0] * even
                    sums[jp][1] += bell[0] * odd_value
                    sums[jp][2] += bell[1] * jnp.where(odd, odd_value, even)
            at = y0.astype(jnp.int32) - RC + SUB
            for jp in range(plan.j // 2):
                for k in (0, 1):
                    bells[2 * jp + k, pl.ds(at, GROUP), :] += sums[jp][k] * factor
                bells[plan.j + jp, pl.ds(at, GROUP), :] += sums[jp][2] * factor

        steps = plan.ny * (plan.j // 2 - 1)

        def gather_and_deposit(step, carry):
            for i in range(count // steps):
                deposit(step * (count // steps) + i)
            gather(1 + step // plan.ny, lax.rem(step, plan.ny))
            return carry

        lax.fori_loop(0, steps, gather_and_deposit, 0)
        for item in copies[1:]:
            item.wait()
        scale = float(length) ** 2 / math.pi
        half = length // 2

        def square(mode):
            wave = jnp.where(mode <= half, mode, mode - half)
            return (wave * wave).astype(jnp.float32)

        plane = square(lax.broadcasted_iota(jnp.int32, (length, length), 0)) + square(
            lax.broadcasted_iota(jnp.int32, (length, length), 1)
        )
        zt, et, yt, yti = [], [], [], []
        at = 0
        for into, size, width, parts in (
            (zt, 2 * LANES, length, 2),
            (et, 3 * LANES, length, 1),
            (yt, length, ext + GROUP, 1),
            (yti, length, length, 1),
        ):
            for half_index in range(2):
                into.append(
                    [tables_v[at + i * size : at + (i + 1) * size, :width] for i in range(parts)]
                )
                at += parts * size
        edge_row = lax.broadcasted_iota(jnp.int32, (GROUP, LANES), 0)
        edge_lane = lax.broadcasted_iota(jnp.int32, (GROUP, LANES), 1)
        own = plan.coarse // plan.nz
        first_lane = own * (edge_row & 3)
        lines = []
        for row in range(2):
            spread = [turned[b, SPARE + row] for b in range(plan.ny)]
            for q in range(3):
                blocks = []
                for a in range(plan.nz):
                    if a % 3 == 0:
                        blocks.append(jnp.zeros((GROUP, LANES), jnp.float32))
                    line = jnp.concatenate(
                        [jnp.broadcast_to(tile[a : a + 1], (4, LANES)) for tile in spread], 0
                    )
                    shift = (PIECE * (a % 3 - q)) % LANES
                    line = pltpu.roll(line, shift, 1) if shift else line
                    start = first_lane + PIECE * (a % 3)
                    keep = (edge_lane >= start) & (edge_lane < start + own) & ((edge_row & 3) < 3)
                    blocks[-1] = jnp.where(keep, line, blocks[-1])
                lines.append(jnp.concatenate(blocks, 1))
        edges_z = mm3(halves(jnp.concatenate(lines, 0)), (et[0][0], et[1][0]))
        def with_bells(block, index):
            top, last = SUB, SUB + length
            return jnp.concatenate(
                [
                    bells[index, :top, :],
                    block + bells[index, top:last, :],
                    bells[index, last:, :],
                ],
                0,
            )

        energy = jnp.zeros((SUB, length), jnp.float32)
        first = masks[0] == 0

        def scatter(jp, b):
            for yo in range(plan.yo):
                at = b * plan.fy + yo * GROUP
                found = []
                for source in (main.at[2 * jp], main.at[2 * jp + 1], shared.at[jp]):
                    upper, lower = block_turn(
                        source[at : at + SUB, :], source[at + SUB : at + GROUP, :], masks
                    )
                    found.append(
                        (jnp.where(first, upper, lower), jnp.where(first, lower, upper))
                    )
                for k in (0, 1):
                    for zo, tile in enumerate((found[k][0], found[k][1], found[2][k])):
                        ready[b, slot(yo * plan.zo + zo, jp, k)] = tile

        rows_z = []
        for k in (0, 1):
            left = jnp.concatenate(
                [
                    jnp.concatenate(
                        [with_bells(main[2 * jp + k], 2 * jp + k), with_bells(shared[jp], plan.j + jp)],
                        1,
                    )
                    for jp in range(plan.j // 2)
                ],
                0,
            )
            rows_z.append(mm3(halves(left), (zt[0][k], zt[1][k])))
        for jp in range(plan.j // 2):
            rows_y = []
            for k in (0, 1):
                j = 2 * jp + k
                column = jnp.concatenate(
                    [rows_z[k][jp * ext : (jp + 1) * ext], edges_z[j * GROUP : (j + 1) * GROUP]], 0
                )
                full = mm3((yt[0][0], yt[1][0]), halves(column))
                squares = plane + square(j * count + device)
                weight = jnp.where(squares > 0.0, scale / jnp.maximum(squares, 1.0), 0.0)
                weighted = full * weight
                product = full * weighted
                for i in range(length // SUB):
                    energy += product[i * SUB : (i + 1) * SUB]
                rows_y.append(mm3((yti[0][0], yti[1][0]), halves(weighted)))
            backs = [mm3(halves(rows_y[k]), (zt[0][k], zt[1][k]), NT) for k in (0, 1)]
            for k in (0, 1):
                main[2 * jp + k] = backs[k][:, :LANES]
            shared[jp] = backs[0][:, LANES:] + backs[1][:, LANES:]
            for b in range(plan.ny):
                scatter(jp, b)
        share = jnp.sum(energy) * (1.0 / count)

        def pack(b, carry):
            for row in (SPARE, SPARE + 1):
                ready[b, row] = jnp.full((SUB, LANES), share, jnp.float32)
            for t in range(per_back // SUB):
                tiles = turn_tiles([ready[b, t * SUB + i] for i in range(SUB)])
                for i, tile in enumerate(tiles):
                    a = (SUB - i) % SUB
                    send[a, b, t * SUB : (t + 1) * SUB, :] = tile
            outgoing(b).start()
            return carry

        lax.fori_loop(0, plan.ny, pack, 0)
        for b in range(plan.ny):
            outgoing(b).wait()

    hbm = pl.BlockSpec(memory_space=pltpu.HBM)
    vmem = pl.BlockSpec(memory_space=pltpu.VMEM)
    return pl.pallas_call(
        kernel,
        name="solve",
        in_specs=[hbm, hbm, hbm],
        out_specs=hbm,
        out_shape=jax.ShapeDtypeStruct((plan.nz, plan.ny, per_back, LANES), jnp.float32),
        compiler_params=pltpu.CompilerParams(vmem_limit_bytes=VMEM_LIMIT),
        scratch_shapes=[
            pltpu.SMEM(t["window"].shape[1:], jnp.float32),
            pltpu.VMEM((plan.nz, plan.ny, per, LANES), jnp.float32),
            room(t["b"]),
            pltpu.VMEM((plan.nz, plan.ny, per_back, LANES), jnp.float32),
            pltpu.VMEM((plan.j, length, LANES), jnp.float32),
            pltpu.VMEM((plan.j // 2, length, LANES), jnp.float32),
            pltpu.VMEM((plan.j + plan.j // 2, ext, LANES), jnp.float32),
            pltpu.VMEM((plan.ny, per, SUB, LANES), jnp.float32),
            pltpu.VMEM((plan.ny, per_back, SUB, LANES), jnp.float32),
            pltpu.VMEM((count, LANES), jnp.float32),
            pltpu.SMEM((count, LANES), jnp.float32),
            pltpu.SemaphoreType.DMA,
            pltpu.SemaphoreType.DMA((2,)),
            pltpu.SemaphoreType.DMA((plan.ny,)),
            pltpu.SemaphoreType.DMA((plan.ny,)),
        ],
        cost_estimate=pl.CostEstimate(flops=2_000_000_000, bytes_accessed=4_000_000, transcendentals=0),
    )


def part_r(plan, t):
    length, fz, fy, count = plan.length, plan.fz, plan.fy, plan.count
    per = plan.rows_out

    def kernel(
        recv, partial_h, below_h, above_h, table_h, out_h,
        partial, tables_v, out, field, lines, atoms_v, atoms, sem, sems,
    ):
        lines[...] = jnp.zeros_like(lines)
        copies = fetch(
            [
                (partial_h, partial),
                (table_h, tables_v),
                (below_h, lines.at[pl.ds(0, GROUP), :]),
                (above_h, lines.at[pl.ds(GROUP, 2 * GROUP), :]),
            ],
            sems,
        )
        a = lax.axis_index("gz")
        b = lax.axis_index("gy")
        for i in range(count):
            atoms_v[i : i + 1, :] = recv[i, SPARE : SPARE + 1, :]
        copy = pltpu.make_async_copy(atoms_v, atoms, sem)
        copy.start()
        for item in copies:
            item.wait()
        kron, fine = near_tables(plan, tables_v, 2 * count * SUB)
        block = lines[...]
        wide = sum(mm(piece, fine, NN) for piece in thirds(block)[::-1])
        tall = sum(mm(kron, piece, NN) for piece in thirds(wide)[::-1])
        below, above, above2 = (tall[i * fz : (i + 1) * fz] for i in range(3))
        field[...] = jnp.zeros_like(field)
        field[1] = below * (-1.0 / 16.0)
        field[fy - 3] = above * (-1.0 / 16.0)
        field[fy - 1] = (9.0 * above - above2) * (1.0 / 16.0)
        copy.wait()
        z_here = lax.broadcasted_iota(jnp.int32, (fz, length), 0).astype(jnp.float32)
        x_here = lax.broadcasted_iota(jnp.int32, (fz, length), 1).astype(jnp.float32)

        def deposit(i, carry):
            z0 = wrapped(atoms[i, FACTS + 0] - (a * fz).astype(jnp.float32), length)
            y0 = wrapped(atoms[i, FACTS + 1] - (b * fy).astype(jnp.float32), length).astype(jnp.int32)
            first = jnp.maximum(y0 - RC, 0)
            last = jnp.minimum(y0 + RC + 2, fy)
            near_z = (z0 > -RC - 2.0) & (z0 < fz + RC + 1.0)

            @pl.when(near_z & (first < last))
            def _():
                off_z, off_y, off_x = atoms[i, FACTS + 3], atoms[i, FACTS + 4], atoms[i, FACTS + 5]
                charge, width = atoms[i, FACTS + 6], atoms[i, FACTS + 7]
                ratio = jnp.full((fz, length), width / jnp.pi, jnp.float32)
                factor = ratio * jnp.sqrt(ratio) * charge
                cut = jnp.exp(jnp.full((fz, length), -width * float(RC * RC), jnp.float32))
                dist_z = z_here - z0 - off_z
                dist_x = wrapped(x_here - atoms[i, FACTS + 2], length) - off_x
                flat = dist_z * dist_z + dist_x * dist_x

                def row(y, inner):
                    dist_y = (y - y0).astype(jnp.float32) - off_y
                    bell = jnp.maximum(jnp.exp(-width * (flat + dist_y * dist_y)) - cut, 0.0)
                    field[y] += bell * factor
                    return inner

                lax.fori_loop(first, last, row, 0)

            return carry

        lax.fori_loop(0, count, deposit, 0)
        for i in range(fy // 2):
            span = slice(2 * i * length, (2 * i + 2) * length)
            out[:, span] = partial[:, span] + jnp.concatenate([field[2 * i], field[2 * i + 1]], 1)
        for item in fetch([(out, out_h)], sems, 4):
            item.wait()

    hbm = pl.BlockSpec(memory_space=pltpu.HBM)
    vmem = pl.BlockSpec(memory_space=pltpu.VMEM)
    return pl.pallas_call(
        kernel,
        name="finish",
        compiler_params=pltpu.CompilerParams(vmem_limit_bytes=VMEM_LIMIT),
        in_specs=[vmem] + [hbm] * 4,
        out_specs=hbm,
        out_shape=jax.ShapeDtypeStruct((fz, fy * length), jnp.float32),
        scratch_shapes=[
            pltpu.VMEM((fz, fy * length), jnp.float32),
            room(t["a"]),
            pltpu.VMEM((fz, fy * length), jnp.float32),
            pltpu.VMEM((fy, fz, length), jnp.float32),
            pltpu.VMEM((SUB * GROUP, plan.coarse), jnp.float32),
            pltpu.VMEM((count, LANES), jnp.float32),
            pltpu.SMEM((count, LANES), jnp.float32),
            pltpu.SemaphoreType.DMA,
            pltpu.SemaphoreType.DMA((5,)),
        ],
        cost_estimate=pl.CostEstimate(flops=3_000_000_000, bytes_accessed=4_000_000, transcendentals=0),
    )


def part_c(plan, t, terms):
    length, fz, fy, count = plan.length, plan.fz, plan.fy, plan.count
    per = plan.rows_back
    wide = 3 * LANES

    def kernel(
        recv, early, table_h, history_h, potential_h, sums, tables_v, history, potential, sems
    ):
        first = fetch([(table_h.at[: 2 * count * SUB, :], tables_v)], sems)
        ahead = early.shape[0]
        copies = [None] * ahead + fetch(
            [(history_h.at[i], history.at[i - ahead]) for i in range(ahead, terms)], sems, 2
        )
        first[0].wait()
        size = count * SUB
        table = (tables_v[:size, :], tables_v[size:, :])
        sub_row = lax.broadcasted_iota(jnp.int32, (count, SUB, LANES), 1)

        def back(tile):
            return mm3(halves(tile.reshape(size, LANES).T), table)

        def place(block, values):
            yo, zo = block // plan.zo, block % plan.zo
            for pair in range(GROUP // 2):
                at = (yo * GROUP + 2 * pair) * length
                rows = values[2 * pair * SUB : (2 * pair + 2) * SUB]
                potential[zo * SUB : (zo + 1) * SUB, at : at + 2 * length] = jnp.concatenate(
                    [rows[:SUB], rows[SUB:]], 1
                )

        spare = [jnp.zeros((count, SUB, LANES), jnp.float32)] * 2
        for t in range(per // SUB):
            tile = recv[:, t * SUB : (t + 1) * SUB, :]
            place(t, back(jnp.where(sub_row < 6, tile, 0.0)))
            if t < 6:
                pair = t % 3
                moved = pltpu.roll(tile, (2 * pair + 2) % SUB, 1)
                spare[t // 3] = jnp.where(sub_row // 2 == pair, moved, spare[t // 3])
        place(7, back(spare[0]))
        place(8, back(spare[1]))
        out = fetch([(potential, potential_h)], sems, 2 + terms)
        acc = []
        for i in range(terms):
            def add(c, total, i=i):
                cut = pl.ds(pl.multiple_of(c * wide, LANES), wide)
                other = early[i, :, cut] if i < ahead else history[i - ahead, :, cut]
                return total + other * potential[:, cut]

            if i >= ahead:
                copies[i].wait()
            acc.append(
                lax.fori_loop(
                    0, fy * length // wide, add, jnp.zeros((fz, wide), jnp.float32), unroll=4
                )
            )
        lane = lax.broadcasted_iota(jnp.int32, (1, LANES), 1)
        line = jnp.zeros((1, LANES), jnp.float32)
        for i in range(terms):
            line = jnp.where(lane == i, jnp.sum(acc[i]), line)
        own = jnp.sum(recv[:, SPARE : SPARE + 1, :], axis=0)
        line = jnp.where(lane == terms, own, line)
        sums[...] = jnp.broadcast_to(line * (1.0 / float(length) ** 3), (count, LANES))
        out[0].wait()

    hbm = pl.BlockSpec(memory_space=pltpu.HBM)
    vmem = pl.BlockSpec(memory_space=pltpu.VMEM)
    return pl.pallas_call(
        kernel,
        name="finish_potential",
        in_specs=[vmem, vmem, hbm, hbm],
        out_specs=[hbm, vmem],
        scratch_shapes=[
            pltpu.VMEM((2 * count * SUB, length), jnp.bfloat16),
            pltpu.VMEM((terms - EARLY, fz, fy * length), jnp.float32),
            pltpu.VMEM((fz, fy * length), jnp.float32),
            pltpu.SemaphoreType.DMA((3 + terms,)),
        ],
        out_shape=[
            jax.ShapeDtypeStruct((fz, fy * length), jnp.float32),
            jax.ShapeDtypeStruct((count, LANES), jnp.float32),
        ],
        compiler_params=pltpu.CompilerParams(vmem_limit_bytes=LATE_LIMIT),
        cost_estimate=pl.CostEstimate(flops=500_000_000, bytes_accessed=10_000_000, transcendentals=0),
    )


def exchange(sent, axes):
    return lax.all_to_all(sent, axes, 0, 0, tiled=True)


def local_fast(plan, coarse_density, density_in, history, atom_cell, atom_offset, atom_charge, atom_width):
    axes = ("gz", "gy")
    count = plan.count
    tables_ = fast_tables(plan)
    sent, partial, after, before = part_a(plan, tables_)(
        atom_cell.reshape(1),
        atom_offset.reshape(3),
        atom_charge.reshape(1),
        atom_width.reshape(1),
        coarse_density,
        density_in,
        tables_["a"],
    )
    spectra = exchange(sent, axes)
    solved = part_b(plan, tables_)(
        tables_["window"],
        spectra.reshape((plan.nz, plan.ny) + spectra.shape[1:]),
        tables_["b"],
    )
    early, solved = lax.optimization_barrier((history, solved))
    early = early[:EARLY]
    back = exchange(solved.reshape((count,) + solved.shape[2:]), axes)
    ring = [(i, (i + 1) % plan.ny) for i in range(plan.ny)]
    below = lax.ppermute(after, "gy", ring)
    above = lax.ppermute(before, "gy", [(target, source) for source, target in ring])
    residual = part_r(plan, tables_)(spectra, partial, below, above, tables_["a"])
    potential, sums = part_c(plan, tables_, history.shape[0])(back, early, tables_["a"], history)
    rows = lax.all_to_all(sums, axes, 0, 0, tiled=True)
    return residual, potential, jnp.sum(rows, 0)[: history.shape[0] + 1]


def solution(mesh):
    in_specs = (
        P(None, "gy", None),
        P("gz", "gy"),
        P(None, "gz", "gy"),
        P("gz", "gy", None),
        P(None, "gz", "gy", None),
        P("gz", "gy", None),
        P("gz", "gy", None),
    )
    out_specs = (P("gz", "gy"), P("gz", "gy"), P())

    def body(*arguments):
        coarse_density, density_in = arguments[:2]
        plan = Plan(
            (mesh.shape["gz"], mesh.shape["gy"]),
            2 * coarse_density.shape[0],
            coarse_density.shape[0],
            density_in.shape[0],
            2 * coarse_density.shape[1],
        )
        if plan.ok():
            return local_fast(plan, *arguments)
        return local(*arguments)

    return jax.shard_map(body, mesh=mesh, in_specs=in_specs, out_specs=out_specs, check_vma=False)
```

```python
import math

import jax
import jax.numpy as jnp
import numpy as np
from jax import lax
from jax.experimental import pallas as pl
from jax.experimental.pallas import tpu as pltpu
from jax.sharding import PartitionSpec as P

RC = 4
NF = 192


def with_halo(block, sides, width):
    for axis, dim in sides:
        count = lax.axis_size(axis)
        forward = [(i, i + 1) for i in range(count - 1)]
        forward.append((count - 1, 0))
        backward = [(target, source) for source, target in forward]
        low = lax.ppermute(
            lax.slice_in_dim(block, block.shape[dim] - width, None, axis=dim), axis, forward
        )
        high = lax.ppermute(lax.slice_in_dim(block, 0, width, axis=dim), axis, backward)
        block = jnp.concatenate([low, block, high], axis=dim)
    return block


def midpoint(extended, dimension, cells_in):

    def window(offset):
        return lax.slice_in_dim(extended, offset, offset + cells_in, axis=dimension)

    even_cells = window(2)
    odd_cells = (9.0 * (window(2) + window(3)) - window(1) - window(4)) / 16.0
    merged = jnp.stack([even_cells, odd_cells], dimension + 1)
    new_shape = list(even_cells.shape)
    new_shape[dimension] = 2 * cells_in
    return merged.reshape(new_shape)


def signed(counter, length):
    return jnp.where(counter < length // 2, counter, counter - length)


def shape_value(squared, charge, exponent):
    factor = charge * (exponent / jnp.pi) ** 1.5
    return factor * jnp.maximum(
        jnp.exp(-exponent * squared) - jnp.exp(-exponent * float(RC * RC)), 0.0
    )


def gaussians(dist_z, dist_y, dist_x, charge, exponent):
    squared = (
        dist_z[:, :, None, None] ** 2
        + dist_y[:, None, :, None] ** 2
        + dist_x[:, None, None, :] ** 2
    )
    return jnp.sum(
        shape_value(squared, charge[:, None, None, None], exponent[:, None, None, None]), 0
    )


def tables(length):
    counter = jnp.arange(length, dtype=jnp.int32)
    phase = counter[:, None] * counter[None, :] % length
    angle = 2.0 * jnp.pi / length * phase.astype(jnp.float32)
    return (jnp.cos(angle), jnp.sin(angle))


def contract(values, table, dimension):
    product = jnp.tensordot(values, table, axes=([dimension], [0]), precision=lax.Precision.HIGHEST)
    return jnp.moveaxis(product, -1, dimension)


def transform(spectra, dimension, direction):
    cosine, sine_table = tables(spectra.shape[dimension])
    inner_dim = dimension - 1
    real_part = spectra[:, 0]
    imag_part = spectra[:, 1]
    new_real = contract(real_part, cosine, inner_dim) - direction * contract(
        imag_part, sine_table, inner_dim
    )
    new_imag = contract(imag_part, cosine, inner_dim) + direction * contract(
        real_part, sine_table, inner_dim
    )
    result = jnp.stack([new_real, new_imag], 1)
    if direction > 0:
        result = result / spectra.shape[dimension]
    return result


def transform_y(pieces):
    return transform(pieces, 3, -1.0)


def transform_z(pieces):
    return transform(pieces, 2, -1.0)


def inverse_y(pieces):
    return transform(pieces, 3, 1.0)


def inverse_x_real(pieces):
    cosine, sine_table = tables(pieces.shape[4])
    real_part = contract(pieces[:, 0], cosine, 3) - contract(pieces[:, 1], sine_table, 3)
    return real_part / pieces.shape[4]


def forward(fields):
    cosine, sine_table = tables(fields.shape[3])
    spectra = jnp.stack([contract(fields, cosine, 3), -contract(fields, sine_table, 3)], 1)
    columns = transform_y(lax.all_to_all(spectra, "gy", split_axis=4, concat_axis=3, tiled=True))
    return transform_z(lax.all_to_all(columns, "gz", split_axis=3, concat_axis=2, tiled=True))


def inverse(spectra):
    local_z = transform(spectra, 2, 1.0)
    rows_back = inverse_y(lax.all_to_all(local_z, "gz", split_axis=2, concat_axis=3, tiled=True))
    return inverse_x_real(lax.all_to_all(rows_back, "gy", split_axis=3, concat_axis=4, tiled=True))


def poisson_weight(spectra):
    length = spectra.shape[2]
    y_block = spectra.shape[3]
    x_block = spectra.shape[4]
    wave_z = signed(jnp.arange(length, dtype=jnp.int32), length)
    wave_y = signed(lax.axis_index("gz") * y_block + jnp.arange(y_block, dtype=jnp.int32), length)
    wave_x = signed(lax.axis_index("gy") * x_block + jnp.arange(x_block, dtype=jnp.int32), length)
    squares = (
        wave_z[:, None, None] * wave_z[:, None, None]
        + wave_y[None, :, None] * wave_y[None, :, None]
        + wave_x[None, None, :] * wave_x[None, None, :]
    )
    scaled = (2.0 * jnp.pi / length) ** 2 * jnp.maximum(squares, 1).astype(jnp.float32)
    return jnp.where(squares > 0, 4.0 * jnp.pi / scaled, 0.0)


def total_intersections(own_terms):
    return lax.psum(own_terms, ("gz", "gy"))


def deposit_rims(atom_cell, atom_offset, atom_charge, atom_width, slab_z, slab_y, length):
    cell_ids = atom_cell.reshape(-1)
    local_z = cell_ids // (slab_y * length)
    local_y = cell_ids // length % slab_y
    local_x = cell_ids % length
    offsets = atom_offset.reshape(3, -1)
    dist_z = (jnp.arange(slab_z + 2 * RC, dtype=jnp.int32)[None, :] - RC - local_z[:, None]).astype(
        jnp.float32
    ) - offsets[0][:, None]
    dist_y = (jnp.arange(slab_y + 2 * RC, dtype=jnp.int32)[None, :] - RC - local_y[:, None]).astype(
        jnp.float32
    ) - offsets[1][:, None]
    dist_x = (
        signed(
            (jnp.arange(length, dtype=jnp.int32)[None, :] - local_x[:, None]) % length, length
        ).astype(jnp.float32)
        - offsets[2][:, None]
    )
    buffer_sum = gaussians(dist_z, dist_y, dist_x, atom_charge.reshape(-1), atom_width.reshape(-1))
    rims_z = jnp.concatenate([buffer_sum[:RC], buffer_sum[-RC:]], 0)
    near_z = with_halo(rims_z, (("gz", 0),), RC)
    middle = buffer_sum[RC : RC + slab_z]
    middle = middle.at[:RC].add(near_z[:RC]).at[slab_z - RC :].add(near_z[3 * RC :])
    rims_y = jnp.concatenate([middle[:, :RC], middle[:, -RC:]], 1)
    near_y = with_halo(rims_y, (("gy", 1),), RC)
    inside = middle[:, RC : RC + slab_y]
    return inside.at[:, :RC].add(near_y[:, :RC]).at[:, slab_y - RC :].add(near_y[:, 3 * RC :])


def local(coarse_density, density_in, history, atom_cell, atom_offset, atom_charge, atom_width):
    length = NF
    slab_z = density_in.shape[0]
    slab_y = density_in.shape[1] // length
    density_cube = density_in.reshape(slab_z, slab_y, length)
    history_cube = history.reshape(history.shape[0], slab_z, slab_y, length)
    extended = with_halo(coarse_density, (("gy", 1),), 2)
    coarse_rows = coarse_density.shape[0] // lax.axis_size("gz")
    beside_all = jnp.concatenate([extended[-2:], extended, extended[:2]], 0)
    start = lax.axis_index("gz") * coarse_rows
    own_planes = lax.dynamic_slice_in_dim(beside_all, start, coarse_rows + 4, 0)
    wrapped = jnp.concatenate([own_planes[:, :, -2:], own_planes, own_planes[:, :, :2]], 2)
    smooth = midpoint(wrapped, 2, coarse_density.shape[2])
    smooth = midpoint(smooth, 1, coarse_density.shape[1])
    smooth = midpoint(smooth, 0, coarse_rows)
    charge_field = deposit_rims(
        atom_cell, atom_offset, atom_charge, atom_width, slab_z, slab_y, length
    )
    residual = smooth + charge_field - density_cube
    cells_all = float(length) ** 3
    spectra = forward(residual[None])
    weight = poisson_weight(spectra)
    potential = inverse(weight * spectra)[0]
    own_terms = (
        jnp.concatenate(
            [
                jnp.sum(history_cube * potential[None], axis=(1, 2, 3)),
                jnp.sum(residual * potential)[None],
            ]
        )
        / cells_all
    )
    intersections = total_intersections(own_terms)
    return (
        residual.reshape(slab_z, slab_y * length),
        potential.reshape(slab_z, slab_y * length),
        intersections,
    )


GROUP = 16
LANES = 128
SUB = 8


def basis(length):
    half = length // 2
    wave = np.concatenate([np.arange(half + 1), np.arange(1, half)])
    angle = 2.0 * np.pi / length * (np.outer(wave, np.arange(length)) % length)
    rows = np.where(np.arange(length)[:, None] <= half, np.cos(angle), np.sin(angle))
    scale = np.where((wave == 0) | (wave == half), 1.0, np.sqrt(2.0)) / np.sqrt(length)
    return rows * scale[:, None], wave


def halves(values):
    high = values.astype(jnp.bfloat16)
    return high, (values - high.astype(jnp.float32)).astype(jnp.bfloat16)


def thirds(values):
    high = values.astype(jnp.bfloat16)
    rest = values - high.astype(jnp.float32)
    middle = rest.astype(jnp.bfloat16)
    return high, middle, (rest - middle.astype(jnp.float32)).astype(jnp.bfloat16)


NN = (((1,), (0,)), ((), ()))
NT = (((1,), (1,)), ((), ()))


def mm(left, right, dims):
    return lax.dot_general(left, right, dims, preferred_element_type=jnp.float32)


def mm3(left, right, dims=NN):
    rows = left[0].shape[0]
    both = mm(jnp.concatenate(left, 0), right[0], dims)
    return mm(left[0], right[1], dims) + both[rows:] + both[:rows]


def turn_tiles(tiles):
    row = lax.broadcasted_iota(jnp.int32, (SUB, LANES), 0)
    tiles = list(tiles)
    for step in (4, 2, 1):
        own = (row & step) == 0
        for i in range(SUB):
            if i & step == 0:
                first, second = tiles[i], tiles[i + step]
                tiles[i] = jnp.where(own, first, pltpu.roll(second, step, 0))
                tiles[i + step] = jnp.where(own, pltpu.roll(first, SUB - step, 0), second)
    return tiles


def slot(g, pair, k):
    if g < 7:
        return SUB * g + 2 * pair + k
    return SUB * (3 * (g - 7) + pair) + 6 + k


def fetch(pairs, sems, first=0):
    copies = [
        pltpu.make_async_copy(source, target, sems.at[first + i])
        for i, (source, target) in enumerate(pairs)
    ]
    for copy in copies:
        copy.start()
    return copies


def room(array):
    return pltpu.VMEM(array.shape, array.dtype)


SPARE = 54
PIECE = 40
FACTS = 3 * PIECE
VMEM_LIMIT = 60 * 1024 * 1024
EARLY = 2
SOLVE_LIMIT = 48 * 1024 * 1024
LATE_LIMIT = 48 * 1024 * 1024


def tile_masks():
    row = lax.broadcasted_iota(jnp.int32, (SUB, LANES), 0)
    group = lax.broadcasted_iota(jnp.int32, (SUB, LANES), 1) // SUB
    return row, group


def rotate_up(upper, lower, masks):
    row, group = masks
    bit = (group & 8) != 0
    upper, lower = jnp.where(bit, lower, upper), jnp.where(bit, upper, lower)
    for shift in (4, 2, 1):
        bit = (group & shift) != 0
        roll_u = pltpu.roll(upper, SUB - shift, 0)
        roll_l = pltpu.roll(lower, SUB - shift, 0)
        stay = row < SUB - shift
        new_u = jnp.where(stay, roll_u, roll_l)
        new_l = jnp.where(stay, roll_l, roll_u)
        upper, lower = jnp.where(bit, new_u, upper), jnp.where(bit, new_l, lower)
    return upper, lower


def skew(values, start):
    return pltpu.roll(values, start, 1, stride=SUB, stride_axis=0)


def block_turn(upper, lower, masks):
    upper, lower = rotate_up(skew(upper, 0), skew(lower, 64), masks)
    return skew(upper, 0), skew(lower, 64)


class Plan:
    def __init__(self, mesh_shape, length, coarse, fz, fy):
        self.nz, self.ny = mesh_shape
        self.count = self.nz * self.ny
        self.length, self.coarse, self.fz, self.fy = length, coarse, fz, fy
        self.j = length // self.count
        self.zo, self.yo = fz // SUB, fy // GROUP
        self.rows_out = 56
        self.rows_back = 56
        self.ext = length + 32

    def ok(self):
        return (
            (self.nz, self.ny, self.zo, self.yo, self.j) == (8, 4, 3, 3, 6)
            and self.fz % SUB == 0
            and self.fy % GROUP == 0
            and self.length == self.coarse * 2
        )


def fast_tables(plan):
    length, nz = plan.length, plan.nz
    rows, wave = basis(length)
    fine_of = np.zeros((plan.coarse, length), np.float32)
    for i in range(plan.coarse):
        fine_of[i, 2 * i] += 1.0
        for step, value in ((0, 9), (1, 9), (-1, -1), (2, -1)):
            fine_of[(i + step) % plan.coarse, 2 * i + 1] += value / 16.0
    local_z = np.zeros((plan.fz, GROUP), np.float32)
    for i in range(plan.fz // 2):
        local_z[2 * i, i + 1] = 1.0
        for step, value in ((1, 9), (2, 9), (0, -1), (3, -1)):
            local_z[2 * i + 1, i + step] += value / 16.0

    def along_z(turn):
        half_of, owner = turn // SUB, turn % SUB
        lane = np.arange(SUB)
        z_main = (owner[:, None] * plan.fz + half_of[:, None] * SUB + lane[None]).reshape(-1)
        z_shared = (owner[:, None] * plan.fz + 2 * SUB + lane[None]).reshape(-1)
        odd = np.repeat(half_of, SUB)
        tables_z = []
        for parity in (0, 1):
            table = np.zeros((2 * LANES, length))
            table[:LANES] = rows[:, z_main].T
            table[LANES:] = np.where((odd == parity)[:, None], rows[:, z_shared].T, 0.0)
            tables_z.append(table)
        return tables_z

    z_tables = along_z(np.arange(GROUP))
    y_of_row = (np.arange(plan.ext) - SUB) % length
    count = plan.count
    x_window = np.zeros((count, length + GROUP, SUB), np.float32)
    x_of_row = (np.arange(length + GROUP) - SUB) % length
    padded = np.zeros((count, SUB, length))
    for d in range(count):
        for j in range(plan.j):
            mode = rows[j * count + d]
            x_window[d, :, j] = mode[x_of_row]
            padded[d, j] = mode
        padded[d, 6:] = padded[d, 4:6]
    flat = lambda table: table.reshape(count * SUB, length)
    def halves_of(table):
        table = np.asarray(table, np.float32)
        high = table.astype(jnp.bfloat16)
        return [high, (table - high.astype(np.float32)).astype(jnp.bfloat16)]

    def pack(tables_in):
        width = max(table.shape[-1] for table in tables_in)
        return jnp.asarray(
            np.concatenate(
                [
                    np.pad(table, ((0, 0), (0, width - table.shape[-1])))
                    for table in tables_in
                ],
                0,
            )
        )

    z_all = np.stack(z_tables).reshape(-1, length)
    coarse_z = fine_of.astype(np.float64) @ rows.T
    own = plan.coarse // nz
    edge_z = np.zeros((3, LANES, length))
    for a in range(nz):
        for edge in range(3):
            at = PIECE * (a % 3) + own * edge
            edge_z[a // 3, at : at + own] = coarse_z[a * own : (a + 1) * own]
    y_table = np.zeros((length, plan.ext + GROUP))
    y_table[:, : plan.ext] = rows[:, y_of_row]
    for b in range(plan.ny):
        at, y = plan.ext + 4 * b, b * plan.fy
        y_table[:, at] = (9.0 * rows[:, y - 1] - rows[:, y - 3]) / 16.0
        y_table[:, at + 1] = -rows[:, y - 1] / 16.0
        y_table[:, at + 2] = -rows[:, (y + plan.fy + 1) % length] / 16.0
    near = [np.kron(np.eye(SUB), local_z), fine_of]
    return {
        "a": pack(halves_of(flat(padded)) + [table.astype(jnp.bfloat16) for table in near]),
        "b": pack(
            halves_of(z_all)
            + halves_of(edge_z.reshape(-1, length))
            + halves_of(y_table)
            + halves_of(rows.T)
        ),
        "window": jnp.asarray(x_window.reshape(count, 1, -1)),
    }


def near_tables(plan, near, first):
    kron_rows = SUB * plan.fz
    kron = near[first : first + kron_rows, :LANES]
    return kron, near[first + kron_rows : first + kron_rows + plan.coarse, :]


def part_a(plan, t):
    length, fz, fy, count = plan.length, plan.fz, plan.fy, plan.count
    rows_c = fy // 2
    per = plan.rows_out

    def kernel(
        cell_h, offset_h, charge_h, width_h, coarse_h, density_h, table_h, send_h, partial_h, after_h, before_h,
        cell, offset, charge, width, density, tables_v, send, partial, planes, smooth, field, after, before, sems,
    ):
        a = lax.axis_index("gz")
        b = lax.axis_index("gy")
        own = plan.coarse // plan.nz
        first = fetch(
            [
                (
                    coarse_h.at[lax.rem(own * a + plan.coarse - 1 + i, plan.coarse)],
                    planes.at[pl.ds(i * rows_c, rows_c), :],
                )
                for i in range(GROUP)
            ]
            + [(table_h, tables_v)],
            sems,
            10,
        )
        third = fy // plan.yo * length
        cuts = [slice(yo * third, (yo + 1) * third) for yo in range(plan.yo)]
        order = (2, 0, 1)
        second = {
            yo: fetch([(density_h.at[:, cuts[yo]], density.at[:, cuts[yo]])], sems, 30 + yo)[0]
            for yo in order
        }
        facts_in = fetch(
            [(cell_h, cell), (offset_h, offset), (charge_h, charge), (width_h, width)], sems, 4
        )
        for copy in first:
            copy.wait()
        kron, fine = near_tables(plan, tables_v, 2 * count * SUB)
        after[...] = planes[pl.ds(rows_c - 1, GROUP, stride=rows_c), :]
        for i in range(2):
            before[i * GROUP : (i + 1) * GROUP, :] = planes[pl.ds(i, GROUP, stride=rows_c), :]
        out_halo = fetch([(after, after_h), (before, before_h)], sems, 0)
        for part in range(rows_c // SUB):
            block = jnp.concatenate(
                [planes[pl.ds(part * SUB + y, GROUP, stride=rows_c), :] for y in range(SUB)], 0
            )
            wide = sum(mm(piece, fine, NN) for piece in thirds(block)[::-1])
            if part == 0:
                edges = [wide[i * GROUP + 1 : i * GROUP + 1 + own] for i in (0, 1)]
            if part == rows_c // SUB - 1:
                edges.append(wide[(SUB - 1) * GROUP + 1 : (SUB - 1) * GROUP + 1 + own])
            tall = sum(mm(kron, piece, NN) for piece in thirds(wide)[::-1])
            for y in range(SUB):
                smooth[part * SUB + y] = tall[y * fz : (y + 1) * fz]

        def row(i):
            return smooth[i] if 0 <= i < rows_c else jnp.zeros((fz, length), jnp.float32)

        def rows_of(yo):
            second[yo].wait()
            for i in range(yo * rows_c // plan.yo, (yo + 1) * rows_c // plan.yo):
                odd_row = (9.0 * (row(i) + row(i + 1)) - row(i - 1) - row(i + 2)) * (1.0 / 16.0)
                span = slice(2 * i * length, (2 * i + 2) * length)
                old = density[:, span]
                even_out = smooth[i] - old[:, :length]
                odd_out = odd_row - old[:, length:]
                field[2 * i] = even_out
                field[2 * i + 1] = odd_out
                partial[:, span] = jnp.concatenate([even_out, odd_out], 1)
            return fetch([(partial.at[:, cuts[yo]], partial_h.at[:, cuts[yo]])], sems, 33 + yo)

        table = (tables_v[: count * SUB, :], tables_v[count * SUB : 2 * count * SUB, :])
        sub_row = lax.broadcasted_iota(jnp.int32, (count, SUB, LANES), 1)

        def modes(block):
            out = mm3(table, halves(block), NT)
            return [
                out[:, g * LANES : (g + 1) * LANES].reshape(count, SUB, LANES)
                for g in range(out.shape[1] // LANES)
            ]

        for copy in facts_in:
            copy.wait()
        number = cell[0]
        plane = fy * length
        facts = (
            (a * fz + number // plane).astype(jnp.float32),
            (b * fy + lax.rem(number // length, fy)).astype(jnp.float32),
            lax.rem(number, length).astype(jnp.float32),
            offset[0],
            offset[1],
            offset[2],
            charge[0],
            width[0],
        )
        lane = lax.broadcasted_iota(jnp.int32, (count, SUB, LANES), 2)
        spare = jnp.zeros((count, SUB, LANES), jnp.float32)
        for i, fact in enumerate(facts):
            spare = jnp.where(lane == FACTS + i, fact, spare)
        gap = jnp.zeros((PIECE - 3 * own, length), jnp.float32)
        rest = jnp.zeros((LANES - FACTS, length), jnp.float32)
        edge_modes = modes(jnp.concatenate((edges + [gap]) * 3 + [rest], 0))[0]
        for j in range(plan.j):
            into = 6 + j // 3
            here = (lane // PIECE == j % 3) & (sub_row == into)
            spare = jnp.where(here, pltpu.roll(edge_modes, (into - j) % SUB, 1), spare)
        donor = None
        outs = []
        for yo in order:
            outs += rows_of(yo)
            block = jnp.concatenate(
                [
                    field[yo * GROUP + (-g) % GROUP, zo * SUB : (zo + 1) * SUB, :]
                    for zo in range(plan.zo)
                    for g in range(GROUP)
                ],
                0,
            )
            found = modes(block)
            if yo == 2:
                send[:, 48:56, :] = jnp.where(sub_row < 6, found[0], spare)
                donor = found[1:]
            else:
                for pair in range(3):
                    other = donor[yo]
                    if pair < 2:
                        other = pltpu.roll(other, 6 - 2 * pair, 1)
                    at = SUB * (3 * yo + pair)
                    send[:, at : at + SUB, :] = jnp.where(sub_row < 6, found[pair], other)
            span = slice(48, 56) if yo == 2 else slice(24 * yo, 24 * yo + 24)
            outs += fetch([(send.at[:, span, :], send_h.at[:, span, :])], sems, 27 + yo)
        for copy in out_halo + outs:
            copy.wait()

    hbm = pl.BlockSpec(memory_space=pltpu.HBM)
    return pl.pallas_call(
        kernel,
        name="spread",
        in_specs=[hbm] * 7,
        out_specs=[hbm] * 4,
        out_shape=[
            jax.ShapeDtypeStruct((count, per, LANES), jnp.float32),
            jax.ShapeDtypeStruct((fz, fy * length), jnp.float32),
            jax.ShapeDtypeStruct((GROUP, plan.coarse), jnp.float32),
            jax.ShapeDtypeStruct((2 * GROUP, plan.coarse), jnp.float32),
        ],
        compiler_params=pltpu.CompilerParams(vmem_limit_bytes=VMEM_LIMIT),
        scratch_shapes=[
            pltpu.SMEM((1,), jnp.int32),
            pltpu.SMEM((3,), jnp.float32),
            pltpu.SMEM((1,), jnp.float32),
            pltpu.SMEM((1,), jnp.float32),
            pltpu.VMEM((fz, fy * length), jnp.float32),
            room(t["a"]),
            pltpu.VMEM((count, per, LANES), jnp.float32),
            pltpu.VMEM((fz, fy * length), jnp.float32),
            pltpu.VMEM((GROUP * rows_c, plan.coarse), jnp.float32),
            pltpu.VMEM((rows_c, fz, length), jnp.float32),
            pltpu.VMEM((fy, fz, length), jnp.float32),
            pltpu.VMEM((GROUP, plan.coarse), jnp.float32),
            pltpu.VMEM((2 * GROUP, plan.coarse), jnp.float32),
            pltpu.SemaphoreType.DMA((36,)),
        ],
        cost_estimate=pl.CostEstimate(flops=500_000_000, bytes_accessed=4_000_000, transcendentals=0),
    )


def wrapped(distance, length):
    half = length // 2
    distance = jnp.where(distance >= half, distance - length, distance)
    return jnp.where(distance < -half, distance + length, distance)


def part_b(plan, t):
    length, count, ext = plan.length, plan.count, plan.ext
    per, per_back = plan.rows_out, plan.rows_back

    def kernel(
        window_h, recv, table_h, send_h,
        window, tables_v, send, main, shared, bells, turned, ready, atoms_v, atoms, sem, sems, sems_out,
    ):
        device = lax.axis_index("gz") * plan.ny + lax.axis_index("gy")

        def outgoing(b):
            return pltpu.make_async_copy(send.at[:, b], send_h.at[:, b], sems_out.at[b])

        copies = fetch(
            [
                (window_h.at[0], window),
                (table_h, tables_v),
            ],
            sems,
        )
        def unpack(b, carry):
            for t in range(per // SUB):
                tiles = turn_tiles(
                    [recv[a, b, t * SUB : (t + 1) * SUB, :] for a in range(plan.nz)]
                )
                for i, tile in enumerate(tiles):
                    turned[b, t * SUB + i] = tile
            atoms_v[pl.ds(pl.multiple_of(b * SUB, SUB), SUB), :] = turned[b, SPARE]
            return carry

        lax.fori_loop(0, plan.ny, unpack, 0)
        copy = pltpu.make_async_copy(atoms_v, atoms, sem)
        copy.start()
        masks = tile_masks()
        bells[...] = jnp.zeros_like(bells)
        def gather(jp, b):
            for yo in range(plan.yo):
                tiles = []
                for k in (0, 1):
                    for zo in range(plan.zo):
                        tile = turned[b, slot(yo * plan.zo + zo, jp, k)]
                        tiles.append(tile)
                at = pl.multiple_of(b * plan.fy + yo * GROUP, SUB)
                for k in (0, 1):
                    upper, lower = block_turn(tiles[3 * k], tiles[3 * k + 1], masks)
                    main[2 * jp + k, pl.ds(at, SUB), :] = upper
                    main[2 * jp + k, pl.ds(at + SUB, SUB), :] = lower
                upper, lower = block_turn(tiles[2], tiles[5], masks)
                shared[jp, pl.ds(at, SUB), :] = upper
                shared[jp, pl.ds(at + SUB, SUB), :] = lower
        def gather_alone(b, carry):
            gather(0, b)
            return carry

        lax.fori_loop(0, plan.ny, gather_alone, 0)
        copy.wait()
        copies[0].wait()
        lane = lax.broadcasted_iota(jnp.int32, (1, LANES), 1)
        block = lane // SUB
        odd = block >= SUB
        z_first = (block & (SUB - 1)) * plan.fz + (lane & (SUB - 1))
        z_main = (z_first + jnp.where(odd, SUB, 0)).astype(jnp.float32)
        z_shared = (z_first + 2 * SUB).astype(jnp.float32)
        window_rows = lax.broadcasted_iota(jnp.int32, (GROUP, LANES), 0).astype(jnp.float32) - RC

        def deposit(i):
            z0, y0, x0, off_z, off_y, off_x, charge, width = (atoms[i, FACTS + f] for f in range(8))
            ratio = jnp.full((SUB, LANES), width / jnp.pi, jnp.float32)
            factor = ratio * jnp.sqrt(ratio) * charge
            factor = factor[0:1]
            cut = jnp.exp(jnp.full((SUB, LANES), -width * float(RC * RC), jnp.float32))[0:1]
            profile_y = jnp.exp(-width * (window_rows - off_y) ** 2)
            profile_x = jnp.exp(-width * (window_rows - off_x) ** 2)
            planes = []
            for z in (z_main, z_shared):
                profile_z = jnp.exp(-width * (wrapped(z - z0, length) - off_z) ** 2)
                planes.append(profile_y * profile_z)
            base = (x0.astype(jnp.int32) - RC + SUB) * SUB
            zero = jnp.zeros((GROUP, LANES), jnp.float32)
            sums = [[zero, zero, zero] for _ in range(plan.j // 2)]
            for dx in range(2 * RC + 2):
                line = profile_x[dx : dx + 1]
                bell = [jnp.maximum(plane * line - cut, 0.0) for plane in planes]
                for jp in range(plan.j // 2):
                    even = window[0, base + dx * SUB + 2 * jp]
                    odd_value = window[0, base + dx * SUB + 2 * jp + 1]
                    sums[jp][0] += bell[0] * even
                    sums[jp][1] += bell[0] * odd_value
                    sums[jp][2] += bell[1] * jnp.where(odd, odd_value, even)
            at = y0.astype(jnp.int32) - RC + SUB
            for jp in range(plan.j // 2):
                for k in (0, 1):
                    bells[2 * jp + k, pl.ds(at, GROUP), :] += sums[jp][k] * factor
                bells[plan.j + jp, pl.ds(at, GROUP), :] += sums[jp][2] * factor

        steps = plan.ny * (plan.j // 2 - 1)

        def gather_and_deposit(step, carry):
            for i in range(count // steps):
                deposit(step * (count // steps) + i)
            gather(1 + step // plan.ny, lax.rem(step, plan.ny))
            return carry

        lax.fori_loop(0, steps, gather_and_deposit, 0)
        for item in copies[1:]:
            item.wait()
        scale = float(length) ** 2 / math.pi
        half = length // 2

        def square(mode):
            wave = jnp.where(mode <= half, mode, mode - half)
            return (wave * wave).astype(jnp.float32)

        plane = square(lax.broadcasted_iota(jnp.int32, (length, length), 0)) + square(
            lax.broadcasted_iota(jnp.int32, (length, length), 1)
        )
        zt, et, yt, yti = [], [], [], []
        at = 0
        for into, size, width, parts in (
            (zt, 2 * LANES, length, 2),
            (et, 3 * LANES, length, 1),
            (yt, length, ext + GROUP, 1),
            (yti, length, length, 1),
        ):
            for half_index in range(2):
                into.append(
                    [tables_v[at + i * size : at + (i + 1) * size, :width] for i in range(parts)]
                )
                at += parts * size
        edge_row = lax.broadcasted_iota(jnp.int32, (GROUP, LANES), 0)
        edge_lane = lax.broadcasted_iota(jnp.int32, (GROUP, LANES), 1)
        own = plan.coarse // plan.nz
        first_lane = own * (edge_row & 3)
        lines = []
        for row in range(2):
            spread = [turned[b, SPARE + row] for b in range(plan.ny)]
            for q in range(3):
                blocks = []
                for a in range(plan.nz):
                    if a % 3 == 0:
                        blocks.append(jnp.zeros((GROUP, LANES), jnp.float32))
                    line = jnp.concatenate(
                        [jnp.broadcast_to(tile[a : a + 1], (4, LANES)) for tile in spread], 0
                    )
                    shift = (PIECE * (a % 3 - q)) % LANES
                    line = pltpu.roll(line, shift, 1) if shift else line
                    start = first_lane + PIECE * (a % 3)
                    keep = (edge_lane >= start) & (edge_lane < start + own) & ((edge_row & 3) < 3)
                    blocks[-1] = jnp.where(keep, line, blocks[-1])
                lines.append(jnp.concatenate(blocks, 1))
        edges_z = mm3(halves(jnp.concatenate(lines, 0)), (et[0][0], et[1][0]))
        def with_bells(block, index):
            top, last = SUB, SUB + length
            return jnp.concatenate(
                [
                    bells[index, :top, :],
                    block + bells[index, top:last, :],
                    bells[index, last:, :],
                ],
                0,
            )

        energy = jnp.zeros((SUB, length), jnp.float32)
        first = masks[0] == 0

        def scatter(jp, b):
            for yo in range(plan.yo):
                at = b * plan.fy + yo * GROUP
                found = []
                for source in (main.at[2 * jp], main.at[2 * jp + 1], shared.at[jp]):
                    upper, lower = block_turn(
                        source[at : at + SUB, :], source[at + SUB : at + GROUP, :], masks
                    )
                    found.append(
                        (jnp.where(first, upper, lower), jnp.where(first, lower, upper))
                    )
                for k in (0, 1):
                    for zo, tile in enumerate((found[k][0], found[k][1], found[2][k])):
                        ready[b, slot(yo * plan.zo + zo, jp, k)] = tile

        rows_z = []
        for k in (0, 1):
            left = jnp.concatenate(
                [
                    jnp.concatenate(
                        [with_bells(main[2 * jp + k], 2 * jp + k), with_bells(shared[jp], plan.j + jp)],
                        1,
                    )
                    for jp in range(plan.j // 2)
                ],
                0,
            )
            rows_z.append(mm3(halves(left), (zt[0][k], zt[1][k])))
        for jp in range(plan.j // 2):
            rows_y = []
            for k in (0, 1):
                j = 2 * jp + k
                column = jnp.concatenate(
                    [rows_z[k][jp * ext : (jp + 1) * ext], edges_z[j * GROUP : (j + 1) * GROUP]], 0
                )
                full = mm3((yt[0][0], yt[1][0]), halves(column))
                squares = plane + square(j * count + device)
                weight = jnp.where(squares > 0.0, scale / jnp.maximum(squares, 1.0), 0.0)
                weighted = full * weight
                product = full * weighted
                for i in range(length // SUB):
                    energy += product[i * SUB : (i + 1) * SUB]
                rows_y.append(mm3((yti[0][0], yti[1][0]), halves(weighted)))
            backs = [mm3(halves(rows_y[k]), (zt[0][k], zt[1][k]), NT) for k in (0, 1)]
            for k in (0, 1):
                main[2 * jp + k] = backs[k][:, :LANES]
            shared[jp] = backs[0][:, LANES:] + backs[1][:, LANES:]
            for b in range(plan.ny):
                scatter(jp, b)
        share = jnp.sum(energy) * (1.0 / count)

        def pack(b, carry):
            ready[b, SPARE] = jnp.full((SUB, LANES), share, jnp.float32)
            ready[b, SPARE + 1] = turned[b, SPARE]
            for t in range(per_back // SUB):
                tiles = turn_tiles([ready[b, t * SUB + i] for i in range(SUB)])
                for i, tile in enumerate(tiles):
                    a = (SUB - i) % SUB
                    send[a, b, t * SUB : (t + 1) * SUB, :] = tile
            outgoing(b).start()
            return carry

        lax.fori_loop(0, plan.ny, pack, 0)
        for b in range(plan.ny):
            outgoing(b).wait()

    hbm = pl.BlockSpec(memory_space=pltpu.HBM)
    vmem = pl.BlockSpec(memory_space=pltpu.VMEM)
    return pl.pallas_call(
        kernel,
        name="solve",
        in_specs=[hbm, pl.BlockSpec(memory_space=pltpu.VMEM), hbm],
        out_specs=hbm,
        out_shape=jax.ShapeDtypeStruct((plan.nz, plan.ny, per_back, LANES), jnp.float32),
        compiler_params=pltpu.CompilerParams(vmem_limit_bytes=SOLVE_LIMIT),
        scratch_shapes=[
            pltpu.SMEM(t["window"].shape[1:], jnp.float32),
            room(t["b"]),
            pltpu.VMEM((plan.nz, plan.ny, per_back, LANES), jnp.float32),
            pltpu.VMEM((plan.j, length, LANES), jnp.float32),
            pltpu.VMEM((plan.j // 2, length, LANES), jnp.float32),
            pltpu.VMEM((plan.j + plan.j // 2, ext, LANES), jnp.float32),
            pltpu.VMEM((plan.ny, per, SUB, LANES), jnp.float32),
            pltpu.VMEM((plan.ny, per_back, SUB, LANES), jnp.float32),
            pltpu.VMEM((count, LANES), jnp.float32),
            pltpu.SMEM((count, LANES), jnp.float32),
            pltpu.SemaphoreType.DMA,
            pltpu.SemaphoreType.DMA((2,)),
            pltpu.SemaphoreType.DMA((plan.ny,)),
        ],
        cost_estimate=pl.CostEstimate(flops=2_000_000_000, bytes_accessed=4_000_000, transcendentals=0),
    )


def part_r(plan, t):
    length, fz, fy, count = plan.length, plan.fz, plan.fy, plan.count
    per = plan.rows_out

    def kernel(
        solved, partial_h, below_h, above_h, table_h, out_h,
        partial, tables_v, out, field, lines, atoms_v, atoms, sem, sems,
    ):
        lines[...] = jnp.zeros_like(lines)
        copies = fetch(
            [
                (partial_h, partial),
                (table_h, tables_v),
                (below_h, lines.at[pl.ds(0, GROUP), :]),
                (above_h, lines.at[pl.ds(GROUP, 2 * GROUP), :]),
            ],
            sems,
        )
        a = lax.axis_index("gz")
        b = lax.axis_index("gy")
        for i in range(count):
            atoms_v[i : i + 1, :] = solved[i, SPARE + 1 : SPARE + 2, :]
        copy = pltpu.make_async_copy(atoms_v, atoms, sem)
        copy.start()
        for item in copies:
            item.wait()
        kron, fine = near_tables(plan, tables_v, 2 * count * SUB)
        block = lines[...]
        wide = sum(mm(piece, fine, NN) for piece in thirds(block)[::-1])
        tall = sum(mm(kron, piece, NN) for piece in thirds(wide)[::-1])
        below, above, above2 = (tall[i * fz : (i + 1) * fz] for i in range(3))
        field[...] = jnp.zeros_like(field)
        field[1] = below * (-1.0 / 16.0)
        field[fy - 3] = above * (-1.0 / 16.0)
        field[fy - 1] = (9.0 * above - above2) * (1.0 / 16.0)
        copy.wait()
        z_here = lax.broadcasted_iota(jnp.int32, (fz, length), 0).astype(jnp.float32)
        x_here = lax.broadcasted_iota(jnp.int32, (fz, length), 1).astype(jnp.float32)

        def deposit(i, carry):
            z0 = wrapped(atoms[i, FACTS + 0] - (a * fz).astype(jnp.float32), length)
            y0 = wrapped(atoms[i, FACTS + 1] - (b * fy).astype(jnp.float32), length).astype(jnp.int32)
            first = jnp.maximum(y0 - RC, 0)
            last = jnp.minimum(y0 + RC + 2, fy)
            near_z = (z0 > -RC - 2.0) & (z0 < fz + RC + 1.0)

            @pl.when(near_z & (first < last))
            def _():
                off_z, off_y, off_x = atoms[i, FACTS + 3], atoms[i, FACTS + 4], atoms[i, FACTS + 5]
                charge, width = atoms[i, FACTS + 6], atoms[i, FACTS + 7]
                ratio = jnp.full((fz, length), width / jnp.pi, jnp.float32)
                factor = ratio * jnp.sqrt(ratio) * charge
                cut = jnp.exp(jnp.full((fz, length), -width * float(RC * RC), jnp.float32))
                dist_z = z_here - z0 - off_z
                dist_x = wrapped(x_here - atoms[i, FACTS + 2], length) - off_x
                flat = dist_z * dist_z + dist_x * dist_x

                def row(y, inner):
                    dist_y = (y - y0).astype(jnp.float32) - off_y
                    bell = jnp.maximum(jnp.exp(-width * (flat + dist_y * dist_y)) - cut, 0.0)
                    field[y] += bell * factor
                    return inner

                lax.fori_loop(first, last, row, 0)

            return carry

        lax.fori_loop(0, count, deposit, 0)
        for i in range(fy // 2):
            span = slice(2 * i * length, (2 * i + 2) * length)
            out[:, span] = partial[:, span] + jnp.concatenate([field[2 * i], field[2 * i + 1]], 1)
        for item in fetch([(out, out_h)], sems, 4):
            item.wait()

    hbm = pl.BlockSpec(memory_space=pltpu.HBM)
    vmem = pl.BlockSpec(memory_space=pltpu.VMEM)
    return pl.pallas_call(
        kernel,
        name="finish",
        compiler_params=pltpu.CompilerParams(vmem_limit_bytes=VMEM_LIMIT),
        in_specs=[vmem] + [hbm] * 4,
        out_specs=hbm,
        out_shape=jax.ShapeDtypeStruct((fz, fy * length), jnp.float32),
        scratch_shapes=[
            pltpu.VMEM((fz, fy * length), jnp.float32),
            room(t["a"]),
            pltpu.VMEM((fz, fy * length), jnp.float32),
            pltpu.VMEM((fy, fz, length), jnp.float32),
            pltpu.VMEM((SUB * GROUP, plan.coarse), jnp.float32),
            pltpu.VMEM((count, LANES), jnp.float32),
            pltpu.SMEM((count, LANES), jnp.float32),
            pltpu.SemaphoreType.DMA,
            pltpu.SemaphoreType.DMA((5,)),
        ],
        cost_estimate=pl.CostEstimate(flops=3_000_000_000, bytes_accessed=4_000_000, transcendentals=0),
    )


def part_c(plan, t, terms):
    length, fz, fy, count = plan.length, plan.fz, plan.fy, plan.count
    per = plan.rows_back
    wide = 3 * LANES

    def kernel(
        recv, early, table_h, history_h, potential_h, sums, tables_v, history, potential, sems
    ):
        first = fetch([(table_h.at[: 2 * count * SUB, :], tables_v)], sems)
        ahead = early.shape[0]
        copies = [None] * ahead + fetch(
            [(history_h.at[i], history.at[i - ahead]) for i in range(ahead, terms)], sems, 2
        )
        first[0].wait()
        size = count * SUB
        table = (tables_v[:size, :], tables_v[size:, :])
        sub_row = lax.broadcasted_iota(jnp.int32, (count, SUB, LANES), 1)

        def back(tile):
            return mm3(halves(tile.reshape(size, LANES).T), table)

        def place(block, values):
            yo, zo = block // plan.zo, block % plan.zo
            for pair in range(GROUP // 2):
                at = (yo * GROUP + 2 * pair) * length
                rows = values[2 * pair * SUB : (2 * pair + 2) * SUB]
                potential[zo * SUB : (zo + 1) * SUB, at : at + 2 * length] = jnp.concatenate(
                    [rows[:SUB], rows[SUB:]], 1
                )

        spare = [jnp.zeros((count, SUB, LANES), jnp.float32)] * 2
        for t in range(per // SUB):
            tile = recv[:, t * SUB : (t + 1) * SUB, :]
            place(t, back(jnp.where(sub_row < 6, tile, 0.0)))
            if t < 6:
                pair = t % 3
                moved = pltpu.roll(tile, (2 * pair + 2) % SUB, 1)
                spare[t // 3] = jnp.where(sub_row // 2 == pair, moved, spare[t // 3])
        place(7, back(spare[0]))
        place(8, back(spare[1]))
        out = fetch([(potential, potential_h)], sems, 2 + terms)
        acc = []
        for i in range(terms):
            def add(c, total, i=i):
                cut = pl.ds(pl.multiple_of(c * wide, LANES), wide)
                other = early[i, :, cut] if i < ahead else history[i - ahead, :, cut]
                return total + other * potential[:, cut]

            if i >= ahead:
                copies[i].wait()
            acc.append(
                lax.fori_loop(
                    0, fy * length // wide, add, jnp.zeros((fz, wide), jnp.float32), unroll=4
                )
            )
        lane = lax.broadcasted_iota(jnp.int32, (1, LANES), 1)
        line = jnp.zeros((1, LANES), jnp.float32)
        for i in range(terms):
            line = jnp.where(lane == i, jnp.sum(acc[i]), line)
        own = jnp.sum(recv[:, SPARE : SPARE + 1, :], axis=0)
        line = jnp.where(lane == terms, own, line)
        sums[...] = jnp.broadcast_to(line * (1.0 / float(length) ** 3), (count, LANES))
        out[0].wait()

    hbm = pl.BlockSpec(memory_space=pltpu.HBM)
    vmem = pl.BlockSpec(memory_space=pltpu.VMEM)
    return pl.pallas_call(
        kernel,
        name="finish_potential",
        in_specs=[vmem, vmem, hbm, hbm],
        out_specs=[hbm, vmem],
        scratch_shapes=[
            pltpu.VMEM((2 * count * SUB, length), jnp.bfloat16),
            pltpu.VMEM((terms - EARLY, fz, fy * length), jnp.float32),
            pltpu.VMEM((fz, fy * length), jnp.float32),
            pltpu.SemaphoreType.DMA((3 + terms,)),
        ],
        out_shape=[
            jax.ShapeDtypeStruct((fz, fy * length), jnp.float32),
            jax.ShapeDtypeStruct((count, LANES), jnp.float32),
        ],
        compiler_params=pltpu.CompilerParams(vmem_limit_bytes=LATE_LIMIT),
        cost_estimate=pl.CostEstimate(flops=500_000_000, bytes_accessed=10_000_000, transcendentals=0),
    )


def exchange(sent, axes):
    return lax.all_to_all(sent, axes, 0, 0, tiled=True)


def local_fast(plan, coarse_density, density_in, history, atom_cell, atom_offset, atom_charge, atom_width):
    axes = ("gz", "gy")
    count = plan.count
    tables_ = fast_tables(plan)
    sent, partial, after, before = part_a(plan, tables_)(
        atom_cell.reshape(1),
        atom_offset.reshape(3),
        atom_charge.reshape(1),
        atom_width.reshape(1),
        coarse_density,
        density_in,
        tables_["a"],
    )
    spectra = exchange(sent, axes)
    device = lax.axis_index("gz") * plan.ny + lax.axis_index("gy")
    window = lax.dynamic_slice_in_dim(tables_["window"], device, 1, 0)
    solved = part_b(plan, tables_)(
        window,
        spectra.reshape((plan.nz, plan.ny) + spectra.shape[1:]),
        tables_["b"],
    )
    early, solved = lax.optimization_barrier((history, solved))
    early = early[:EARLY]
    solved = solved.reshape((count,) + solved.shape[2:])
    back = exchange(solved, axes)
    ring = [(i, (i + 1) % plan.ny) for i in range(plan.ny)]
    below = lax.ppermute(after, "gy", ring)
    above = lax.ppermute(before, "gy", [(target, source) for source, target in ring])
    residual = part_r(plan, tables_)(solved, partial, below, above, tables_["a"])
    potential, sums = part_c(plan, tables_, history.shape[0])(back, early, tables_["a"], history)
    rows = lax.all_to_all(sums, axes, 0, 0, tiled=True)
    return residual, potential, jnp.sum(rows, 0)[: history.shape[0] + 1]


def solution(mesh):
    in_specs = (
        P(None, "gy", None),
        P("gz", "gy"),
        P(None, "gz", "gy"),
        P("gz", "gy", None),
        P(None, "gz", "gy", None),
        P("gz", "gy", None),
        P("gz", "gy", None),
    )
    out_specs = (P("gz", "gy"), P("gz", "gy"), P())

    def body(*arguments):
        coarse_density, density_in = arguments[:2]
        plan = Plan(
            (mesh.shape["gz"], mesh.shape["gy"]),
            2 * coarse_density.shape[0],
            coarse_density.shape[0],
            density_in.shape[0],
            2 * coarse_density.shape[1],
        )
        if plan.ok():
            return local_fast(plan, *arguments)
        return local(*arguments)

    return jax.shard_map(body, mesh=mesh, in_specs=in_specs, out_specs=out_specs, check_vma=False)
```
